32 devices in a mesh: batch: 8 (over z, y), vocab: 4 (over x, core).
Axes of the slice: x: 2, y: 2, z: 4, core: 2. Of those that a mesh axis runs over, the one named last changes fastest.
Arguments:
- hidden: bfloat16 [4096, 3584], P(('batch', 'vocab')), may hold values from -6 to 6
- head_weight: bfloat16 [3072, 3584], P('vocab', 'batch'), may hold values from -0.3125 to 0.3125
- targets: int32 [4096], P(('batch', 'vocab')), may hold values from 0 to 3071
- valid_mask: int32 [4096], P(('batch', 'vocab')), may hold values 0 or 1
Outputs:
- head_grad: float32 [3072, 3584], P('vocab', 'batch')
- hidden_grad: float32 [4096, 3584], P(('batch', 'vocab'))
- mean_loss: float32 [], replicated
The draws below stay inside these ranges and needn't reach their ends.
All inputs are finite; a program needn't handle non-finite values. No bound on the sum of `valid_mask` on one device may be relied on, other than what follows from the above.
Results may differ from the reference program's by a relative error of at most 0.0019.
Values may be sent and summed in bfloat16 or wider, within the bound.
A program may use at most 128 MiB of HBM per device.

```python
import jax
import jax.numpy as jnp
from jax import lax

D = 3584
GROUP_TOK = 512
TOKENS = 4096
VOCAB = 3072
N_BATCH = 8


def set_ends(drawn, stream_key, smallest, top_value):
    spot = [jax.random.randint(jax.random.fold_in(stream_key, axis), (), 0, length) for axis, length in enumerate(drawn.shape)]
    longest = drawn.shape.index(max(drawn.shape))
    neighbour = spot[:longest] + [(spot[longest] + 1) % drawn.shape[longest]] + spot[longest + 1:]
    return drawn.at[tuple(spot)].set(smallest).at[tuple(neighbour)].set(top_value)


def steps_of(rng, dims, split, low, high):
    def one(axis_at, parts):
        steps = jax.random.uniform(jax.random.fold_in(jax.random.fold_in(rng, 6), axis_at), (parts,), jnp.float32, low / len(split), high / len(split))
        return jnp.repeat(jnp.exp(steps), dims[axis_at] // parts).reshape((-1,) + (1,) * (len(dims) - axis_at - 1))

    gain = one(*split[0])
    for cut in split[1:]:
        gain = gain * one(*cut)
    return gain


def normal_values(stream_key, dims, scale, most, shards=(), held_as=jnp.bfloat16):
    factor_of = steps_of(stream_key, dims, shards, -0.22, 0.18) if shards else 1.0
    array = jax.random.normal(stream_key, dims, jnp.float32) * scale * factor_of
    return jnp.minimum(jnp.maximum(array, -most), most).astype(held_as)


def setup_inputs(seed: int = 0) -> dict:
    arg_keys = jax.random.split(jax.random.key(seed), 5)
    hidden = normal_values(arg_keys[0], (TOKENS, D), 1.0, 6.0, ((0, 32),))
    head_weight = normal_values(arg_keys[1], (VOCAB, D), (D // 9) ** -0.5, 0.3125, ((0, 4), (1, 8)))
    targets = set_ends(jax.random.randint(arg_keys[2], (TOKENS,), 0, VOCAB), jax.random.fold_in(arg_keys[2], 1), 0, VOCAB - 1).astype(jnp.int32)
    valid_mask = set_ends((jax.random.randint(arg_keys[3], (TOKENS,), 0, 4) < 3).astype(jnp.int32), jax.random.fold_in(arg_keys[3], 1), 0, 1)
    return {"hidden": hidden, "head_weight": head_weight, "targets": targets, "valid_mask": valid_mask}


softcap = 30.0


def reference(hidden, head_weight, targets, valid_mask):
    positions = hidden.shape[0]
    model_width = hidden.shape[1]
    state_blocks = hidden.reshape(N_BATCH, GROUP_TOK, model_width)
    target_blocks = targets.reshape(N_BATCH, GROUP_TOK)
    mask_blocks = valid_mask.reshape(N_BATCH, GROUP_TOK)
    vocab_ids = jnp.arange(VOCAB, dtype=jnp.int32)

    def token_block(running, scanned):
        grad_total, loss_total = running
        row_block, target_ids, mask_block = scanned
        scores = lax.dot_general(row_block, head_weight, (((1,), (1,)), ((), ())), preferred_element_type=jnp.float32)
        logits = softcap * jnp.tanh(scores / softcap)
        target_hit = vocab_ids[None, :] == target_ids[:, None]
        exponent = jnp.exp(logits)
        partition = jnp.sum(exponent, axis=1)
        target_logit = jnp.sum(jnp.where(target_hit, logits, 0.0), axis=1)
        weight = mask_block.astype(jnp.float32)
        slope = 1.0 - (logits / softcap) ** 2
        delta_logit = (weight[:, None] * (exponent / partition[:, None] - target_hit.astype(jnp.float32)) * slope).astype(jnp.bfloat16)
        grad_total = grad_total + lax.dot_general(delta_logit, row_block, (((0,), (0,)), ((), ())), preferred_element_type=jnp.float32)
        loss_total = loss_total + jnp.sum(weight * (jnp.log(partition) - target_logit))
        state_grad = jnp.dot(delta_logit, head_weight, preferred_element_type=jnp.float32)
        return (grad_total, loss_total), state_grad

    start_grad = jnp.zeros(head_weight.shape, jnp.float32)
    start_loss = jnp.zeros((), jnp.float32)
    (head_grad, loss_total), state_grads = lax.scan(token_block, (start_grad, start_loss), (state_blocks, target_blocks, mask_blocks))
    hidden_grad = state_grads.reshape(positions, model_width)
    mean_loss = loss_total / positions
    return head_grad, hidden_grad, mean_loss
```

```python
import functools

import jax
import jax.numpy as jnp
from jax import lax
from jax.experimental import pallas as pl
from jax.experimental.pallas import tpu as pltpu
from jax.sharding import PartitionSpec as P

softcap = 30.0
MESH = pl.DeviceIdType.MESH
f32, bf16 = jnp.float32, jnp.bfloat16


def chunk_of(length, most):
    return max(s for s in range(16, most + 1, 16) if length % s == 0)


def kernel(sizes, h_in, w_in, code_in, head_out, hid_out, loss_out, h_all, w_all, code_got, code_all,
           logits, delta, stat_own, stat_all, loss_own, loss_all, grad, grad_send, r_in,
           part, core_in, x_out, x_in, y_out, y_in, far_own, far_in, *sems):
    nz, ny, nx, nv = sizes
    (own_sem, hs, hf, hd, hr, ws_up, ws_dn, ws_y, wr, cs, cr, ss, sr, ls, lr,
     rs, rr, ds, dr, xs, xr, ys, yr, fs, fr) = sems
    nb = nz * ny
    rows, width = h_in.shape
    cols, half = w_in.shape[1:]
    group = ny * nv
    tokens = rows * group
    entries = ny * half
    b, v = lax.axis_index("batch"), lax.axis_index("vocab")
    z, y = lax.div(b, ny), lax.rem(b, ny)
    x, core = lax.div(v, 2), lax.rem(v, 2)
    other = x * 2 + 1 - core
    me = y * nv + v

    def at(bb, vv):
        return {"batch": bb, "vocab": vv}

    def copy(src, dst, send, recv, bb, vv):
        return pltpu.make_async_remote_copy(
            src_ref=src, dst_ref=dst, send_sem=send, recv_sem=recv, device_id=at(bb, vv), device_id_type=MESH)

    def hrow(i):
        return pl.ds(pl.multiple_of(i * rows, 16), rows)

    def wrow(i):
        return pl.ds(pl.multiple_of(i * cols, 16), cols)

    def turn_y(k):
        return lax.rem(y + k, ny)

    def turn_x(k):
        return lax.rem(x + k, nx)

    peers = [(k, j) for k in range(ny) for j in range(nv) if k or j]

    def peer(n):
        k, j = peers[n]
        return z * ny + turn_y(k), lax.rem(v + j, nv), turn_y(k) * nv + lax.rem(v + j, nv)

    barrier = pltpu.get_barrier_semaphore()
    for k in range(1, nb):
        pl.semaphore_signal(barrier, inc=1, device_id=at(lax.rem(b + k, nb), v), device_id_type=MESH)
    met = [n for n in range(len(peers)) if peers[n][1]]
    for n in met:
        bb, vv, _ = peer(n)
        pl.semaphore_signal(barrier, inc=1, device_id=at(bb, vv), device_id_type=MESH)
    pl.semaphore_wait(barrier, nb - 1 + len(met))

    def w_z(zz, yy, up, own=False):
        i = zz * ny + yy
        dst = w_all.at[wrow(i)]
        sem = (ws_up if up else ws_dn).at[i]
        return copy(w_in.at[y] if own else dst, dst, sem, wr.at[i], b + ny if up else b - ny, v)

    def w_y(k):
        return copy(w_in.at[turn_y(k)], w_all.at[wrow(b)], ws_y.at[k - 1], wr.at[b], z * ny + turn_y(k), v)

    def w_got(zz, yy):
        w_z(zz, yy, True).wait_recv()

    has_up, has_down = z + 1 < nz, z >= 1

    def h_send(n_src, sem, bb, vv, own=False):
        dst = h_all.at[hrow(n_src)]
        return copy(h_in if own else dst, dst, sem, hr.at[n_src], bb, vv)

    def h_x(k):
        return h_send(me, hs.at[k - 1], b, turn_x(k) * 2 + core, True)

    def h_y(k):
        return h_send(me, hs.at[nx + k - 1], z * ny + turn_y(k), v, True)

    def h_xy(kx, ky):
        return h_send(y * nv + turn_x(kx) * 2 + core, hf.at[kx, ky], z * ny + turn_y(ky), v)

    def h_yx(kx, ky):
        return h_send(turn_y(ky) * nv + v, hf.at[kx, ky], b, turn_x(kx) * 2 + core)

    def h_core(kx, ky):
        i = turn_y(ky) * nv + turn_x(kx) * 2 + core
        return h_send(i, hd.at[kx, ky], b, other, kx == 0 and ky == 0)

    def h_got(kx, ky, cc):
        i = turn_y(ky) * nv + turn_x(kx) * 2 + cc
        h_send(i, hd.at[kx, ky], b, other).wait_recv()

    def code_copy(n):
        bb, vv, _ = peer(n)
        return copy(code_in, code_got.at[me], cs.at[n], cr.at[me], bb, vv)

    for k in range(1, ny):
        w_y(k).start()
    pl.when(has_up)(lambda: w_z(z, y, True, True).start())
    pl.when(has_down)(lambda: w_z(z, y, False, True).start())
    for k in range(1, nx):
        h_x(k).start()
    for k in range(1, ny):
        h_y(k).start()
    for n in range(len(peers)):
        code_copy(n).start()
    h_core(0, 0).start()
    local = [
        pltpu.make_async_copy(w_in.at[y], w_all.at[wrow(b)], own_sem.at[0]),
        pltpu.make_async_copy(h_in, h_all.at[hrow(me)], own_sem.at[1]),
    ]
    for one in local:
        one.start()

    for k in range(1, ny):
        w_got(z, turn_y(k))
        pl.when(has_up)(lambda: w_z(z, turn_y(k), True).start())
        pl.when(has_down)(lambda: w_z(z, turn_y(k), False).start())

    def h_pass():
        for kx in range(1, nx):
            h_got(kx, 0, core)
            for ky in range(1, ny):
                pl.when(core == 0)(lambda: h_xy(kx, ky).start())
            h_core(kx, 0).start()
        for ky in range(1, ny):
            h_got(0, ky, core)
            for kx in range(1, nx):
                pl.when(core == 1)(lambda: h_yx(kx, ky).start())
            h_core(0, ky).start()

    def h_rest():
        for kx in range(1, nx):
            for ky in range(1, ny):
                h_got(kx, ky, core)
                h_core(kx, ky).start()

    for k in range(1, nz):
        for j in range(ny):
            yy = turn_y(j)

            @pl.when(z - k >= 0)
            def _():
                w_got(z - k, yy)
                pl.when(has_up)(lambda: w_z(z - k, yy, True).start())

            @pl.when(z + k < nz)
            def _():
                w_got(z + k, yy)
                pl.when(has_down)(lambda: w_z(z + k, yy, False).start())
        if k == 1:
            h_pass()
        if k == min(2, nz - 1):
            h_rest()

    for one in local:
        one.wait()
    for kx in range(nx):
        for ky in range(ny):
            h_got(kx, ky, 1 - core)
    code_got[me] = code_in[...]
    for n in range(len(peers)):
        bb, vv, i = peer(n)
        copy(code_in, code_got.at[i], cs.at[n], cr.at[i], bb, vv).wait_recv()
    for i in range(group):
        code_all[i * rows:(i + 1) * rows, :] = jnp.transpose(jnp.concatenate([code_got[i]] * 16, axis=0))

    step = chunk_of(tokens, 256)
    lanes = lax.broadcasted_iota(jnp.int32, (step, 128), 1)
    first = v * entries + y * half

    def span_of(n):
        return pl.ds(pl.multiple_of(n * step, step), step)

    def hits(n):
        ids = lax.broadcasted_iota(jnp.int32, (step, half), 1) + first
        return ids == code_all[span_of(n), 0:1].astype(jnp.int32)

    for n in range(tokens // step):
        span = pl.ds(n * step, step)
        scores = jnp.dot(h_all[span, :], w_all[...], preferred_element_type=f32)
        capped = softcap * jnp.tanh(scores * (1.0 / softcap))
        logits[span, :] = capped
        total = jnp.sum(jnp.exp(capped), axis=1, keepdims=True)
        hit_sum = jnp.sum(jnp.where(hits(n), capped, 0.0), axis=1, keepdims=True)
        turned = jnp.transpose(jnp.where(lax.rem(lanes, 8) < 4, total, hit_sum))
        stat_own[:, n * step:(n + 1) * step] = turned[0:8]

    def stat_copy(n):
        bb, vv, _ = peer(n)
        return copy(stat_own, stat_all.at[me], ss.at[n], sr.at[me], bb, vv)

    for n in range(len(peers)):
        stat_copy(n).start()
    for n in range(len(peers)):
        bb, vv, i = peer(n)
        copy(stat_own, stat_all.at[i], ss.at[n], sr.at[i], bb, vv).wait_recv()
    stats = stat_own[...]
    for n in range(len(peers)):
        stats = stats + stat_all[peer(n)[2]]

    loss = jnp.zeros((1, 1), f32)
    for n in range(tokens // step):
        span = pl.ds(n * step, step)
        weight = (code_all[span, 0:1] >= 0).astype(f32)
        back = jnp.transpose(jnp.concatenate([stats[:, n * step:(n + 1) * step]] * 16, axis=0))
        partition, target_logit = back[:, 0:1], back[:, 4:5]
        loss = loss + jnp.sum(weight * (jnp.log(partition) - target_logit), axis=0, keepdims=True)
        capped = logits[span, :]
        slope = 1.0 - (capped * (1.0 / softcap)) ** 2
        delta[span, :] = ((jnp.exp(capped) * (weight / partition) - jnp.where(hits(n), weight, 0.0)) * slope
                          ).astype(bf16)
    loss_own[...] = jnp.broadcast_to(loss, loss_own.shape)

    def loss_copy(k):
        return copy(loss_own, loss_all.at[b], ls.at[k - 1], lr.at[b], lax.rem(b + k, nb), v)

    def r_copy(zz, yy):
        i = zz * ny + yy
        return copy(grad_send.at[wrow(i)], r_in.at[z, y], rs.at[i], rr.at[b], i, v)

    def grad_share(span):
        return lax.dot_general(h_all[:, span], delta[...], (((0,), (0,)), ((), ())), preferred_element_type=f32)

    slab = ny * cols
    relay = nz == 4 and slab % 128 == 0
    turn = jnp.where(z * 2 >= nz, 1, nz - 1)
    order = [lax.rem(z + turn * k, nz) for k in range(1, nz)] + [z]
    at_end = (z == 0) | (z == nz - 1)
    far = jnp.where(z * 2 >= nz, 0, nz - 1)
    near = jnp.where(z * 2 >= nz, z - 1, z + 1)

    def far_copy(yy):
        return copy(grad_send.at[wrow(far * ny + yy)], far_in.at[yy], fs.at[yy], fr.at[yy], near * ny + y, v)

    def direct(zz):
        return jnp.logical_not(at_end & (zz == far))
    if slab % 128 == 0:
        mine = y * cols
        for n in range(nz):
            zz = order[n]
            span = pl.ds(pl.multiple_of(zz * slab, 128), slab)
            share = grad_share(span)
            held = relay and n == 1
            if n == nz - 1:
                grad[...] = share
            if held:
                @pl.when(jnp.logical_not(at_end))
                def _():
                    far_own[...] = share

                @pl.when(at_end)
                def _():
                    grad_send[span, :] = share.astype(bf16)
                    for k in range(ny):
                        r_copy(zz, turn_y(k)).start()
            else:
                grad_send[span, :] = share.astype(bf16)
                for k in range(ny):
                    yy = turn_y(k)
                    if relay and n == 0:
                        pl.when(at_end)(lambda: far_copy(yy).start())
                        pl.when(jnp.logical_not(at_end))(lambda: r_copy(zz, yy).start())
                    elif n < nz - 1 or k:
                        r_copy(zz, yy).start()
    else:
        mine = b * cols
        wide = chunk_of(width, 256)

        def grad_step(j, carry):
            span = pl.ds(pl.multiple_of(j * wide, wide), wide)
            share = grad_share(span)
            grad[span, :] = share
            grad_send[span, :] = share.astype(bf16)
            return carry

        lax.fori_loop(0, width // wide, grad_step, 0)
        for n in range(nz):
            for k in range(ny):
                if n < nz - 1 or k:
                    r_copy(order[n], turn_y(k)).start()
    for k in range(1, nb):
        loss_copy(k).start()

    wide = chunk_of(width, 256)

    def part_step(j, carry):
        span = pl.ds(pl.multiple_of(j * wide, wide), wide)
        part[:, span] = lax.dot_general(
            delta[...], w_all[span, :], (((1,), (1,)), ((), ())), preferred_element_type=f32)
        return carry

    lax.fori_loop(0, width // wide, part_step, 0)

    def core_copy(kx, ky):
        i = turn_y(ky) * nv + turn_x(kx) * 2 + 1 - core
        return copy(part.at[hrow(i)], core_in.at[kx, ky], ds.at[kx, ky], dr.at[kx, ky], b, other)

    def x_copy(kx, ky):
        return copy(x_out.at[kx - 1, ky], x_in.at[kx - 1, ky], xs.at[kx, ky], xr.at[kx, ky],
                    b, turn_x(kx) * 2 + core)

    def y_copy(ky):
        return copy(y_out.at[ky - 1], y_in.at[ky - 1], ys.at[ky], yr.at[ky], z * ny + turn_y(ky), v)

    ways = [(kx % nx, ky % ny) for kx in range(1, nx + 1) for ky in range(1, ny + 1)]
    for kx, ky in ways:
        core_copy(kx, ky).start()
    hstep = 16

    def over_rows(start, body):
        def one(r, carry):
            body(pl.ds(pl.multiple_of(r * hstep, hstep), hstep),
                 pl.ds(pl.multiple_of(start + r * hstep, hstep), hstep))
            return carry

        lax.fori_loop(0, rows // hstep, one, 0)

    def start_of(kx, ky):
        return (turn_y(ky) * nv + turn_x(kx) * 2 + core) * rows

    for kx, ky in ways:
        core_copy(kx, ky).wait_recv()

        def core_sum(span, here):
            both = part[here, :] + core_in[kx, ky, span, :]
            if kx:
                x_out[kx - 1, ky, span, :] = both.astype(bf16)
            else:
                part[here, :] = both

        over_rows(start_of(kx, ky), core_sum)
        if kx:
            x_copy(kx, ky).start()

    cstep = chunk_of(cols, 64)

    def over_cols(body):
        def one(r, carry):
            body(pl.multiple_of(r * cstep, 16))
            return carry

        lax.fori_loop(0, cols // cstep, one, 0)

    if relay:
        @pl.when(jnp.logical_not(at_end))
        def _():
            for k in range(ny):
                yy = turn_y(k)
                far_copy(yy).wait_recv()

                def far_sum(r):
                    here = pl.ds(pl.multiple_of(yy * cols + r, 16), cstep)
                    there = pl.ds(pl.multiple_of((far * ny + yy) * cols + r, 16), cstep)
                    grad_send[there, :] = (far_own[here, :] + far_in[yy, pl.ds(r, cstep), :].astype(f32)).astype(bf16)

                over_cols(far_sum)
                r_copy(far, yy).start()

    for ky in [k % ny for k in range(1, ny + 1)]:
        for kx in range(1, nx):
            x_copy(kx, ky).wait_recv()

        def x_sum(span, here):
            total = part[here, :]
            for kx in range(1, nx):
                total = total + x_in[kx - 1, ky, span, :].astype(f32)
            if ky:
                y_out[ky - 1, span, :] = total.astype(bf16)
            else:
                hid_out[span, :] = total

        over_rows(start_of(0, ky), x_sum)
        if ky:
            y_copy(ky).start()

    def r_got(zz, yy):
        i = zz * ny + yy
        copy(grad_send.at[wrow(i)], r_in.at[zz, yy], rs.at[i], rr.at[i], i, v).wait_recv()

    for k in range(1, ny):
        r_got(z, turn_y(k))

    def first_sum(r):
        head_out[y, pl.ds(r, cstep), :] = grad[pl.ds(pl.multiple_of(mine + r, 16), cstep), :]
        for k in range(1, ny):
            head_out[turn_y(k), pl.ds(r, cstep), :] = r_in[z, turn_y(k), pl.ds(r, cstep), :].astype(f32)

    over_cols(first_sum)
    hops = [jnp.where(z * 2 >= nz, lax.rem(z + nz - n, nz), lax.rem(z + n, nz)) for n in range(1, nz)]
    for n in range(1, nz):
        zz = hops[n - 1]
        if n == nz - 1:
            for ky in range(1, ny):
                y_copy(ky).wait_recv()

                def y_sum(span, here):
                    hid_out[span, :] += y_in[ky - 1, span, :].astype(f32)

                over_rows(0, y_sum)

        def more_sum(r):
            for k in range(ny):
                head_out[turn_y(k), pl.ds(r, cstep), :] += r_in[zz, turn_y(k), pl.ds(r, cstep), :].astype(f32)

        def arrived():
            for k in range(ny):
                r_got(zz, turn_y(k))
            over_cols(more_sum)

        if relay:
            pl.when(direct(zz))(arrived)
        else:
            arrived()

    losses = loss_own[...]
    for k in range(1, nb):
        i = lax.rem(b + k, nb)
        copy(loss_own, loss_all.at[i], ls.at[k - 1], lr.at[i], i, v).wait_recv()
        losses = losses + loss_all[i]
    loss_out[...] = losses * (1.0 / (tokens * nb))

    for j in range(ny):
        yy = turn_y(j)
        pl.when(has_up)(lambda: w_z(z, yy, True, j == 0).wait_send())
        pl.when(has_down)(lambda: w_z(z, yy, False, j == 0).wait_send())
        for k in range(1, nz):
            @pl.when(z - k >= 0)
            def _():
                pl.when(has_up)(lambda: w_z(z - k, yy, True).wait_send())

            @pl.when(z + k < nz)
            def _():
                pl.when(has_down)(lambda: w_z(z + k, yy, False).wait_send())
    for k in range(1, ny):
        w_y(k).wait_send()
        h_y(k).wait_send()
        y_copy(k).wait_send()
    for k in range(1, nx):
        h_x(k).wait_send()
        for ky in range(1, ny):
            pl.when(core == 0)(lambda: h_xy(k, ky).wait_send())
            pl.when(core == 1)(lambda: h_yx(k, ky).wait_send())
    for kx, ky in ways:
        h_core(kx, ky).wait_send()
        core_copy(kx, ky).wait_send()
        if kx:
            x_copy(kx, ky).wait_send()
    for n in range(len(peers)):
        code_copy(n).wait_send()
        stat_copy(n).wait_send()
    for k in range(1, nb):
        loss_copy(k).wait_send()
    for n in range(nz):
        for k in range(ny):
            yy = turn_y(k)
            if relay and n == 0:
                pl.when(at_end)(lambda: far_copy(yy).wait_send())
                pl.when(jnp.logical_not(at_end))(lambda: r_copy(order[n], yy).wait_send())
            elif n < nz - 1 or k:
                r_copy(order[n], yy).wait_send()


def local(nb, nv, hidden, head_weight, targets, valid_mask):
    nx = nv // 2
    ny = nx if nx <= 2 and nb % nx == 0 else 1
    nz = nb // ny
    rows, width = hidden.shape
    entries, cols = head_weight.shape
    half = entries // ny
    group = ny * nv
    tokens = rows * group
    code = jnp.broadcast_to(jnp.where(valid_mask != 0, targets, -1).astype(f32)[None, :], (8, rows))
    weight = jnp.transpose(head_weight.reshape(ny, half, cols), (0, 2, 1))
    vm = pltpu.VMEM
    dma = pltpu.SemaphoreType.DMA
    slab = ny * cols
    ly, lx = max(ny - 1, 1), max(nx - 1, 1)
    buffers = [
        vm((tokens, width), bf16), vm((width, half), bf16), vm((group, 8, rows), f32), vm((tokens, 128), f32),
        vm((tokens, half), f32), vm((tokens, half), bf16),
        vm((8, tokens), f32), vm((group, 8, tokens), f32), vm((8, 128), f32), vm((nb, 8, 128), f32),
        vm((slab if slab % 128 == 0 else width, half), f32), vm((width, half), bf16), vm((nz, ny, cols, half), bf16),
        vm((tokens, width), f32), vm((nx, ny, rows, width), f32),
        vm((lx, ny, rows, width), bf16), vm((lx, ny, rows, width), bf16),
        vm((ly, rows, width), bf16), vm((ly, rows, width), bf16),
        vm((slab if nz == 4 else 16, half), f32), vm((ny, cols if nz == 4 else 16, half), bf16),
    ]
    sems = [
        dma((2,)), dma((nx + ny,)), dma((nx, ny)), dma((nx, ny)), dma((group,)), dma((nb,)), dma((nb,)),
        dma((ly,)), dma((nb,)), dma((group,)), dma((group,)), dma((group,)), dma((group,)), dma((nb,)), dma((nb,)),
        dma((nb,)), dma((nb,)), dma((nx, ny)), dma((nx, ny)), dma((nx, ny)), dma((nx, ny)), dma((ny,)), dma((ny,)),
        dma((ny,)), dma((ny,)),
    ]
    whole = pl.BlockSpec(memory_space=vm)
    head_t, hidden_grad, loss = pl.pallas_call(
        functools.partial(kernel, (nz, ny, nx, nv)),
        out_shape=(
            jax.ShapeDtypeStruct((ny, cols, half), f32),
            jax.ShapeDtypeStruct((rows, width), f32),
            jax.ShapeDtypeStruct((8, 128), f32),
        ),
        in_specs=[whole] * 3,
        out_specs=(whole,) * 3,
        scratch_shapes=buffers + sems,
        compiler_params=pltpu.CompilerParams(
            collective_id=0, has_side_effects=True, vmem_limit_bytes=67043328),
    )(hidden, weight, code)
    return jnp.transpose(head_t, (0, 2, 1)).reshape(entries, cols), hidden_grad, loss[0, 0]


def column_groups(width):
    units = width // 256
    sizes, left = [2], units - 2
    while left > 6:
        sizes.append(3)
        left -= 3
    while left > 0:
        take = max(1, (left + 1) // 2)
        sizes.append(take)
        left -= take
    starts = [sum(sizes[:n]) for n in range(len(sizes))]
    return [(s, n) for s, n in zip(starts, sizes)]


def plane_kernel(h_in, w_in, code_in, head_out, hid_out, loss_out, h_all, w_all, code_got, code_all,
                 logits, expo, delta, stat_own, stat_all, loss_one, loss_two, loss_all, loss_zs,
                 grad_own, held, grad_send, far_in, r_in, part, core_in, x_out, x_in, y_out, y_in, *sems):
    (own_sem, hs, hf, hd, hr, w_up, w_dn, wr, wys, cs, cr, ss, sr, ls, lr, ms, mr,
     es, er, rs, rr, fs, fr, ds, dr, xs, xr, ys, yr) = sems
    nz, ny, nv = 4, 2, 4
    nb = nz * ny
    rows, width = h_in.shape
    cols, half = w_in.shape[0], w_in.shape[1] // ny
    piece = cols // 2
    group = ny * nv
    tokens = rows * group
    slab = ny * cols
    shift, lo = cols % 128, cols - cols % 128
    win = -(-(cols + shift) // 128) * 128
    b, v = lax.axis_index("batch"), lax.axis_index("vocab")
    z, y = lax.div(b, ny), lax.rem(b, ny)
    x, core = lax.div(v, 2), lax.rem(v, 2)
    me = y * nv + v
    low = z * 2 < nz
    at_end = (z == 0) | (z == nz - 1)
    inside = jnp.logical_not(at_end)

    def flip(a, k):
        return 1 - a if k else a

    def copy(src, dst, send, recv, bb, vv):
        return pltpu.make_async_remote_copy(
            src_ref=src, dst_ref=dst, send_sem=send, recv_sem=recv,
            device_id={"batch": bb, "vocab": vv}, device_id_type=MESH)

    def hrow(i):
        return pl.ds(pl.multiple_of(i * rows, 16), rows)

    over_x, over_y, over_core = (1 - x) * 2 + core, z * ny + 1 - y, x * 2 + 1 - core
    peers = [(ky, kx, kc) for ky in range(2) for kx in range(2) for kc in range(2) if ky or kx or kc]

    def peer(n):
        ky, kx, kc = peers[n]
        yy, vv = flip(y, ky), flip(x, kx) * 2 + flip(core, kc)
        return z * ny + yy, vv, yy * nv + vv

    def z_peer(k):
        return lax.rem(z + k, nz) * ny + y

    barrier = pltpu.get_barrier_semaphore()
    for k in range(1, nz):
        pl.semaphore_signal(barrier, inc=1, device_id={"batch": z_peer(k), "vocab": v}, device_id_type=MESH)
    for n in range(len(peers)):
        bb, vv, _ = peer(n)
        pl.semaphore_signal(barrier, inc=1, device_id={"batch": bb, "vocab": vv}, device_id_type=MESH)
    pl.semaphore_wait(barrier, nz - 1 + len(peers))

    def w_ref(i, h):
        return w_all.at[pl.ds(pl.multiple_of(i * cols + h * piece, 16), piece)]

    def w_mine(yy, h):
        return w_in.at[pl.ds(h * piece, piece), pl.ds(pl.multiple_of(yy * half, 128), half)]

    def w_z(i, h, up, own=False):
        return copy(w_mine(y, h) if own else w_ref(i, h), w_ref(i, h), (w_up if up else w_dn).at[i, h],
                    wr.at[i, h], b + ny if up else b - ny, v)

    def w_pass(i, h, up):
        return copy(w_ref(i, h), w_ref(i, h), w_up.at[i, h], wr.at[i, h], jnp.where(up, b + ny, b - ny), v)

    def w_y(h):
        return copy(w_mine(1 - y, h), w_ref(b, h), wys.at[h], wr.at[b, h], over_y, v)

    def w_got(i, h):
        copy(w_ref(i, h), w_ref(i, h), wys.at[h], wr.at[i, h], over_y, v).wait_recv()

    has_up, has_down = z + 1 < nz, z >= 1
    near = z + 1 - 2 * lax.rem(z, 2)
    slabs = [z, near, jnp.where(low, 2, 1), jnp.where(low, 3, 0)]

    def h_send(i, sem, bb, vv, own=False):
        dst = h_all.at[hrow(i)]
        return copy(h_in if own else dst, dst, sem, hr.at[i], bb, vv)

    def h_x():
        return h_send(me, hs.at[0], b, over_x, True)

    def h_y():
        return h_send(me, hs.at[1], over_y, v, True)

    def h_xy():
        return h_send(y * nv + over_x, hf.at[0], over_y, v)

    def h_yx():
        return h_send((1 - y) * nv + v, hf.at[0], b, over_x)

    def h_core(kx, ky):
        i = flip(y, ky) * nv + flip(x, kx) * 2 + core
        return h_send(i, hd.at[kx, ky], b, over_core, kx == 0 and ky == 0)

    def h_got(kx, ky, cc):
        i = flip(y, ky) * nv + flip(x, kx) * 2 + cc
        h_send(i, hd.at[kx, ky], b, over_core).wait_recv()

    def code_copy(n):
        bb, vv, _ = peer(n)
        return copy(code_in, code_got.at[me], cs.at[n], cr.at[me], bb, vv)

    for h in range(2):
        w_y(h).start()
    for h in range(2):
        pl.when(has_up)(lambda: w_z(b, h, True, True).start())
        pl.when(has_down)(lambda: w_z(b, h, False, True).start())
    h_x().start()
    h_y().start()
    for n in range(len(peers)):
        code_copy(n).start()
    h_core(0, 0).start()
    local = [pltpu.make_async_copy(w_mine(y, h), w_ref(b, h), own_sem.at[h]) for h in range(2)]
    local.append(pltpu.make_async_copy(h_in, h_all.at[hrow(me)], own_sem.at[2]))
    for one in local:
        one.start()

    for h in range(2):
        i = z * ny + 1 - y
        w_got(i, h)
        pl.when(has_up)(lambda: w_z(i, h, True).start())
        pl.when(has_down)(lambda: w_z(i, h, False).start())

    def w_slab(zz, onward):
        for k in range(ny):
            for h in range(2):
                i = zz * ny + flip(y, k)
                w_got(i, h)
                if onward:
                    w_pass(i, h, zz < z).start()

    @pl.when(at_end)
    def _():
        w_slab(slabs[1], False)

    @pl.when(inside)
    def _():
        w_slab(slabs[1], True)
        w_slab(slabs[2], True)

    h_got(1, 0, core)
    pl.when(core == 0)(lambda: h_xy().start())
    h_core(1, 0).start()
    h_got(0, 1, core)
    pl.when(core == 1)(lambda: h_yx().start())
    h_core(0, 1).start()

    @pl.when(at_end)
    def _():
        w_slab(slabs[2], False)

    @pl.when(inside)
    def _():
        w_slab(slabs[3], True)

    for one in local:
        one.wait()
    code_got[me] = code_in[...]
    for n in range(len(peers)):
        bb, vv, i = peer(n)
        copy(code_in, code_got.at[i], cs.at[n], cr.at[i], bb, vv).wait_recv()
    for i in range(group):
        code_all[i * rows:(i + 1) * rows, :] = jnp.transpose(jnp.concatenate([code_got[i]] * (rows // 8), axis=0))

    h_got(1, 1, core)
    h_core(1, 1).start()
    for kx in range(2):
        for ky in range(2):
            h_got(kx, ky, 1 - core)

    step = 2 * rows
    steps = tokens // step
    lines = lax.broadcasted_iota(jnp.int32, (8, rows), 0)

    def scores(n, zz):
        here = pl.ds(pl.multiple_of(zz * slab, 128), slab)
        there = pl.ds(pl.multiple_of(zz * slab, 16), slab)
        return jnp.dot(h_all[n * step:(n + 1) * step, here], w_all[there, :], preferred_element_type=f32)

    for j in range(nz - 1):
        for n in range(steps):
            span = pl.ds(n * step, step)
            if j:
                logits[span, :] += scores(n, slabs[j])
            else:
                logits[span, :] = scores(n, slabs[j])

    pl.when(at_end)(lambda: w_slab(slabs[3], False))

    sums = jnp.zeros((8, rows), f32)
    for n in range(steps):
        span = pl.ds(n * step, step)
        capped = softcap * jnp.tanh((logits[span, :] + scores(n, slabs[nz - 1])) * (1.0 / softcap))
        raised = jnp.exp(capped)
        logits[span, :] = capped
        expo[span, :] = raised
        total = jnp.broadcast_to(jnp.sum(raised, axis=1, keepdims=True), (step, 128))
        for k in range(2):
            turned = jnp.transpose(total[k * rows:(k + 1) * rows])
            sums = jnp.where(lines == 2 * n + k, turned[0:8], sums)
    stat_own[...] = sums

    def stat_copy(n):
        bb, vv, _ = peer(n)
        return copy(stat_own, stat_all.at[me], ss.at[n], sr.at[me], bb, vv)

    for n in range(len(peers)):
        stat_copy(n).start()

    ids = (lax.broadcasted_iota(jnp.int32, (step, half), 1) + (v * ny + y) * half).astype(f32)
    hit_total = jnp.zeros((step, 1), f32)
    for n in range(steps):
        span = pl.ds(n * step, step)
        capped = logits[span, :]
        hit = ids == code_all[span, 0:1]
        slope = 1.0 - (capped * (1.0 / softcap)) ** 2
        expo[span, :] = expo[span, :] * slope
        logits[span, :] = jnp.where(hit, slope, 0.0)
        hit_total = hit_total + jnp.sum(jnp.where(hit, capped, 0.0), axis=1, keepdims=True)
    hit_total = jnp.sum(hit_total, axis=0, keepdims=True)
    code_rows = jnp.zeros((8, rows), f32)
    for i in range(group):
        code_rows = jnp.where(lines == i, code_got[i], code_rows)
    weight = (code_rows >= 0).astype(f32)

    stat_all[me] = sums
    for n in range(len(peers)):
        bb, vv, i = peer(n)
        copy(stat_own, stat_all.at[i], ss.at[n], sr.at[i], bb, vv).wait_recv()
    partition = stat_all[0]
    for i in range(1, group):
        partition = partition + stat_all[i]
    scale = weight / partition

    def delta_copy(n):
        span = pl.ds(n * step, step)
        return copy(delta.at[0, span], delta.at[1, span], es.at[n], er.at[n], over_y, v)

    for n in range(steps):
        for k in range(2):
            i = 2 * n + k
            span = pl.ds(i * rows, rows)
            by_row = jnp.transpose(jnp.broadcast_to(scale[i:i + 1, :], (rows, rows)))
            factor = jnp.concatenate([by_row] * (half // rows), axis=1)
            delta[0, span, :] = (expo[span, :] * factor - logits[span, :]).astype(bf16)
        delta_copy(n).start()

    share_loss = jnp.sum(weight * jnp.log(partition), axis=1, keepdims=True)
    loss = jnp.sum(share_loss, axis=0, keepdims=True) * (1.0 / group) - hit_total
    loss_one[...] = jnp.broadcast_to(loss, loss_one.shape)

    def loss_copy(n):
        bb, vv, _ = peer(n)
        return copy(loss_one, loss_all.at[me], ls.at[n], lr.at[me], bb, vv)

    near_end = jnp.where(low, 1, 2)
    far = jnp.where(low, nz - 1, 0)
    targets = [jnp.where(lax.rem(z, 2) == 0, nz - 1, 0), jnp.where(low, 2, 1),
               jnp.where(at_end, near_end, far), z]
    top = y * shift

    def grad_share(zz, r):
        here = pl.ds(pl.multiple_of(zz * slab + y * lo, 128), win)
        return lax.dot_general(h_all[:, here], delta[r], (((0,), (0,)), ((), ())), preferred_element_type=f32)

    def sent(k, r):
        return grad_send.at[k, r, pl.ds(pl.multiple_of(top, 16), cols)]

    def r_copy(k, r):
        return copy(sent(k, r), r_in.at[z, r], rs.at[k, r], rr.at[z, r], targets[k] * ny + y, v)

    def far_copy(r):
        return copy(sent(0, r), far_in.at[r], fs.at[r], fr.at[r], near_end * ny + y, v)

    def head_piece(k, r):
        share = grad_share(targets[k], r)
        if k == nz - 1:
            grad_own[r] = share
        elif k == 2:
            @pl.when(at_end)
            def _():
                grad_send[k, r] = share.astype(bf16)
                r_copy(k, r).start()

            @pl.when(inside)
            def _():
                held[r] = share
        else:
            grad_send[k, r] = share.astype(bf16)
            if k == 0:
                pl.when(at_end)(lambda: far_copy(r).start())
                pl.when(inside)(lambda: r_copy(k, r).start())
            else:
                r_copy(k, r).start()

    cstep = chunk_of(cols, 64)

    def over_cols(body):
        def one(n, carry):
            body(pl.multiple_of(n * cstep, 16))
            return carry

        lax.fori_loop(0, cols // cstep, one, 0)

    def relay(r):
        @pl.when(inside)
        def _():
            far_copy(r).wait_recv()

            def add(n):
                here = pl.ds(pl.multiple_of(top + n, 16), cstep)
                grad_send[2, r, here, :] = (held[r, here, :] + far_in[r, pl.ds(n, cstep), :].astype(f32)).astype(bf16)

            over_cols(add)
            r_copy(2, r).start()

    groups = column_groups(width)
    blocks = [(1, 1), (1, 0), (0, 1), (0, 0)]
    unit = width // (width // 256)

    def span_of(g):
        first, n = groups[g]
        return pl.ds(first * unit, n * unit)

    def block(kx, ky, cc):
        return flip(y, ky) * nv + flip(x, kx) * 2 + cc

    def core_copy(g, kx, ky):
        return copy(part.at[hrow(block(kx, ky, 1 - core)), span_of(g)], core_in.at[kx, ky, :, span_of(g)],
                    ds.at[g, kx, ky], dr.at[g, kx, ky], b, over_core)

    def x_copy(g, ky):
        return copy(x_out.at[ky, :, span_of(g)], x_in.at[ky, :, span_of(g)], xs.at[g, ky], xr.at[g, ky], b, over_x)

    def y_copy(g):
        return copy(y_out.at[:, span_of(g)], y_in.at[:, span_of(g)], ys.at[g], yr.at[g], over_y, v)

    def part_group(g):
        first, n = groups[g]

        def one(j, carry):
            span = pl.ds(pl.multiple_of(j * unit, 128), unit)
            part[:, span] = lax.dot_general(
                delta[0], w_all[span, :], (((1,), (1,)), ((), ())), preferred_element_type=f32)
            return carry

        lax.fori_loop(first, first + n, one, 0)
        for kx, ky in blocks:
            core_copy(g, kx, ky).start()

    hstep = 16

    def over_rows(body):
        def one(n, carry):
            body(pl.multiple_of(n * hstep, hstep))
            return carry

        lax.fori_loop(0, rows // hstep, one, 0)

    def core_sum(g):
        span = span_of(g)
        for kx, ky in blocks:
            core_copy(g, kx, ky).wait_recv()
            start = block(kx, ky, core) * rows

            def add(n):
                here = pl.ds(pl.multiple_of(start + n, hstep), hstep)
                both = part[here, span] + core_in[kx, ky, pl.ds(n, hstep), span]
                if kx:
                    x_out[ky, pl.ds(n, hstep), span] = both.astype(bf16)
                else:
                    part[here, span] = both

            over_rows(add)
            if kx:
                x_copy(g, ky).start()

    def x_sum(g):
        span = span_of(g)
        for ky in (1, 0):
            x_copy(g, ky).wait_recv()
            start = block(0, ky, core) * rows

            def add(n):
                here = pl.ds(pl.multiple_of(start + n, hstep), hstep)
                total = part[here, span] + x_in[ky, pl.ds(n, hstep), span].astype(f32)
                if ky:
                    y_out[pl.ds(n, hstep), span] = total.astype(bf16)
                else:
                    hid_out[pl.ds(n, hstep), span] = total

            over_rows(add)
            if ky:
                y_copy(g).start()

    def y_sum(g):
        span = span_of(g)
        y_copy(g).wait_recv()

        def add(n):
            here = pl.ds(n, hstep)
            hid_out[here, span] += y_in[here, span].astype(f32)

        over_rows(add)

    count = len(groups)
    head_piece(0, 0)
    part_group(0)
    head_piece(1, 0)
    part_group(1)
    for n in range(len(peers)):
        loss_copy(n).start()
    core_sum(0)
    head_piece(2, 0)
    for g in range(2, count):
        part_group(g)
        core_sum(g - 1)
        if g == 3:
            relay(0)
    core_sum(count - 1)
    head_piece(3, 0)

    loss_all[me] = loss_one[...]
    for n in range(len(peers)):
        bb, vv, i = peer(n)
        copy(loss_one, loss_all.at[i], ls.at[n], lr.at[i], bb, vv).wait_recv()
    losses = loss_all[0]
    for i in range(1, group):
        losses = losses + loss_all[i]
    loss_two[...] = losses

    def plane_copy(k):
        return copy(loss_two, loss_zs.at[z], ms.at[k - 1], mr.at[z], z_peer(k), v)

    for k in range(1, nz):
        plane_copy(k).start()

    x_sum(0)
    for n in range(steps):
        delta_copy(n).wait_recv()
    for k in range(nz):
        head_piece(k, 1)
        if k == 1:
            x_sum(1)
    x_sum(2)
    relay(1)
    for g in range(3, count):
        x_sum(g)
        y_sum(g - 3)

    def r_got(zz, r):
        copy(r_in.at[zz, r], r_in.at[zz, r], rs.at[0, r], rr.at[zz, r], z_peer(1), v).wait_recv()

    def lanes(r):
        return pl.ds(pl.multiple_of(flip(y, r) * half, 128), half)

    sources = [near, jnp.where(low, 2, 1), far]

    def head_sum(r):
        for k in range(2):
            r_got(sources[k], r)

        def add(n):
            here = pl.ds(n, cstep)
            total = grad_own[r, pl.ds(pl.multiple_of(top + n, 16), cstep), :]
            for k in range(2):
                total = total + r_in[sources[k], r, here, :].astype(f32)
            head_out[here, lanes(r)] = total

        over_cols(add)

        @pl.when(inside)
        def _():
            r_got(sources[2], r)

            def last(n):
                here = pl.ds(n, cstep)
                head_out[here, lanes(r)] += r_in[sources[2], r, here, :].astype(f32)

            over_cols(last)

    head_sum(0)
    y_sum(count - 3)
    y_sum(count - 2)
    loss_zs[z] = loss_two[...]
    for k in range(1, nz):
        i = lax.rem(z + k, nz)
        copy(loss_two, loss_zs.at[i], ms.at[k - 1], mr.at[i], z_peer(k), v).wait_recv()
    losses = loss_zs[0]
    for i in range(1, nz):
        losses = losses + loss_zs[i]
    loss_out[...] = losses * (1.0 / (tokens * nz))
    y_sum(count - 1)
    head_sum(1)

    for h in range(2):
        w_y(h).wait_send()
        pl.when(has_up)(lambda: w_z(b, h, True, True).wait_send())
        pl.when(has_down)(lambda: w_z(b, h, False, True).wait_send())
        pl.when(has_up)(lambda: w_z(z * ny + 1 - y, h, True).wait_send())
        pl.when(has_down)(lambda: w_z(z * ny + 1 - y, h, False).wait_send())

    @pl.when(inside)
    def _():
        for j in range(1, nz):
            for k in range(ny):
                for h in range(2):
                    w_pass(slabs[j] * ny + flip(y, k), h, slabs[j] < z).wait_send()

    h_x().wait_send()
    h_y().wait_send()
    pl.when(core == 0)(lambda: h_xy().wait_send())
    pl.when(core == 1)(lambda: h_yx().wait_send())
    for kx, ky in blocks:
        h_core(kx, ky).wait_send()
    for n in range(len(peers)):
        code_copy(n).wait_send()
        stat_copy(n).wait_send()
        loss_copy(n).wait_send()
    for k in range(1, nz):
        plane_copy(k).wait_send()
    for n in range(steps):
        delta_copy(n).wait_send()
    for r in range(2):
        pl.when(at_end)(lambda: far_copy(r).wait_send())
        pl.when(inside)(lambda: r_copy(0, r).wait_send())
        r_copy(1, r).wait_send()
        r_copy(2, r).wait_send()
    for g in range(count):
        for kx, ky in blocks:
            core_copy(g, kx, ky).wait_send()
        for ky in range(2):
            x_copy(g, ky).wait_send()
        y_copy(g).wait_send()


def plane_local(hidden, head_weight, targets, valid_mask):
    nz, ny, nv = 4, 2, 4
    rows, width = hidden.shape
    entries, cols = head_weight.shape
    half = entries // ny
    group = ny * nv
    tokens = rows * group
    shift = cols % 128
    win = -(-(cols + shift) // 128) * 128
    code = jnp.broadcast_to(jnp.where(valid_mask != 0, targets, -1).astype(f32)[None, :], (8, rows))
    vm = pltpu.VMEM
    dma = pltpu.SemaphoreType.DMA
    count = len(column_groups(width))
    line = vm((8, rows), f32)
    buffers = [
        vm((tokens, width), bf16), vm((width, half), bf16), vm((group, 8, rows), f32), vm((tokens, 128), f32),
        vm((tokens, half), f32), vm((tokens, half), f32), vm((2, tokens, half), bf16),
        line, vm((group, 8, rows), f32), line, line, vm((group, 8, rows), f32), vm((nz, 8, rows), f32),
        vm((2, win, half), f32), vm((2, win, half), f32), vm((3, 2, win, half), bf16),
        vm((2, cols, half), bf16), vm((nz, 2, cols, half), bf16),
        vm((tokens, width), f32), vm((2, 2, rows, width), f32),
        vm((2, rows, width), bf16), vm((2, rows, width), bf16), vm((rows, width), bf16), vm((rows, width), bf16),
    ]
    sems = [
        dma((3,)), dma((2,)), dma((1,)), dma((2, 2)), dma((group,)), dma((8, 2)), dma((8, 2)), dma((8, 2)), dma((2,)),
        dma((7,)), dma((group,)), dma((7,)), dma((group,)), dma((7,)), dma((group,)), dma((3,)), dma((nz,)),
        dma((4,)), dma((4,)), dma((3, 2)), dma((nz, 2)), dma((2,)), dma((2,)),
        dma((count, 2, 2)), dma((count, 2, 2)), dma((count, 2)), dma((count, 2)), dma((count,)), dma((count,)),
    ]
    whole = pl.BlockSpec(memory_space=vm)
    head_t, hidden_grad, loss = pl.pallas_call(
        plane_kernel,
        out_shape=(
            jax.ShapeDtypeStruct((cols, entries), f32),
            jax.ShapeDtypeStruct((rows, width), f32),
            jax.ShapeDtypeStruct((8, rows), f32),
        ),
        in_specs=[whole] * 3,
        out_specs=(whole,) * 3,
        scratch_shapes=buffers + sems,
        compiler_params=pltpu.CompilerParams(
            collective_id=1, has_side_effects=True, vmem_limit_bytes=67043328),
    )(hidden, jnp.transpose(head_weight), code)
    return jnp.transpose(head_t), hidden_grad, loss[0, 0]


def in_planes(nb, nv, hidden, head_weight, targets, valid_mask):
    rows, width = hidden.shape
    entries, cols = head_weight.shape
    fits = nb == 8 and nv == 4 and rows == 128 and width % 256 == 0 and width >= 2048
    return fits and entries % 256 == 0 and cols % 32 == 0 and (2 * cols) % 128 == 0


def device(nb, nv, *arrays):
    if in_planes(nb, nv, *arrays):
        return plane_local(*arrays)
    return local(nb, nv, *arrays)


def solution(mesh):
    placed = (
        P(("batch", "vocab"), None),
        P("vocab", "batch"),
        P(("batch", "vocab")),
        P(("batch", "vocab")),
    )
    return jax.shard_map(
        functools.partial(device, mesh.shape["batch"], mesh.shape["vocab"]),
        mesh=mesh,
        in_specs=placed,
        out_specs=(P("vocab", "batch"), P(("batch", "vocab"), None), P()),
        check_vma=False,
    )
```

```python
import functools

import jax
import jax.numpy as jnp
from jax import lax
from jax.experimental import pallas as pl
from jax.experimental.pallas import tpu as pltpu
from jax.sharding import PartitionSpec as P

softcap = 30.0
MESH = pl.DeviceIdType.MESH
f32, bf16 = jnp.float32, jnp.bfloat16


def chunk_of(length, most):
    return max(s for s in range(16, most + 1, 16) if length % s == 0)


def kernel(sizes, h_in, w_in, code_in, head_out, hid_out, loss_out, h_all, w_all, code_got, code_all,
           logits, delta, stat_own, stat_all, loss_own, loss_all, grad, grad_send, r_in,
           part, core_in, x_out, x_in, y_out, y_in, far_own, far_in, *sems):
    nz, ny, nx, nv = sizes
    (own_sem, hs, hf, hd, hr, ws_up, ws_dn, ws_y, wr, cs, cr, ss, sr, ls, lr,
     rs, rr, ds, dr, xs, xr, ys, yr, fs, fr) = sems
    nb = nz * ny
    rows, width = h_in.shape
    cols, half = w_in.shape[1:]
    group = ny * nv
    tokens = rows * group
    entries = ny * half
    b, v = lax.axis_index("batch"), lax.axis_index("vocab")
    z, y = lax.div(b, ny), lax.rem(b, ny)
    x, core = lax.div(v, 2), lax.rem(v, 2)
    other = x * 2 + 1 - core
    me = y * nv + v

    def at(bb, vv):
        return {"batch": bb, "vocab": vv}

    def copy(src, dst, send, recv, bb, vv):
        return pltpu.make_async_remote_copy(
            src_ref=src, dst_ref=dst, send_sem=send, recv_sem=recv, device_id=at(bb, vv), device_id_type=MESH)

    def hrow(i):
        return pl.ds(pl.multiple_of(i * rows, 16), rows)

    def wrow(i):
        return pl.ds(pl.multiple_of(i * cols, 16), cols)

    def turn_y(k):
        return lax.rem(y + k, ny)

    def turn_x(k):
        return lax.rem(x + k, nx)

    peers = [(k, j) for k in range(ny) for j in range(nv) if k or j]

    def peer(n):
        k, j = peers[n]
        return z * ny + turn_y(k), lax.rem(v + j, nv), turn_y(k) * nv + lax.rem(v + j, nv)

    barrier = pltpu.get_barrier_semaphore()
    for k in range(1, nb):
        pl.semaphore_signal(barrier, inc=1, device_id=at(lax.rem(b + k, nb), v), device_id_type=MESH)
    met = [n for n in range(len(peers)) if peers[n][1]]
    for n in met:
        bb, vv, _ = peer(n)
        pl.semaphore_signal(barrier, inc=1, device_id=at(bb, vv), device_id_type=MESH)
    pl.semaphore_wait(barrier, nb - 1 + len(met))

    def w_z(zz, yy, up, own=False):
        i = zz * ny + yy
        dst = w_all.at[wrow(i)]
        sem = (ws_up if up else ws_dn).at[i]
        return copy(w_in.at[y] if own else dst, dst, sem, wr.at[i], b + ny if up else b - ny, v)

    def w_y(k):
        return copy(w_in.at[turn_y(k)], w_all.at[wrow(b)], ws_y.at[k - 1], wr.at[b], z * ny + turn_y(k), v)

    def w_got(zz, yy):
        w_z(zz, yy, True).wait_recv()

    has_up, has_down = z + 1 < nz, z >= 1

    def h_send(n_src, sem, bb, vv, own=False):
        dst = h_all.at[hrow(n_src)]
        return copy(h_in if own else dst, dst, sem, hr.at[n_src], bb, vv)

    def h_x(k):
        return h_send(me, hs.at[k - 1], b, turn_x(k) * 2 + core, True)

    def h_y(k):
        return h_send(me, hs.at[nx + k - 1], z * ny + turn_y(k), v, True)

    def h_xy(kx, ky):
        return h_send(y * nv + turn_x(kx) * 2 + core, hf.at[kx, ky], z * ny + turn_y(ky), v)

    def h_yx(kx, ky):
        return h_send(turn_y(ky) * nv + v, hf.at[kx, ky], b, turn_x(kx) * 2 + core)

    def h_core(kx, ky):
        i = turn_y(ky) * nv + turn_x(kx) * 2 + core
        return h_send(i, hd.at[kx, ky], b, other, kx == 0 and ky == 0)

    def h_got(kx, ky, cc):
        i = turn_y(ky) * nv + turn_x(kx) * 2 + cc
        h_send(i, hd.at[kx, ky], b, other).wait_recv()

    def code_copy(n):
        bb, vv, _ = peer(n)
        return copy(code_in, code_got.at[me], cs.at[n], cr.at[me], bb, vv)

    for k in range(1, ny):
        w_y(k).start()
    pl.when(has_up)(lambda: w_z(z, y, True, True).start())
    pl.when(has_down)(lambda: w_z(z, y, False, True).start())
    for k in range(1, nx):
        h_x(k).start()
    for k in range(1, ny):
        h_y(k).start()
    for n in range(len(peers)):
        code_copy(n).start()
    h_core(0, 0).start()
    local = [
        pltpu.make_async_copy(w_in.at[y], w_all.at[wrow(b)], own_sem.at[0]),
        pltpu.make_async_copy(h_in, h_all.at[hrow(me)], own_sem.at[1]),
    ]
    for one in local:
        one.start()

    for k in range(1, ny):
        w_got(z, turn_y(k))
        pl.when(has_up)(lambda: w_z(z, turn_y(k), True).start())
        pl.when(has_down)(lambda: w_z(z, turn_y(k), False).start())

    def h_pass():
        for kx in range(1, nx):
            h_got(kx, 0, core)
            for ky in range(1, ny):
                pl.when(core == 0)(lambda: h_xy(kx, ky).start())
            h_core(kx, 0).start()
        for ky in range(1, ny):
            h_got(0, ky, core)
            for kx in range(1, nx):
                pl.when(core == 1)(lambda: h_yx(kx, ky).start())
            h_core(0, ky).start()

    def h_rest():
        for kx in range(1, nx):
            for ky in range(1, ny):
                h_got(kx, ky, core)
                h_core(kx, ky).start()

    for k in range(1, nz):
        for j in range(ny):
            yy = turn_y(j)

            @pl.when(z - k >= 0)
            def _():
                w_got(z - k, yy)
                pl.when(has_up)(lambda: w_z(z - k, yy, True).start())

            @pl.when(z + k < nz)
            def _():
                w_got(z + k, yy)
                pl.when(has_down)(lambda: w_z(z + k, yy, False).start())
        if k == 1:
            h_pass()
        if k == min(2, nz - 1):
            h_rest()

    for one in local:
        one.wait()
    for kx in range(nx):
        for ky in range(ny):
            h_got(kx, ky, 1 - core)
    code_got[me] = code_in[...]
    for n in range(len(peers)):
        bb, vv, i = peer(n)
        copy(code_in, code_got.at[i], cs.at[n], cr.at[i], bb, vv).wait_recv()
    for i in range(group):
        code_all[i * rows:(i + 1) * rows, :] = jnp.transpose(jnp.concatenate([code_got[i]] * 16, axis=0))

    step = chunk_of(tokens, 256)
    lanes = lax.broadcasted_iota(jnp.int32, (step, 128), 1)
    first = v * entries + y * half

    def span_of(n):
        return pl.ds(pl.multiple_of(n * step, step), step)

    def hits(n):
        ids = lax.broadcasted_iota(jnp.int32, (step, half), 1) + first
        return ids == code_all[span_of(n), 0:1].astype(jnp.int32)

    for n in range(tokens // step):
        span = pl.ds(n * step, step)
        scores = jnp.dot(h_all[span, :], w_all[...], preferred_element_type=f32)
        capped = softcap * jnp.tanh(scores * (1.0 / softcap))
        logits[span, :] = capped
        total = jnp.sum(jnp.exp(capped), axis=1, keepdims=True)
        hit_sum = jnp.sum(jnp.where(hits(n), capped, 0.0), axis=1, keepdims=True)
        turned = jnp.transpose(jnp.where(lax.rem(lanes, 8) < 4, total, hit_sum))
        stat_own[:, n * step:(n + 1) * step] = turned[0:8]

    def stat_copy(n):
        bb, vv, _ = peer(n)
        return copy(stat_own, stat_all.at[me], ss.at[n], sr.at[me], bb, vv)

    for n in range(len(peers)):
        stat_copy(n).start()
    for n in range(len(peers)):
        bb, vv, i = peer(n)
        copy(stat_own, stat_all.at[i], ss.at[n], sr.at[i], bb, vv).wait_recv()
    stats = stat_own[...]
    for n in range(len(peers)):
        stats = stats + stat_all[peer(n)[2]]

    loss = jnp.zeros((1, 1), f32)
    for n in range(tokens // step):
        span = pl.ds(n * step, step)
        weight = (code_all[span, 0:1] >= 0).astype(f32)
        back = jnp.transpose(jnp.concatenate([stats[:, n * step:(n + 1) * step]] * 16, axis=0))
        partition, target_logit = back[:, 0:1], back[:, 4:5]
        loss = loss + jnp.sum(weight * (jnp.log(partition) - target_logit), axis=0, keepdims=True)
        capped = logits[span, :]
        slope = 1.0 - (capped * (1.0 / softcap)) ** 2
        delta[span, :] = ((jnp.exp(capped) * (weight / partition) - jnp.where(hits(n), weight, 0.0)) * slope
                          ).astype(bf16)
    loss_own[...] = jnp.broadcast_to(loss, loss_own.shape)

    def loss_copy(k):
        return copy(loss_own, loss_all.at[b], ls.at[k - 1], lr.at[b], lax.rem(b + k, nb), v)

    def r_copy(zz, yy):
        i = zz * ny + yy
        return copy(grad_send.at[wrow(i)], r_in.at[z, y], rs.at[i], rr.at[b], i, v)

    def grad_share(span):
        return lax.dot_general(h_all[:, span], delta[...], (((0,), (0,)), ((), ())), preferred_element_type=f32)

    slab = ny * cols
    relay = nz == 4 and slab % 128 == 0
    turn = jnp.where(z * 2 >= nz, 1, nz - 1)
    order = [lax.rem(z + turn * k, nz) for k in range(1, nz)] + [z]
    at_end = (z == 0) | (z == nz - 1)
    far = jnp.where(z * 2 >= nz, 0, nz - 1)
    near = jnp.where(z * 2 >= nz, z - 1, z + 1)

    def far_copy(yy):
        return copy(grad_send.at[wrow(far * ny + yy)], far_in.at[yy], fs.at[yy], fr.at[yy], near * ny + y, v)

    def direct(zz):
        return jnp.logical_not(at_end & (zz == far))
    if slab % 128 == 0:
        mine = y * cols
        for n in range(nz):
            zz = order[n]
            span = pl.ds(pl.multiple_of(zz * slab, 128), slab)
            share = grad_share(span)
            held = relay and n == 1
            if n == nz - 1:
                grad[...] = share
            if held:
                @pl.when(jnp.logical_not(at_end))
                def _():
                    far_own[...] = share

                @pl.when(at_end)
                def _():
                    grad_send[span, :] = share.astype(bf16)
                    for k in range(ny):
                        r_copy(zz, turn_y(k)).start()
            else:
                grad_send[span, :] = share.astype(bf16)
                for k in range(ny):
                    yy = turn_y(k)
                    if relay and n == 0:
                        pl.when(at_end)(lambda: far_copy(yy).start())
                        pl.when(jnp.logical_not(at_end))(lambda: r_copy(zz, yy).start())
                    elif n < nz - 1 or k:
                        r_copy(zz, yy).start()
    else:
        mine = b * cols
        wide = chunk_of(width, 256)

        def grad_step(j, carry):
            span = pl.ds(pl.multiple_of(j * wide, wide), wide)
            share = grad_share(span)
            grad[span, :] = share
            grad_send[span, :] = share.astype(bf16)
            return carry

        lax.fori_loop(0, width // wide, grad_step, 0)
        for n in range(nz):
            for k in range(ny):
                if n < nz - 1 or k:
                    r_copy(order[n], turn_y(k)).start()
    for k in range(1, nb):
        loss_copy(k).start()

    wide = chunk_of(width, 256)

    def part_step(j, carry):
        span = pl.ds(pl.multiple_of(j * wide, wide), wide)
        part[:, span] = lax.dot_general(
            delta[...], w_all[span, :], (((1,), (1,)), ((), ())), preferred_element_type=f32)
        return carry

    lax.fori_loop(0, width // wide, part_step, 0)

    def core_copy(kx, ky):
        i = turn_y(ky) * nv + turn_x(kx) * 2 + 1 - core
        return copy(part.at[hrow(i)], core_in.at[kx, ky], ds.at[kx, ky], dr.at[kx, ky], b, other)

    def x_copy(kx, ky):
        return copy(x_out.at[kx - 1, ky], x_in.at[kx - 1, ky], xs.at[kx, ky], xr.at[kx, ky],
                    b, turn_x(kx) * 2 + core)

    def y_copy(ky):
        return copy(y_out.at[ky - 1], y_in.at[ky - 1], ys.at[ky], yr.at[ky], z * ny + turn_y(ky), v)

    ways = [(kx % nx, ky % ny) for kx in range(1, nx + 1) for ky in range(1, ny + 1)]
    for kx, ky in ways:
        core_copy(kx, ky).start()
    hstep = 16

    def over_rows(start, body):
        def one(r, carry):
            body(pl.ds(pl.multiple_of(r * hstep, hstep), hstep),
                 pl.ds(pl.multiple_of(start + r * hstep, hstep), hstep))
            return carry

        lax.fori_loop(0, rows // hstep, one, 0)

    def start_of(kx, ky):
        return (turn_y(ky) * nv + turn_x(kx) * 2 + core) * rows

    for kx, ky in ways:
        core_copy(kx, ky).wait_recv()

        def core_sum(span, here):
            both = part[here, :] + core_in[kx, ky, span, :]
            if kx:
                x_out[kx - 1, ky, span, :] = both.astype(bf16)
            else:
                part[here, :] = both

        over_rows(start_of(kx, ky), core_sum)
        if kx:
            x_copy(kx, ky).start()

    cstep = chunk_of(cols, 64)

    def over_cols(body):
        def one(r, carry):
            body(pl.multiple_of(r * cstep, 16))
            return carry

        lax.fori_loop(0, cols // cstep, one, 0)

    if relay:
        @pl.when(jnp.logical_not(at_end))
        def _():
            for k in range(ny):
                yy = turn_y(k)
                far_copy(yy).wait_recv()

                def far_sum(r):
                    here = pl.ds(pl.multiple_of(yy * cols + r, 16), cstep)
                    there = pl.ds(pl.multiple_of((far * ny + yy) * cols + r, 16), cstep)
                    grad_send[there, :] = (far_own[here, :] + far_in[yy, pl.ds(r, cstep), :].astype(f32)).astype(bf16)

                over_cols(far_sum)
                r_copy(far, yy).start()

    for ky in [k % ny for k in range(1, ny + 1)]:
        for kx in range(1, nx):
            x_copy(kx, ky).wait_recv()

        def x_sum(span, here):
            total = part[here, :]
            for kx in range(1, nx):
                total = total + x_in[kx - 1, ky, span, :].astype(f32)
            if ky:
                y_out[ky - 1, span, :] = total.astype(bf16)
            else:
                hid_out[span, :] = total

        over_rows(start_of(0, ky), x_sum)
        if ky:
            y_copy(ky).start()

    def r_got(zz, yy):
        i = zz * ny + yy
        copy(grad_send.at[wrow(i)], r_in.at[zz, yy], rs.at[i], rr.at[i], i, v).wait_recv()

    for k in range(1, ny):
        r_got(z, turn_y(k))

    def first_sum(r):
        head_out[y, pl.ds(r, cstep), :] = grad[pl.ds(pl.multiple_of(mine + r, 16), cstep), :]
        for k in range(1, ny):
            head_out[turn_y(k), pl.ds(r, cstep), :] = r_in[z, turn_y(k), pl.ds(r, cstep), :].astype(f32)

    over_cols(first_sum)
    hops = [jnp.where(z * 2 >= nz, lax.rem(z + nz - n, nz), lax.rem(z + n, nz)) for n in range(1, nz)]
    for n in range(1, nz):
        zz = hops[n - 1]
        if n == nz - 1:
            for ky in range(1, ny):
                y_copy(ky).wait_recv()

                def y_sum(span, here):
                    hid_out[span, :] += y_in[ky - 1, span, :].astype(f32)

                over_rows(0, y_sum)

        def more_sum(r):
            for k in range(ny):
                head_out[turn_y(k), pl.ds(r, cstep), :] += r_in[zz, turn_y(k), pl.ds(r, cstep), :].astype(f32)

        def arrived():
            for k in range(ny):
                r_got(zz, turn_y(k))
            over_cols(more_sum)

        if relay:
            pl.when(direct(zz))(arrived)
        else:
            arrived()

    losses = loss_own[...]
    for k in range(1, nb):
        i = lax.rem(b + k, nb)
        copy(loss_own, loss_all.at[i], ls.at[k - 1], lr.at[i], i, v).wait_recv()
        losses = losses + loss_all[i]
    loss_out[...] = losses * (1.0 / (tokens * nb))

    for j in range(ny):
        yy = turn_y(j)
        pl.when(has_up)(lambda: w_z(z, yy, True, j == 0).wait_send())
        pl.when(has_down)(lambda: w_z(z, yy, False, j == 0).wait_send())
        for k in range(1, nz):
            @pl.when(z - k >= 0)
            def _():
                pl.when(has_up)(lambda: w_z(z - k, yy, True).wait_send())

            @pl.when(z + k < nz)
            def _():
                pl.when(has_down)(lambda: w_z(z + k, yy, False).wait_send())
    for k in range(1, ny):
        w_y(k).wait_send()
        h_y(k).wait_send()
        y_copy(k).wait_send()
    for k in range(1, nx):
        h_x(k).wait_send()
        for ky in range(1, ny):
            pl.when(core == 0)(lambda: h_xy(k, ky).wait_send())
            pl.when(core == 1)(lambda: h_yx(k, ky).wait_send())
    for kx, ky in ways:
        h_core(kx, ky).wait_send()
        core_copy(kx, ky).wait_send()
        if kx:
            x_copy(kx, ky).wait_send()
    for n in range(len(peers)):
        code_copy(n).wait_send()
        stat_copy(n).wait_send()
    for k in range(1, nb):
        loss_copy(k).wait_send()
    for n in range(nz):
        for k in range(ny):
            yy = turn_y(k)
            if relay and n == 0:
                pl.when(at_end)(lambda: far_copy(yy).wait_send())
                pl.when(jnp.logical_not(at_end))(lambda: r_copy(order[n], yy).wait_send())
            elif n < nz - 1 or k:
                r_copy(order[n], yy).wait_send()


def local(nb, nv, hidden, head_weight, targets, valid_mask):
    nx = nv // 2
    ny = nx if nx <= 2 and nb % nx == 0 else 1
    nz = nb // ny
    rows, width = hidden.shape
    entries, cols = head_weight.shape
    half = entries // ny
    group = ny * nv
    tokens = rows * group
    code = jnp.broadcast_to(jnp.where(valid_mask != 0, targets, -1).astype(f32)[None, :], (8, rows))
    weight = jnp.transpose(head_weight.reshape(ny, half, cols), (0, 2, 1))
    vm = pltpu.VMEM
    dma = pltpu.SemaphoreType.DMA
    slab = ny * cols
    ly, lx = max(ny - 1, 1), max(nx - 1, 1)
    buffers = [
        vm((tokens, width), bf16), vm((width, half), bf16), vm((group, 8, rows), f32), vm((tokens, 128), f32),
        vm((tokens, half), f32), vm((tokens, half), bf16),
        vm((8, tokens), f32), vm((group, 8, tokens), f32), vm((8, 128), f32), vm((nb, 8, 128), f32),
        vm((slab if slab % 128 == 0 else width, half), f32), vm((width, half), bf16), vm((nz, ny, cols, half), bf16),
        vm((tokens, width), f32), vm((nx, ny, rows, width), f32),
        vm((lx, ny, rows, width), bf16), vm((lx, ny, rows, width), bf16),
        vm((ly, rows, width), bf16), vm((ly, rows, width), bf16),
        vm((slab if nz == 4 else 16, half), f32), vm((ny, cols if nz == 4 else 16, half), bf16),
    ]
    sems = [
        dma((2,)), dma((nx + ny,)), dma((nx, ny)), dma((nx, ny)), dma((group,)), dma((nb,)), dma((nb,)),
        dma((ly,)), dma((nb,)), dma((group,)), dma((group,)), dma((group,)), dma((group,)), dma((nb,)), dma((nb,)),
        dma((nb,)), dma((nb,)), dma((nx, ny)), dma((nx, ny)), dma((nx, ny)), dma((nx, ny)), dma((ny,)), dma((ny,)),
        dma((ny,)), dma((ny,)),
    ]
    whole = pl.BlockSpec(memory_space=vm)
    head_t, hidden_grad, loss = pl.pallas_call(
        functools.partial(kernel, (nz, ny, nx, nv)),
        out_shape=(
            jax.ShapeDtypeStruct((ny, cols, half), f32),
            jax.ShapeDtypeStruct((rows, width), f32),
            jax.ShapeDtypeStruct((8, 128), f32),
        ),
        in_specs=[whole] * 3,
        out_specs=(whole,) * 3,
        scratch_shapes=buffers + sems,
        compiler_params=pltpu.CompilerParams(
            collective_id=0, has_side_effects=True, vmem_limit_bytes=67043328),
    )(hidden, weight, code)
    return jnp.transpose(head_t, (0, 2, 1)).reshape(entries, cols), hidden_grad, loss[0, 0]


def column_groups(width):
    units = width // 256
    sizes, left = [2], units - 2
    while left > 6:
        sizes.append(3)
        left -= 3
    while left > 0:
        take = max(1, (left + 1) // 2)
        sizes.append(take)
        left -= take
    starts = [sum(sizes[:n]) for n in range(len(sizes))]
    return [(s, n) for s, n in zip(starts, sizes)]


def plane_kernel(h_in, w_in, ids_in, mask_in, head_out, hid_out, loss_out, h_all, w_all, w_over, ids_own, mask_own,
                 code_own, code_got, code_all,
                 logits, expo, delta, stat_own, stat_all, loss_one, loss_two, loss_all, loss_zs,
                 grad_own, held, grad_send, far_in, r_in, part, core_in, x_out, x_in, y_out, y_in, *sems):
    (own_sem, hs, hf, hd, hr, w_up, w_dn, wr, wys, cs, cr, ss, sr, ls, lr, ms, mr,
     es, er, rs, rr, fs, fr, ds, dr, xs, xr, ys, yr) = sems
    nz, ny, nv = 4, 2, 4
    nb = nz * ny
    rows, width = h_in.shape
    cols, half = w_in.shape[0], w_in.shape[1] // ny
    piece = cols // 2
    group = ny * nv
    tokens = rows * group
    slab = ny * cols
    shift, lo = cols % 128, cols - cols % 128
    win = -(-(cols + shift) // 128) * 128
    b, v = lax.axis_index("batch"), lax.axis_index("vocab")
    z, y = lax.div(b, ny), lax.rem(b, ny)
    x, core = lax.div(v, 2), lax.rem(v, 2)
    me = y * nv + v
    low = z * 2 < nz
    at_end = (z == 0) | (z == nz - 1)
    inside = jnp.logical_not(at_end)

    def flip(a, k):
        return 1 - a if k else a

    def copy(src, dst, send, recv, bb, vv):
        return pltpu.make_async_remote_copy(
            src_ref=src, dst_ref=dst, send_sem=send, recv_sem=recv,
            device_id={"batch": bb, "vocab": vv}, device_id_type=MESH)

    def hrow(i):
        return pl.ds(pl.multiple_of(i * rows, 16), rows)

    over_x, over_y, over_core = (1 - x) * 2 + core, z * ny + 1 - y, x * 2 + 1 - core
    peers = [(ky, kx, kc) for ky in range(2) for kx in range(2) for kc in range(2) if ky or kx or kc]

    def peer(n):
        ky, kx, kc = peers[n]
        yy, vv = flip(y, ky), flip(x, kx) * 2 + flip(core, kc)
        return z * ny + yy, vv, yy * nv + vv

    def z_peer(k):
        return lax.rem(z + k, nz) * ny + y

    barrier = pltpu.get_barrier_semaphore()
    for k in range(1, nz):
        pl.semaphore_signal(barrier, inc=1, device_id={"batch": z_peer(k), "vocab": v}, device_id_type=MESH)
    for n in range(len(peers)):
        bb, vv, _ = peer(n)
        pl.semaphore_signal(barrier, inc=1, device_id={"batch": bb, "vocab": vv}, device_id_type=MESH)
    first = pl.ds(pl.multiple_of(y * half, 128), half)
    second = pl.ds(pl.multiple_of((1 - y) * half, 128), half)
    local = [
        pltpu.make_async_copy(w_in.at[:, second], w_over, own_sem.at[0]),
        pltpu.make_async_copy(w_in.at[:, first], w_all.at[pl.ds(pl.multiple_of(b * cols, 16), cols)], own_sem.at[1]),
        pltpu.make_async_copy(ids_in, ids_own, own_sem.at[2]),
        pltpu.make_async_copy(mask_in, mask_own, own_sem.at[3]),
        pltpu.make_async_copy(h_in, h_all.at[hrow(me)], own_sem.at[4]),
    ]
    for one in local:
        one.start()
    for one in local:
        one.wait()
    code = jnp.where(mask_own[...] != 0, ids_own[...], -1).astype(f32)
    code_own[...] = jnp.broadcast_to(code, code_own.shape)
    pl.semaphore_wait(barrier, nz - 1 + len(peers))

    def w_ref(i, h):
        return w_all.at[pl.ds(pl.multiple_of(i * cols + h * piece, 16), piece)]

    def w_z(i, h, up):
        return copy(w_ref(i, h), w_ref(i, h), (w_up if up else w_dn).at[i, h],
                    wr.at[i, h], b + ny if up else b - ny, v)

    def w_pass(i, h, up):
        return copy(w_ref(i, h), w_ref(i, h), w_up.at[i, h], wr.at[i, h], jnp.where(up, b + ny, b - ny), v)

    def w_y(h):
        return copy(w_over.at[pl.ds(h * piece, piece)], w_ref(b, h), wys.at[h], wr.at[b, h], over_y, v)

    def w_got(i, h):
        copy(w_ref(i, h), w_ref(i, h), wys.at[h], wr.at[i, h], over_y, v).wait_recv()

    has_up, has_down = z + 1 < nz, z >= 1
    near = z + 1 - 2 * lax.rem(z, 2)
    slabs = [z, near, jnp.where(low, 2, 1), jnp.where(low, 3, 0)]

    def h_send(i, sem, bb, vv):
        return copy(h_all.at[hrow(i)], h_all.at[hrow(i)], sem, hr.at[i], bb, vv)

    def h_x():
        return h_send(me, hs.at[0], b, over_x)

    def h_y():
        return h_send(me, hs.at[1], over_y, v)

    def h_xy():
        return h_send(y * nv + over_x, hf.at[0], over_y, v)

    def h_yx():
        return h_send((1 - y) * nv + v, hf.at[0], b, over_x)

    def h_core(kx, ky):
        i = flip(y, ky) * nv + flip(x, kx) * 2 + core
        return h_send(i, hd.at[kx, ky], b, over_core)

    def h_got(kx, ky, cc):
        i = flip(y, ky) * nv + flip(x, kx) * 2 + cc
        h_send(i, hd.at[kx, ky], b, over_core).wait_recv()

    def code_copy(n):
        bb, vv, _ = peer(n)
        return copy(code_own, code_got.at[me], cs.at[n], cr.at[me], bb, vv)

    for h in range(2):
        w_y(h).start()
    for h in range(2):
        pl.when(has_up)(lambda: w_z(b, h, True).start())
        pl.when(has_down)(lambda: w_z(b, h, False).start())
    h_x().start()
    h_y().start()
    for n in range(len(peers)):
        code_copy(n).start()
    h_core(0, 0).start()
    for h in range(2):
        i = z * ny + 1 - y
        w_got(i, h)
        pl.when(has_up)(lambda: w_z(i, h, True).start())
        pl.when(has_down)(lambda: w_z(i, h, False).start())

    def w_slab(zz, onward, which=(0, 1)):
        for k in which:
            for h in range(2):
                i = zz * ny + flip(y, k)
                w_got(i, h)
                if onward:
                    w_pass(i, h, zz < z).start()

    @pl.when(at_end)
    def _():
        w_slab(slabs[1], False)

    @pl.when(inside)
    def _():
        w_slab(slabs[1], True)
        w_slab(slabs[2], True)

    h_got(1, 0, core)
    pl.when(core == 0)(lambda: h_xy().start())
    h_core(1, 0).start()
    h_got(0, 1, core)
    pl.when(core == 1)(lambda: h_yx().start())
    h_core(0, 1).start()

    @pl.when(at_end)
    def _():
        w_slab(slabs[2], False)

    @pl.when(inside)
    def _():
        w_slab(slabs[3], True)

    code_got[me] = code_own[...]
    for n in range(len(peers)):
        bb, vv, i = peer(n)
        copy(code_own, code_got.at[i], cs.at[n], cr.at[i], bb, vv).wait_recv()
    for i in range(group):
        code_all[i * rows:(i + 1) * rows, :] = jnp.transpose(jnp.concatenate([code_got[i]] * (rows // 8), axis=0))

    h_got(1, 1, core)
    h_core(1, 1).start()
    for kx in range(2):
        for ky in range(2):
            h_got(kx, ky, 1 - core)

    step = 2 * rows
    steps = tokens // step
    lines = lax.broadcasted_iota(jnp.int32, (8, rows), 0)

    def scores(n, zz, at=0, wide=slab):
        here = pl.ds(pl.multiple_of(zz * slab + at, 128), wide)
        there = pl.ds(pl.multiple_of(zz * slab + at, 16), wide)
        return jnp.dot(h_all[n * step:(n + 1) * step, here], w_all[there, :], preferred_element_type=f32)

    for j in range(nz - 1):
        for n in range(steps):
            span = pl.ds(n * step, step)
            if j:
                logits[span, :] += scores(n, slabs[j])
            else:
                logits[span, :] = scores(n, slabs[j])

    early = lo
    pl.when(at_end)(lambda: w_slab(slabs[3], False, (0,)))
    for n in range(steps):
        logits[n * step:(n + 1) * step, :] += scores(n, slabs[3], y * (slab - early), early)
    pl.when(at_end)(lambda: w_slab(slabs[3], False, (1,)))

    sums = jnp.zeros((8, rows), f32)
    for n in range(steps):
        span = pl.ds(n * step, step)
        capped = softcap * jnp.tanh((logits[span, :] + scores(n, slabs[3], (1 - y) * early, slab - early)) * (1.0 / softcap))
        raised = jnp.exp(capped)
        logits[span, :] = capped
        expo[span, :] = raised
        total = jnp.broadcast_to(jnp.sum(raised, axis=1, keepdims=True), (step, 128))
        for k in range(2):
            turned = jnp.transpose(total[k * rows:(k + 1) * rows])
            sums = jnp.where(lines == 2 * n + k, turned[0:8], sums)
    stat_own[...] = sums

    def stat_copy(n):
        bb, vv, _ = peer(n)
        return copy(stat_own, stat_all.at[me], ss.at[n], sr.at[me], bb, vv)

    for n in range(len(peers)):
        stat_copy(n).start()

    ids = (lax.broadcasted_iota(jnp.int32, (step, half), 1) + (v * ny + y) * half).astype(f32)
    hit_total = jnp.zeros((step, 1), f32)
    for n in range(steps):
        span = pl.ds(n * step, step)
        capped = logits[span, :]
        hit = ids == code_all[span, 0:1]
        slope = 1.0 - (capped * (1.0 / softcap)) ** 2
        expo[span, :] = expo[span, :] * slope
        logits[span, :] = jnp.where(hit, slope, 0.0)
        hit_total = hit_total + jnp.sum(jnp.where(hit, capped, 0.0), axis=1, keepdims=True)
    hit_total = jnp.sum(hit_total, axis=0, keepdims=True)
    code_rows = jnp.zeros((8, rows), f32)
    for i in range(group):
        code_rows = jnp.where(lines == i, code_got[i], code_rows)
    weight = (code_rows >= 0).astype(f32)

    stat_all[me] = sums
    for n in range(len(peers)):
        bb, vv, i = peer(n)
        copy(stat_own, stat_all.at[i], ss.at[n], sr.at[i], bb, vv).wait_recv()
    partition = stat_all[0]
    for i in range(1, group):
        partition = partition + stat_all[i]
    scale = weight / partition

    def delta_copy(n):
        span = pl.ds(n * step, step)
        return copy(delta.at[0, span], delta.at[1, span], es.at[n], er.at[n], over_y, v)

    for n in range(steps):
        for k in range(2):
            i = 2 * n + k
            span = pl.ds(i * rows, rows)
            by_row = jnp.transpose(jnp.broadcast_to(scale[i:i + 1, :], (rows, rows)))
            factor = jnp.concatenate([by_row] * (half // rows), axis=1)
            delta[0, span, :] = (expo[span, :] * factor - logits[span, :]).astype(bf16)
        delta_copy(n).start()

    share_loss = jnp.sum(weight * jnp.log(partition), axis=1, keepdims=True)
    loss = jnp.sum(share_loss, axis=0, keepdims=True) * (1.0 / group) - hit_total
    loss_one[...] = jnp.broadcast_to(loss, loss_one.shape)

    def loss_copy(n):
        bb, vv, _ = peer(n)
        return copy(loss_one, loss_all.at[me], ls.at[n], lr.at[me], bb, vv)

    near_end = jnp.where(low, 1, 2)
    far = jnp.where(low, nz - 1, 0)
    targets = [jnp.where(lax.rem(z, 2) == 0, nz - 1, 0), jnp.where(low, 2, 1),
               jnp.where(at_end, near_end, far), z]
    top = y * shift

    def grad_share(zz, r):
        here = pl.ds(pl.multiple_of(zz * slab + y * lo, 128), win)
        return lax.dot_general(h_all[:, here], delta[r], (((0,), (0,)), ((), ())), preferred_element_type=f32)

    def sent(k, r):
        return grad_send.at[k, r, pl.ds(pl.multiple_of(top, 16), cols)]

    def r_copy(k, r):
        return copy(sent(k, r), r_in.at[z, r], rs.at[k, r], rr.at[z, r], targets[k] * ny + y, v)

    def far_copy(r):
        return copy(sent(0, r), far_in.at[r], fs.at[r], fr.at[r], near_end * ny + y, v)

    def head_piece(k, r):
        share = grad_share(targets[k], r)
        if k == nz - 1:
            grad_own[r] = share
        elif k == 2:
            @pl.when(at_end)
            def _():
                grad_send[k, r] = share.astype(bf16)
                r_copy(k, r).start()

            @pl.when(inside)
            def _():
                held[r] = share
        else:
            grad_send[k, r] = share.astype(bf16)
            if k == 0:
                pl.when(at_end)(lambda: far_copy(r).start())
                pl.when(inside)(lambda: r_copy(k, r).start())
            else:
                r_copy(k, r).start()

    cstep = chunk_of(cols, 64)

    def over_cols(body):
        def one(n, carry):
            body(pl.multiple_of(n * cstep, 16))
            return carry

        lax.fori_loop(0, cols // cstep, one, 0)

    def relay(r):
        @pl.when(inside)
        def _():
            far_copy(r).wait_recv()

            def add(n):
                here = pl.ds(pl.multiple_of(top + n, 16), cstep)
                grad_send[2, r, here, :] = (held[r, here, :] + far_in[r, pl.ds(n, cstep), :].astype(f32)).astype(bf16)

            over_cols(add)
            r_copy(2, r).start()

    groups = column_groups(width)
    blocks = [(1, 1), (1, 0), (0, 1), (0, 0)]
    unit = width // (width // 256)

    def span_of(g):
        first, n = groups[g]
        return pl.ds(first * unit, n * unit)

    def block(kx, ky, cc):
        return flip(y, ky) * nv + flip(x, kx) * 2 + cc

    def core_copy(g, kx, ky):
        return copy(part.at[hrow(block(kx, ky, 1 - core)), span_of(g)], core_in.at[kx, ky, :, span_of(g)],
                    ds.at[g, kx, ky], dr.at[g, kx, ky], b, over_core)

    def x_copy(g, ky):
        return copy(x_out.at[ky, :, span_of(g)], x_in.at[ky, :, span_of(g)], xs.at[g, ky], xr.at[g, ky], b, over_x)

    def y_copy(g):
        return copy(y_out.at[:, span_of(g)], y_in.at[:, span_of(g)], ys.at[g], yr.at[g], over_y, v)

    def part_group(g):
        first, n = groups[g]

        def one(j, carry):
            span = pl.ds(pl.multiple_of(j * unit, 128), unit)
            part[:, span] = lax.dot_general(
                delta[0], w_all[span, :], (((1,), (1,)), ((), ())), preferred_element_type=f32)
            return carry

        lax.fori_loop(first, first + n, one, 0)
        for kx, ky in blocks:
            core_copy(g, kx, ky).start()

    hstep = 16

    def over_rows(body):
        def one(n, carry):
            body(pl.multiple_of(n * hstep, hstep))
            return carry

        lax.fori_loop(0, rows // hstep, one, 0)

    def core_sum(g):
        span = span_of(g)
        for kx, ky in blocks:
            core_copy(g, kx, ky).wait_recv()
            start = block(kx, ky, core) * rows

            def add(n):
                here = pl.ds(pl.multiple_of(start + n, hstep), hstep)
                both = part[here, span] + core_in[kx, ky, pl.ds(n, hstep), span]
                if kx:
                    x_out[ky, pl.ds(n, hstep), span] = both.astype(bf16)
                else:
                    part[here, span] = both

            over_rows(add)
            if kx:
                x_copy(g, ky).start()

    def x_sum(g):
        span = span_of(g)
        for ky in (1, 0):
            x_copy(g, ky).wait_recv()
            start = block(0, ky, core) * rows

            def add(n):
                here = pl.ds(pl.multiple_of(start + n, hstep), hstep)
                total = part[here, span] + x_in[ky, pl.ds(n, hstep), span].astype(f32)
                if ky:
                    y_out[pl.ds(n, hstep), span] = total.astype(bf16)
                else:
                    hid_out[pl.ds(n, hstep), span] = total

            over_rows(add)
            if ky:
                y_copy(g).start()

    def y_sum(g):
        span = span_of(g)
        y_copy(g).wait_recv()

        def add(n):
            here = pl.ds(n, hstep)
            hid_out[here, span] += y_in[here, span].astype(f32)

        over_rows(add)

    count = len(groups)
    head_piece(0, 0)
    part_group(0)
    head_piece(1, 0)
    part_group(1)
    for n in range(len(peers)):
        loss_copy(n).start()
    core_sum(0)
    head_piece(2, 0)
    for g in range(2, count):
        part_group(g)
        core_sum(g - 1)
        if g == 3:
            relay(0)
    core_sum(count - 1)
    head_piece(3, 0)

    loss_all[me] = loss_one[...]
    for n in range(len(peers)):
        bb, vv, i = peer(n)
        copy(loss_one, loss_all.at[i], ls.at[n], lr.at[i], bb, vv).wait_recv()
    losses = loss_all[0]
    for i in range(1, group):
        losses = losses + loss_all[i]
    loss_two[...] = losses

    def plane_copy(k):
        return copy(loss_two, loss_zs.at[z], ms.at[k - 1], mr.at[z], z_peer(k), v)

    for k in range(1, nz):
        plane_copy(k).start()

    x_sum(0)
    for n in range(steps):
        delta_copy(n).wait_recv()
    for k in range(nz):
        head_piece(k, 1)
        if k == 1:
            x_sum(1)
    x_sum(2)
    relay(1)
    for g in range(3, count):
        x_sum(g)
        y_sum(g - 3)

    def r_got(zz, r):
        copy(r_in.at[zz, r], r_in.at[zz, r], rs.at[0, r], rr.at[zz, r], z_peer(1), v).wait_recv()

    def lanes(r):
        return pl.ds(pl.multiple_of(flip(y, r) * half, 128), half)

    sources = [near, jnp.where(low, 2, 1), far]

    def head_sum(r):
        for k in range(2):
            r_got(sources[k], r)

        def add(n):
            here = pl.ds(n, cstep)
            total = grad_own[r, pl.ds(pl.multiple_of(top + n, 16), cstep), :]
            for k in range(2):
                total = total + r_in[sources[k], r, here, :].astype(f32)
            head_out[here, lanes(r)] = total

        over_cols(add)

        @pl.when(inside)
        def _():
            r_got(sources[2], r)

            def last(n):
                here = pl.ds(n, cstep)
                head_out[here, lanes(r)] += r_in[sources[2], r, here, :].astype(f32)

            over_cols(last)

    head_sum(0)
    y_sum(count - 3)
    y_sum(count - 2)
    loss_zs[z] = loss_two[...]
    for k in range(1, nz):
        i = lax.rem(z + k, nz)
        copy(loss_two, loss_zs.at[i], ms.at[k - 1], mr.at[i], z_peer(k), v).wait_recv()
    losses = loss_zs[0]
    for i in range(1, nz):
        losses = losses + loss_zs[i]
    loss_out[...] = losses * (1.0 / (tokens * nz))
    y_sum(count - 1)
    head_sum(1)

    for h in range(2):
        w_y(h).wait_send()
        pl.when(has_up)(lambda: w_z(b, h, True).wait_send())
        pl.when(has_down)(lambda: w_z(b, h, False).wait_send())
        pl.when(has_up)(lambda: w_z(z * ny + 1 - y, h, True).wait_send())
        pl.when(has_down)(lambda: w_z(z * ny + 1 - y, h, False).wait_send())

    @pl.when(inside)
    def _():
        for j in range(1, nz):
            for k in range(ny):
                for h in range(2):
                    w_pass(slabs[j] * ny + flip(y, k), h, slabs[j] < z).wait_send()

    h_x().wait_send()
    h_y().wait_send()
    pl.when(core == 0)(lambda: h_xy().wait_send())
    pl.when(core == 1)(lambda: h_yx().wait_send())
    for kx, ky in blocks:
        h_core(kx, ky).wait_send()
    for n in range(len(peers)):
        code_copy(n).wait_send()
        stat_copy(n).wait_send()
        loss_copy(n).wait_send()
    for k in range(1, nz):
        plane_copy(k).wait_send()
    for n in range(steps):
        delta_copy(n).wait_send()
    for r in range(2):
        pl.when(at_end)(lambda: far_copy(r).wait_send())
        pl.when(inside)(lambda: r_copy(0, r).wait_send())
        r_copy(1, r).wait_send()
        r_copy(2, r).wait_send()
    for g in range(count):
        for kx, ky in blocks:
            core_copy(g, kx, ky).wait_send()
        for ky in range(2):
            x_copy(g, ky).wait_send()
        y_copy(g).wait_send()


def plane_local(hidden, head_weight, targets, valid_mask):
    nz, ny, nv = 4, 2, 4
    rows, width = hidden.shape
    entries, cols = head_weight.shape
    half = entries // ny
    group = ny * nv
    tokens = rows * group
    shift = cols % 128
    win = -(-(cols + shift) // 128) * 128
    vm = pltpu.VMEM
    dma = pltpu.SemaphoreType.DMA
    count = len(column_groups(width))
    line = vm((8, rows), f32)
    buffers = [
        vm((tokens, width), bf16), vm((width, half), bf16), vm((cols, half), bf16),
        vm((1, rows), jnp.int32), vm((1, rows), jnp.int32), line, vm((group, 8, rows), f32), vm((tokens, 128), f32),
        vm((tokens, half), f32), vm((tokens, half), f32), vm((2, tokens, half), bf16),
        line, vm((group, 8, rows), f32), line, line, vm((group, 8, rows), f32), vm((nz, 8, rows), f32),
        vm((2, win, half), f32), vm((2, win, half), f32), vm((3, 2, win, half), bf16),
        vm((2, cols, half), bf16), vm((nz, 2, cols, half), bf16),
        vm((tokens, width), f32), vm((2, 2, rows, width), f32),
        vm((2, rows, width), bf16), vm((2, rows, width), bf16), vm((rows, width), bf16), vm((rows, width), bf16),
    ]
    sems = [
        dma((5,)), dma((2,)), dma((1,)), dma((2, 2)), dma((group,)), dma((8, 2)), dma((8, 2)), dma((8, 2)), dma((2,)),
        dma((7,)), dma((group,)), dma((7,)), dma((group,)), dma((7,)), dma((group,)), dma((3,)), dma((nz,)),
        dma((4,)), dma((4,)), dma((3, 2)), dma((nz, 2)), dma((2,)), dma((2,)),
        dma((count, 2, 2)), dma((count, 2, 2)), dma((count, 2)), dma((count, 2)), dma((count,)), dma((count,)),
    ]
    whole = pl.BlockSpec(memory_space=vm)
    head_t, hidden_grad, loss = pl.pallas_call(
        plane_kernel,
        out_shape=(
            vm((cols, entries), f32),
            vm((rows, width), f32),
            vm((8, rows), f32),
        ),
        in_specs=[pl.BlockSpec(memory_space=pl.ANY)] * 4,
        out_specs=(whole,) * 3,
        scratch_shapes=buffers + sems,
        compiler_params=pltpu.CompilerParams(
            collective_id=1, has_side_effects=True, vmem_limit_bytes=58 * 1024 * 1024),
    )(hidden, jnp.transpose(head_weight), targets[None, :], valid_mask[None, :])
    return jnp.transpose(head_t), hidden_grad, loss[0, 0]


def in_planes(nb, nv, hidden, head_weight, targets, valid_mask):
    rows, width = hidden.shape
    entries, cols = head_weight.shape
    fits = nb == 8 and nv == 4 and rows == 128 and width % 256 == 0 and width >= 2048
    return fits and entries % 256 == 0 and cols % 32 == 0 and (2 * cols) % 128 == 0


def device(nb, nv, *arrays):
    if in_planes(nb, nv, *arrays):
        return plane_local(*arrays)
    return local(nb, nv, *arrays)


def solution(mesh):
    placed = (
        P(("batch", "vocab"), None),
        P("vocab", "batch"),
        P(("batch", "vocab")),
        P(("batch", "vocab")),
    )
    return jax.shard_map(
        functools.partial(device, mesh.shape["batch"], mesh.shape["vocab"]),
        mesh=mesh,
        in_specs=placed,
        out_specs=(P("vocab", "batch"), P(("batch", "vocab"), None), P()),
        check_vma=False,
    )
```

```python
import functools

import jax
import jax.numpy as jnp
from jax import lax
from jax.experimental import pallas as pl
from jax.experimental.pallas import tpu as pltpu
from jax.sharding import PartitionSpec as P

softcap = 30.0
MESH = pl.DeviceIdType.MESH
f32, bf16 = jnp.float32, jnp.bfloat16


def chunk_of(length, most):
    return max(s for s in range(16, most + 1, 16) if length % s == 0)


def kernel(sizes, h_in, w_in, code_in, head_out, hid_out, loss_out, h_all, w_all, code_got, code_all,
           logits, delta, stat_own, stat_all, loss_own, loss_all, grad, grad_send, r_in,
           part, core_in, x_out, x_in, y_out, y_in, far_own, far_in, *sems):
    nz, ny, nx, nv = sizes
    (own_sem, hs, hf, hd, hr, ws_up, ws_dn, ws_y, wr, cs, cr, ss, sr, ls, lr,
     rs, rr, ds, dr, xs, xr, ys, yr, fs, fr) = sems
    nb = nz * ny
    rows, width = h_in.shape
    cols, half = w_in.shape[1:]
    group = ny * nv
    tokens = rows * group
    entries = ny * half
    b, v = lax.axis_index("batch"), lax.axis_index("vocab")
    z, y = lax.div(b, ny), lax.rem(b, ny)
    x, core = lax.div(v, 2), lax.rem(v, 2)
    other = x * 2 + 1 - core
    me = y * nv + v

    def at(bb, vv):
        return {"batch": bb, "vocab": vv}

    def copy(src, dst, send, recv, bb, vv):
        return pltpu.make_async_remote_copy(
            src_ref=src, dst_ref=dst, send_sem=send, recv_sem=recv, device_id=at(bb, vv), device_id_type=MESH)

    def hrow(i):
        return pl.ds(pl.multiple_of(i * rows, 16), rows)

    def wrow(i):
        return pl.ds(pl.multiple_of(i * cols, 16), cols)

    def turn_y(k):
        return lax.rem(y + k, ny)

    def turn_x(k):
        return lax.rem(x + k, nx)

    peers = [(k, j) for k in range(ny) for j in range(nv) if k or j]

    def peer(n):
        k, j = peers[n]
        return z * ny + turn_y(k), lax.rem(v + j, nv), turn_y(k) * nv + lax.rem(v + j, nv)

    barrier = pltpu.get_barrier_semaphore()
    for k in range(1, nb):
        pl.semaphore_signal(barrier, inc=1, device_id=at(lax.rem(b + k, nb), v), device_id_type=MESH)
    met = [n for n in range(len(peers)) if peers[n][1]]
    for n in met:
        bb, vv, _ = peer(n)
        pl.semaphore_signal(barrier, inc=1, device_id=at(bb, vv), device_id_type=MESH)
    pl.semaphore_wait(barrier, nb - 1 + len(met))

    def w_z(zz, yy, up, own=False):
        i = zz * ny + yy
        dst = w_all.at[wrow(i)]
        sem = (ws_up if up else ws_dn).at[i]
        return copy(w_in.at[y] if own else dst, dst, sem, wr.at[i], b + ny if up else b - ny, v)

    def w_y(k):
        return copy(w_in.at[turn_y(k)], w_all.at[wrow(b)], ws_y.at[k - 1], wr.at[b], z * ny + turn_y(k), v)

    def w_got(zz, yy):
        w_z(zz, yy, True).wait_recv()

    has_up, has_down = z + 1 < nz, z >= 1

    def h_send(n_src, sem, bb, vv, own=False):
        dst = h_all.at[hrow(n_src)]
        return copy(h_in if own else dst, dst, sem, hr.at[n_src], bb, vv)

    def h_x(k):
        return h_send(me, hs.at[k - 1], b, turn_x(k) * 2 + core, True)

    def h_y(k):
        return h_send(me, hs.at[nx + k - 1], z * ny + turn_y(k), v, True)

    def h_xy(kx, ky):
        return h_send(y * nv + turn_x(kx) * 2 + core, hf.at[kx, ky], z * ny + turn_y(ky), v)

    def h_yx(kx, ky):
        return h_send(turn_y(ky) * nv + v, hf.at[kx, ky], b, turn_x(kx) * 2 + core)

    def h_core(kx, ky):
        i = turn_y(ky) * nv + turn_x(kx) * 2 + core
        return h_send(i, hd.at[kx, ky], b, other, kx == 0 and ky == 0)

    def h_got(kx, ky, cc):
        i = turn_y(ky) * nv + turn_x(kx) * 2 + cc
        h_send(i, hd.at[kx, ky], b, other).wait_recv()

    def code_copy(n):
        bb, vv, _ = peer(n)
        return copy(code_in, code_got.at[me], cs.at[n], cr.at[me], bb, vv)

    for k in range(1, ny):
        w_y(k).start()
    pl.when(has_up)(lambda: w_z(z, y, True, True).start())
    pl.when(has_down)(lambda: w_z(z, y, False, True).start())
    for k in range(1, nx):
        h_x(k).start()
    for k in range(1, ny):
        h_y(k).start()
    for n in range(len(peers)):
        code_copy(n).start()
    h_core(0, 0).start()
    local = [
        pltpu.make_async_copy(w_in.at[y], w_all.at[wrow(b)], own_sem.at[0]),
        pltpu.make_async_copy(h_in, h_all.at[hrow(me)], own_sem.at[1]),
    ]
    for one in local:
        one.start()

    for k in range(1, ny):
        w_got(z, turn_y(k))
        pl.when(has_up)(lambda: w_z(z, turn_y(k), True).start())
        pl.when(has_down)(lambda: w_z(z, turn_y(k), False).start())

    def h_pass():
        for kx in range(1, nx):
            h_got(kx, 0, core)
            for ky in range(1, ny):
                pl.when(core == 0)(lambda: h_xy(kx, ky).start())
            h_core(kx, 0).start()
        for ky in range(1, ny):
            h_got(0, ky, core)
            for kx in range(1, nx):
                pl.when(core == 1)(lambda: h_yx(kx, ky).start())
            h_core(0, ky).start()

    def h_rest():
        for kx in range(1, nx):
            for ky in range(1, ny):
                h_got(kx, ky, core)
                h_core(kx, ky).start()

    for k in range(1, nz):
        for j in range(ny):
            yy = turn_y(j)

            @pl.when(z - k >= 0)
            def _():
                w_got(z - k, yy)
                pl.when(has_up)(lambda: w_z(z - k, yy, True).start())

            @pl.when(z + k < nz)
            def _():
                w_got(z + k, yy)
                pl.when(has_down)(lambda: w_z(z + k, yy, False).start())
        if k == 1:
            h_pass()
        if k == min(2, nz - 1):
            h_rest()

    for one in local:
        one.wait()
    for kx in range(nx):
        for ky in range(ny):
            h_got(kx, ky, 1 - core)
    code_got[me] = code_in[...]
    for n in range(len(peers)):
        bb, vv, i = peer(n)
        copy(code_in, code_got.at[i], cs.at[n], cr.at[i], bb, vv).wait_recv()
    for i in range(group):
        code_all[i * rows:(i + 1) * rows, :] = jnp.transpose(jnp.concatenate([code_got[i]] * 16, axis=0))

    step = chunk_of(tokens, 256)
    lanes = lax.broadcasted_iota(jnp.int32, (step, 128), 1)
    first = v * entries + y * half

    def span_of(n):
        return pl.ds(pl.multiple_of(n * step, step), step)

    def hits(n):
        ids = lax.broadcasted_iota(jnp.int32, (step, half), 1) + first
        return ids == code_all[span_of(n), 0:1].astype(jnp.int32)

    for n in range(tokens // step):
        span = pl.ds(n * step, step)
        scores = jnp.dot(h_all[span, :], w_all[...], preferred_element_type=f32)
        capped = softcap * jnp.tanh(scores * (1.0 / softcap))
        logits[span, :] = capped
        total = jnp.sum(jnp.exp(capped), axis=1, keepdims=True)
        hit_sum = jnp.sum(jnp.where(hits(n), capped, 0.0), axis=1, keepdims=True)
        turned = jnp.transpose(jnp.where(lax.rem(lanes, 8) < 4, total, hit_sum))
        stat_own[:, n * step:(n + 1) * step] = turned[0:8]

    def stat_copy(n):
        bb, vv, _ = peer(n)
        return copy(stat_own, stat_all.at[me], ss.at[n], sr.at[me], bb, vv)

    for n in range(len(peers)):
        stat_copy(n).start()
    for n in range(len(peers)):
        bb, vv, i = peer(n)
        copy(stat_own, stat_all.at[i], ss.at[n], sr.at[i], bb, vv).wait_recv()
    stats = stat_own[...]
    for n in range(len(peers)):
        stats = stats + stat_all[peer(n)[2]]

    loss = jnp.zeros((1, 1), f32)
    for n in range(tokens // step):
        span = pl.ds(n * step, step)
        weight = (code_all[span, 0:1] >= 0).astype(f32)
        back = jnp.transpose(jnp.concatenate([stats[:, n * step:(n + 1) * step]] * 16, axis=0))
        partition, target_logit = back[:, 0:1], back[:, 4:5]
        loss = loss + jnp.sum(weight * (jnp.log(partition) - target_logit), axis=0, keepdims=True)
        capped = logits[span, :]
        slope = 1.0 - (capped * (1.0 / softcap)) ** 2
        delta[span, :] = ((jnp.exp(capped) * (weight / partition) - jnp.where(hits(n), weight, 0.0)) * slope
                          ).astype(bf16)
    loss_own[...] = jnp.broadcast_to(loss, loss_own.shape)

    def loss_copy(k):
        return copy(loss_own, loss_all.at[b], ls.at[k - 1], lr.at[b], lax.rem(b + k, nb), v)

    def r_copy(zz, yy):
        i = zz * ny + yy
        return copy(grad_send.at[wrow(i)], r_in.at[z, y], rs.at[i], rr.at[b], i, v)

    def grad_share(span):
        return lax.dot_general(h_all[:, span], delta[...], (((0,), (0,)), ((), ())), preferred_element_type=f32)

    slab = ny * cols
    relay = nz == 4 and slab % 128 == 0
    turn = jnp.where(z * 2 >= nz, 1, nz - 1)
    order = [lax.rem(z + turn * k, nz) for k in range(1, nz)] + [z]
    at_end = (z == 0) | (z == nz - 1)
    far = jnp.where(z * 2 >= nz, 0, nz - 1)
    near = jnp.where(z * 2 >= nz, z - 1, z + 1)

    def far_copy(yy):
        return copy(grad_send.at[wrow(far * ny + yy)], far_in.at[yy], fs.at[yy], fr.at[yy], near * ny + y, v)

    def direct(zz):
        return jnp.logical_not(at_end & (zz == far))
    if slab % 128 == 0:
        mine = y * cols
        for n in range(nz):
            zz = order[n]
            span = pl.ds(pl.multiple_of(zz * slab, 128), slab)
            share = grad_share(span)
            held = relay and n == 1
            if n == nz - 1:
                grad[...] = share
            if held:
                @pl.when(jnp.logical_not(at_end))
                def _():
                    far_own[...] = share

                @pl.when(at_end)
                def _():
                    grad_send[span, :] = share.astype(bf16)
                    for k in range(ny):
                        r_copy(zz, turn_y(k)).start()
            else:
                grad_send[span, :] = share.astype(bf16)
                for k in range(ny):
                    yy = turn_y(k)
                    if relay and n == 0:
                        pl.when(at_end)(lambda: far_copy(yy).start())
                        pl.when(jnp.logical_not(at_end))(lambda: r_copy(zz, yy).start())
                    elif n < nz - 1 or k:
                        r_copy(zz, yy).start()
    else:
        mine = b * cols
        wide = chunk_of(width, 256)

        def grad_step(j, carry):
            span = pl.ds(pl.multiple_of(j * wide, wide), wide)
            share = grad_share(span)
            grad[span, :] = share
            grad_send[span, :] = share.astype(bf16)
            return carry

        lax.fori_loop(0, width // wide, grad_step, 0)
        for n in range(nz):
            for k in range(ny):
                if n < nz - 1 or k:
                    r_copy(order[n], turn_y(k)).start()
    for k in range(1, nb):
        loss_copy(k).start()

    wide = chunk_of(width, 256)

    def part_step(j, carry):
        span = pl.ds(pl.multiple_of(j * wide, wide), wide)
        part[:, span] = lax.dot_general(
            delta[...], w_all[span, :], (((1,), (1,)), ((), ())), preferred_element_type=f32)
        return carry

    lax.fori_loop(0, width // wide, part_step, 0)

    def core_copy(kx, ky):
        i = turn_y(ky) * nv + turn_x(kx) * 2 + 1 - core
        return copy(part.at[hrow(i)], core_in.at[kx, ky], ds.at[kx, ky], dr.at[kx, ky], b, other)

    def x_copy(kx, ky):
        return copy(x_out.at[kx - 1, ky], x_in.at[kx - 1, ky], xs.at[kx, ky], xr.at[kx, ky],
                    b, turn_x(kx) * 2 + core)

    def y_copy(ky):
        return copy(y_out.at[ky - 1], y_in.at[ky - 1], ys.at[ky], yr.at[ky], z * ny + turn_y(ky), v)

    ways = [(kx % nx, ky % ny) for kx in range(1, nx + 1) for ky in range(1, ny + 1)]
    for kx, ky in ways:
        core_copy(kx, ky).start()
    hstep = 16

    def over_rows(start, body):
        def one(r, carry):
            body(pl.ds(pl.multiple_of(r * hstep, hstep), hstep),
                 pl.ds(pl.multiple_of(start + r * hstep, hstep), hstep))
            return carry

        lax.fori_loop(0, rows // hstep, one, 0)

    def start_of(kx, ky):
        return (turn_y(ky) * nv + turn_x(kx) * 2 + core) * rows

    for kx, ky in ways:
        core_copy(kx, ky).wait_recv()

        def core_sum(span, here):
            both = part[here, :] + core_in[kx, ky, span, :]
            if kx:
                x_out[kx - 1, ky, span, :] = both.astype(bf16)
            else:
                part[here, :] = both

        over_rows(start_of(kx, ky), core_sum)
        if kx:
            x_copy(kx, ky).start()

    cstep = chunk_of(cols, 64)

    def over_cols(body):
        def one(r, carry):
            body(pl.multiple_of(r * cstep, 16))
            return carry

        lax.fori_loop(0, cols // cstep, one, 0)

    if relay:
        @pl.when(jnp.logical_not(at_end))
        def _():
            for k in range(ny):
                yy = turn_y(k)
                far_copy(yy).wait_recv()

                def far_sum(r):
                    here = pl.ds(pl.multiple_of(yy * cols + r, 16), cstep)
                    there = pl.ds(pl.multiple_of((far * ny + yy) * cols + r, 16), cstep)
                    grad_send[there, :] = (far_own[here, :] + far_in[yy, pl.ds(r, cstep), :].astype(f32)).astype(bf16)

                over_cols(far_sum)
                r_copy(far, yy).start()

    for ky in [k % ny for k in range(1, ny + 1)]:
        for kx in range(1, nx):
            x_copy(kx, ky).wait_recv()

        def x_sum(span, here):
            total = part[here, :]
            for kx in range(1, nx):
                total = total + x_in[kx - 1, ky, span, :].astype(f32)
            if ky:
                y_out[ky - 1, span, :] = total.astype(bf16)
            else:
                hid_out[span, :] = total

        over_rows(start_of(0, ky), x_sum)
        if ky:
            y_copy(ky).start()

    def r_got(zz, yy):
        i = zz * ny + yy
        copy(grad_send.at[wrow(i)], r_in.at[zz, yy], rs.at[i], rr.at[i], i, v).wait_recv()

    for k in range(1, ny):
        r_got(z, turn_y(k))

    def first_sum(r):
        head_out[y, pl.ds(r, cstep), :] = grad[pl.ds(pl.multiple_of(mine + r, 16), cstep), :]
        for k in range(1, ny):
            head_out[turn_y(k), pl.ds(r, cstep), :] = r_in[z, turn_y(k), pl.ds(r, cstep), :].astype(f32)

    over_cols(first_sum)
    hops = [jnp.where(z * 2 >= nz, lax.rem(z + nz - n, nz), lax.rem(z + n, nz)) for n in range(1, nz)]
    for n in range(1, nz):
        zz = hops[n - 1]
        if n == nz - 1:
            for ky in range(1, ny):
                y_copy(ky).wait_recv()

                def y_sum(span, here):
                    hid_out[span, :] += y_in[ky - 1, span, :].astype(f32)

                over_rows(0, y_sum)

        def more_sum(r):
            for k in range(ny):
                head_out[turn_y(k), pl.ds(r, cstep), :] += r_in[zz, turn_y(k), pl.ds(r, cstep), :].astype(f32)

        def arrived():
            for k in range(ny):
                r_got(zz, turn_y(k))
            over_cols(more_sum)

        if relay:
            pl.when(direct(zz))(arrived)
        else:
            arrived()

    losses = loss_own[...]
    for k in range(1, nb):
        i = lax.rem(b + k, nb)
        copy(loss_own, loss_all.at[i], ls.at[k - 1], lr.at[i], i, v).wait_recv()
        losses = losses + loss_all[i]
    loss_out[...] = losses * (1.0 / (tokens * nb))

    for j in range(ny):
        yy = turn_y(j)
        pl.when(has_up)(lambda: w_z(z, yy, True, j == 0).wait_send())
        pl.when(has_down)(lambda: w_z(z, yy, False, j == 0).wait_send())
        for k in range(1, nz):
            @pl.when(z - k >= 0)
            def _():
                pl.when(has_up)(lambda: w_z(z - k, yy, True).wait_send())

            @pl.when(z + k < nz)
            def _():
                pl.when(has_down)(lambda: w_z(z + k, yy, False).wait_send())
    for k in range(1, ny):
        w_y(k).wait_send()
        h_y(k).wait_send()
        y_copy(k).wait_send()
    for k in range(1, nx):
        h_x(k).wait_send()
        for ky in range(1, ny):
            pl.when(core == 0)(lambda: h_xy(k, ky).wait_send())
            pl.when(core == 1)(lambda: h_yx(k, ky).wait_send())
    for kx, ky in ways:
        h_core(kx, ky).wait_send()
        core_copy(kx, ky).wait_send()
        if kx:
            x_copy(kx, ky).wait_send()
    for n in range(len(peers)):
        code_copy(n).wait_send()
        stat_copy(n).wait_send()
    for k in range(1, nb):
        loss_copy(k).wait_send()
    for n in range(nz):
        for k in range(ny):
            yy = turn_y(k)
            if relay and n == 0:
                pl.when(at_end)(lambda: far_copy(yy).wait_send())
                pl.when(jnp.logical_not(at_end))(lambda: r_copy(order[n], yy).wait_send())
            elif n < nz - 1 or k:
                r_copy(order[n], yy).wait_send()


def local(nb, nv, hidden, head_weight, targets, valid_mask):
    nx = nv // 2
    ny = nx if nx <= 2 and nb % nx == 0 else 1
    nz = nb // ny
    rows, width = hidden.shape
    entries, cols = head_weight.shape
    half = entries // ny
    group = ny * nv
    tokens = rows * group
    code = jnp.broadcast_to(jnp.where(valid_mask != 0, targets, -1).astype(f32)[None, :], (8, rows))
    weight = jnp.transpose(head_weight.reshape(ny, half, cols), (0, 2, 1))
    vm = pltpu.VMEM
    dma = pltpu.SemaphoreType.DMA
    slab = ny * cols
    ly, lx = max(ny - 1, 1), max(nx - 1, 1)
    buffers = [
        vm((tokens, width), bf16), vm((width, half), bf16), vm((group, 8, rows), f32), vm((tokens, 128), f32),
        vm((tokens, half), f32), vm((tokens, half), bf16),
        vm((8, tokens), f32), vm((group, 8, tokens), f32), vm((8, 128), f32), vm((nb, 8, 128), f32),
        vm((slab if slab % 128 == 0 else width, half), f32), vm((width, half), bf16), vm((nz, ny, cols, half), bf16),
        vm((tokens, width), f32), vm((nx, ny, rows, width), f32),
        vm((lx, ny, rows, width), bf16), vm((lx, ny, rows, width), bf16),
        vm((ly, rows, width), bf16), vm((ly, rows, width), bf16),
        vm((slab if nz == 4 else 16, half), f32), vm((ny, cols if nz == 4 else 16, half), bf16),
    ]
    sems = [
        dma((2,)), dma((nx + ny,)), dma((nx, ny)), dma((nx, ny)), dma((group,)), dma((nb,)), dma((nb,)),
        dma((ly,)), dma((nb,)), dma((group,)), dma((group,)), dma((group,)), dma((group,)), dma((nb,)), dma((nb,)),
        dma((nb,)), dma((nb,)), dma((nx, ny)), dma((nx, ny)), dma((nx, ny)), dma((nx, ny)), dma((ny,)), dma((ny,)),
        dma((ny,)), dma((ny,)),
    ]
    whole = pl.BlockSpec(memory_space=vm)
    head_t, hidden_grad, loss = pl.pallas_call(
        functools.partial(kernel, (nz, ny, nx, nv)),
        out_shape=(
            jax.ShapeDtypeStruct((ny, cols, half), f32),
            jax.ShapeDtypeStruct((rows, width), f32),
            jax.ShapeDtypeStruct((8, 128), f32),
        ),
        in_specs=[whole] * 3,
        out_specs=(whole,) * 3,
        scratch_shapes=buffers + sems,
        compiler_params=pltpu.CompilerParams(
            collective_id=0, has_side_effects=True, vmem_limit_bytes=67043328),
    )(hidden, weight, code)
    return jnp.transpose(head_t, (0, 2, 1)).reshape(entries, cols), hidden_grad, loss[0, 0]


def column_groups(width):
    units = width // 256
    sizes, left = [1, 2], units - 5
    while left > 0:
        sizes.append(min(3, left))
        left -= sizes[-1]
    sizes += [1, 1]
    starts = [sum(sizes[:n]) for n in range(len(sizes))]
    return [(s, n) for s, n in zip(starts, sizes)]


def plane_kernel(h_in, w_in, ids_in, mask_in, head_out, hid_out, loss_out, h_all, w_all, w_over, ids_own, mask_own,
                 code_own, code_got, code_all,
                 logits, expo, delta, stat_own, stat_all, loss_one, loss_two, loss_all, loss_zs,
                 grad_own, held, grad_send, far_in, r_in, part, core_in, x_out, x_in, y_out, y_in, *sems):
    (own_sem, hs, hr, ws, wr, wys, cs, cr, ss, sr, ls, lr, ms, mr,
     es, er, rs, rr, nr, fr, ds, dr, xs, xr, ys, yr) = sems
    nz, ny, nv = 4, 2, 4
    nb = nz * ny
    rows, width = h_in.shape
    cols, half = w_in.shape[0], w_in.shape[1] // ny
    piece = cols // 2
    group = ny * nv
    tokens = rows * group
    slab = ny * cols
    shift, lo = cols % 128, cols - cols % 128
    win = -(-(cols + shift) // 128) * 128
    b, v = lax.axis_index("batch"), lax.axis_index("vocab")
    z, y = lax.div(b, ny), lax.rem(b, ny)
    x, core = lax.div(v, 2), lax.rem(v, 2)
    me = y * nv + v
    low = z * 2 < nz
    at_end = (z == 0) | (z == nz - 1)
    inside = jnp.logical_not(at_end)

    def flip(a, k):
        return 1 - a if k else a

    def copy(src, dst, send, recv, bb, vv):
        return pltpu.make_async_remote_copy(
            src_ref=src, dst_ref=dst, send_sem=send, recv_sem=recv,
            device_id={"batch": bb, "vocab": vv}, device_id_type=MESH)

    def hrow(i):
        return pl.ds(pl.multiple_of(i * rows, 16), rows)

    over_x, over_y, over_core = (1 - x) * 2 + core, z * ny + 1 - y, x * 2 + 1 - core
    peers = [(ky, kx, kc) for ky in range(2) for kx in range(2) for kc in range(2) if ky or kx or kc]

    def peer(n):
        ky, kx, kc = peers[n]
        yy, vv = flip(y, ky), flip(x, kx) * 2 + flip(core, kc)
        return z * ny + yy, vv, yy * nv + vv

    def z_peer(k):
        return lax.rem(z + k, nz) * ny + y

    barrier = pltpu.get_barrier_semaphore()
    for k in range(1, nz):
        pl.semaphore_signal(barrier, inc=1, device_id={"batch": z_peer(k), "vocab": v}, device_id_type=MESH)
    for n in range(len(peers)):
        bb, vv, _ = peer(n)
        pl.semaphore_signal(barrier, inc=1, device_id={"batch": bb, "vocab": vv}, device_id_type=MESH)
    first = pl.ds(pl.multiple_of(y * half, 128), half)
    second = pl.ds(pl.multiple_of((1 - y) * half, 128), half)
    local = [
        pltpu.make_async_copy(w_in.at[:, second], w_over, own_sem.at[0]),
        pltpu.make_async_copy(w_in.at[:, first], w_all.at[pl.ds(pl.multiple_of(b * cols, 16), cols)], own_sem.at[1]),
        pltpu.make_async_copy(ids_in, ids_own, own_sem.at[2]),
        pltpu.make_async_copy(mask_in, mask_own, own_sem.at[3]),
        pltpu.make_async_copy(h_in, h_all.at[hrow(me)], own_sem.at[4]),
    ]
    for one in local:
        one.start()
    for one in local:
        one.wait()
    code = jnp.where(mask_own[...] != 0, ids_own[...], -1).astype(f32)
    code_own[...] = jnp.broadcast_to(code, code_own.shape)
    pl.semaphore_wait(barrier, nz - 1 + len(peers))

    def w_ref(i, h):
        return w_all.at[pl.ds(pl.multiple_of(i * cols + h * piece, 16), piece)]

    def w_z(i, h, up):
        return copy(w_ref(i, h), w_ref(i, h), ws.at[0 if up else 1],
                    wr.at[i, h], b + ny if up else b - ny, v)

    def w_pass(i, h, up):
        return copy(w_ref(i, h), w_ref(i, h), ws.at[jnp.where(up, 0, 1)], wr.at[i, h], jnp.where(up, b + ny, b - ny), v)

    def w_y(h):
        return copy(w_over.at[pl.ds(h * piece, piece)], w_ref(b, h), wys.at[0], wr.at[b, h], over_y, v)

    def w_got(i, h):
        copy(w_ref(i, h), w_ref(i, h), wys.at[0], wr.at[i, h], over_y, v).wait_recv()

    has_up, has_down = z + 1 < nz, z >= 1
    near = z + 1 - 2 * lax.rem(z, 2)
    slabs = [z, near, jnp.where(low, 2, 1), jnp.where(low, 3, 0)]

    def h_send(i, bb, vv):
        return copy(h_all.at[hrow(i)], h_all.at[hrow(i)], hs.at[0], hr.at[i], bb, vv)

    def h_x():
        return h_send(me, b, over_x)

    def h_y():
        return h_send(me, over_y, v)

    def h_xy():
        return h_send(y * nv + over_x, over_y, v)

    def h_yx():
        return h_send((1 - y) * nv + v, b, over_x)

    def h_core(kx, ky):
        i = flip(y, ky) * nv + flip(x, kx) * 2 + core
        return h_send(i, b, over_core)

    def h_got(kx, ky, cc):
        i = flip(y, ky) * nv + flip(x, kx) * 2 + cc
        h_send(i, b, over_core).wait_recv()

    def code_copy(n):
        bb, vv, _ = peer(n)
        return copy(code_own, code_got.at[me], cs.at[0], cr.at[0], bb, vv)

    for h in range(2):
        w_y(h).start()
    for h in range(2):
        pl.when(has_up)(lambda: w_z(b, h, True).start())
        pl.when(has_down)(lambda: w_z(b, h, False).start())
    h_x().start()
    h_y().start()
    for n in range(len(peers)):
        code_copy(n).start()
    h_core(0, 0).start()
    for h in range(2):
        i = z * ny + 1 - y
        w_got(i, h)
        pl.when(has_up)(lambda: w_z(i, h, True).start())
        pl.when(has_down)(lambda: w_z(i, h, False).start())

    def w_slab(zz, onward, which=(0, 1)):
        for k in which:
            for h in range(2):
                i = zz * ny + flip(y, k)
                w_got(i, h)
                if onward:
                    w_pass(i, h, zz < z).start()

    @pl.when(at_end)
    def _():
        w_slab(slabs[1], False)

    @pl.when(inside)
    def _():
        w_slab(slabs[1], True)
        w_slab(slabs[2], True)

    h_got(1, 0, core)
    pl.when(core == 0)(lambda: h_xy().start())
    h_core(1, 0).start()
    h_got(0, 1, core)
    pl.when(core == 1)(lambda: h_yx().start())
    h_core(0, 1).start()

    @pl.when(at_end)
    def _():
        w_slab(slabs[2], False)

    @pl.when(inside)
    def _():
        w_slab(slabs[3], True)

    code_got[me] = code_own[...]
    others = pl.ds(0, group - 1)
    copy(code_got.at[others], code_got.at[others], cs.at[0], cr.at[0], b, over_x).wait_recv()
    for i in range(group):
        code_all[i * rows:(i + 1) * rows, :] = jnp.transpose(jnp.concatenate([code_got[i]] * (rows // 8), axis=0))

    h_got(1, 1, core)
    h_core(1, 1).start()
    for kx in range(2):
        for ky in range(2):
            h_got(kx, ky, 1 - core)

    step = 2 * rows
    steps = tokens // step
    lines = lax.broadcasted_iota(jnp.int32, (8, rows), 0)

    def scores(n, zz, at=0, wide=slab):
        here = pl.ds(pl.multiple_of(zz * slab + at, 128), wide)
        there = pl.ds(pl.multiple_of(zz * slab + at, 16), wide)
        return jnp.dot(h_all[n * step:(n + 1) * step, here], w_all[there, :], preferred_element_type=f32)

    for j in range(nz - 1):
        for n in range(steps):
            span = pl.ds(n * step, step)
            if j:
                logits[span, :] += scores(n, slabs[j])
            else:
                logits[span, :] = scores(n, slabs[j])

    early = lo
    pl.when(at_end)(lambda: w_slab(slabs[3], False, (0,)))
    for n in range(steps):
        logits[n * step:(n + 1) * step, :] += scores(n, slabs[3], y * (slab - early), early)
    pl.when(at_end)(lambda: w_slab(slabs[3], False, (1,)))

    sums = jnp.zeros((8, rows), f32)
    for n in range(steps):
        span = pl.ds(n * step, step)
        capped = softcap * jnp.tanh((logits[span, :] + scores(n, slabs[3], (1 - y) * early, slab - early)) * (1.0 / softcap))
        raised = jnp.exp(capped)
        logits[span, :] = capped
        expo[span, :] = raised
        total = jnp.broadcast_to(jnp.sum(raised, axis=1, keepdims=True), (step, 128))
        for k in range(2):
            turned = jnp.transpose(total[k * rows:(k + 1) * rows])
            sums = jnp.where(lines == 2 * n + k, turned[0:8], sums)
    stat_own[...] = sums

    def stat_copy(n):
        bb, vv, _ = peer(n)
        return copy(stat_own, stat_all.at[me], ss.at[0], sr.at[0], bb, vv)

    for n in range(len(peers)):
        stat_copy(n).start()

    ids = (lax.broadcasted_iota(jnp.int32, (step, half), 1) + (v * ny + y) * half).astype(f32)
    hit_total = jnp.zeros((step, 1), f32)
    for n in range(steps):
        span = pl.ds(n * step, step)
        capped = logits[span, :]
        hit = ids == code_all[span, 0:1]
        slope = 1.0 - (capped * (1.0 / softcap)) ** 2
        expo[span, :] = expo[span, :] * slope
        logits[span, :] = jnp.where(hit, slope, 0.0)
        hit_total = hit_total + jnp.sum(jnp.where(hit, capped, 0.0), axis=1, keepdims=True)
    hit_total = jnp.sum(hit_total, axis=0, keepdims=True)
    loss_one[...] = jnp.broadcast_to(hit_total, loss_one.shape)

    def hit_copy(n):
        bb, vv, _ = peer(n)
        return copy(loss_one, loss_all.at[me], ls.at[0], lr.at[0], bb, vv)

    for n in range(len(peers)):
        hit_copy(n).start()
    code_rows = jnp.zeros((8, rows), f32)
    for i in range(group):
        code_rows = jnp.where(lines == i, code_got[i], code_rows)
    weight = (code_rows >= 0).astype(f32)

    stat_all[me] = sums
    copy(stat_all.at[others], stat_all.at[others], ss.at[0], sr.at[0], b, over_x).wait_recv()
    partition = stat_all[0]
    for i in range(1, group):
        partition = partition + stat_all[i]
    scale = weight / partition

    def delta_copy(n):
        span = pl.ds(n * step, step)
        return copy(delta.at[0, span], delta.at[1, span], es.at[0], er.at[0], over_y, v)

    for n in range(steps):
        for k in range(2):
            i = 2 * n + k
            span = pl.ds(i * rows, rows)
            by_row = jnp.transpose(jnp.broadcast_to(scale[i:i + 1, :], (rows, rows)))
            factor = jnp.concatenate([by_row] * (half // rows), axis=1)
            delta[0, span, :] = (expo[span, :] * factor - logits[span, :]).astype(bf16)
        delta_copy(n).start()

    near_end = jnp.where(low, 1, 2)
    far = jnp.where(low, nz - 1, 0)
    across = jnp.where(low, 2, 1)
    targets = [jnp.where(at_end, far, across), jnp.where(at_end, across, near), jnp.where(at_end, near_end, far), z]
    top = y * shift

    def grad_share(zz, r, first, wide):
        here = pl.ds(pl.multiple_of(zz * slab + y * lo, 128), win)
        return lax.dot_general(h_all[:, here], delta[r, :, first:first + wide], (((0,), (0,)), ((), ())), preferred_element_type=f32)

    def sent(k, r):
        return grad_send.at[k, r, pl.ds(pl.multiple_of(top, 16), cols)]

    def r_copy(k, r):
        return copy(sent(k, r), r_in.at[z, r], rs.at[0], rr.at[z, r], targets[k] * ny + y, v)

    def far_copy(r):
        return copy(sent(0, r), far_in.at[r], rs.at[0], fr.at[r], near_end * ny + y, v)

    bounds = [(0, 128), (128, half - 128)]

    def far_part(n):
        here = pl.ds(*bounds[n])
        return copy(grad_send.at[0, 0, pl.ds(pl.multiple_of(top, 16), cols), here], far_in.at[0, :, here],
                    rs.at[0], fr.at[(0, 2)[n]], near_end * ny + y, v)

    def cross_copy():
        return copy(sent(1, 1), far_in.at[2], rs.at[0], fr.at[3], near_end * ny + y, v)

    def near_copy(r, h):
        src = grad_send.at[2, r, pl.ds(pl.multiple_of(top + h * piece, 16), piece)]
        return copy(src, r_in.at[z, r, pl.ds(h * piece, piece)], rs.at[0], nr.at[r, h], near_end * ny + y, v)

    def first_piece():
        for n in range(2):
            first, wide = bounds[n]
            grad_send[0, 0, :, first:first + wide] = grad_share(targets[0], 0, first, wide).astype(bf16)
            pl.when(at_end)(lambda: far_part(n).start())
        pl.when(inside)(lambda: r_copy(0, 0).start())

    def head_piece(k, r):
        share = grad_share(targets[k], r, 0, half)
        if k == nz - 1:
            grad_own[r] = share
        elif k == 2:
            @pl.when(at_end)
            def _():
                grad_send[k, r] = share.astype(bf16)
                near_copy(r, 0).start()
                if r:
                    near_copy(0, 1).start()
                    near_copy(1, 1).start()

            @pl.when(inside)
            def _():
                held[r] = share
        elif k == 0:
            @pl.when(at_end)
            def _():
                grad_send[k, r] = share.astype(bf16)
                far_copy(r).start()

            @pl.when(inside)
            def _():
                held[2] = share
        else:
            grad_send[k, r] = share.astype(bf16)
            if r:
                pl.when(at_end)(lambda: cross_copy().start())
                pl.when(inside)(lambda: r_copy(k, r).start())
            else:
                r_copy(k, r).start()

    cstep = chunk_of(cols, 64)

    def over_cols(body):
        def one(n, carry):
            body(pl.multiple_of(n * cstep, 16))
            return carry

        lax.fori_loop(0, cols // cstep, one, 0)

    def relay(k, r, slot):
        @pl.when(inside)
        def _():
            if r == 0:
                for n in range(2):
                    far_part(n).wait_recv()
            elif k:
                far_copy(r).wait_recv()
            else:
                cross_copy().wait_recv()

            def add(n):
                here = pl.ds(pl.multiple_of(top + n, 16), cstep)
                there = pl.ds(n, cstep)
                grad_send[k, r, here, :] = (held[slot, here, :] + far_in[slot, there, :].astype(f32)).astype(bf16)

            over_cols(add)
            r_copy(k, r).start()

    groups = column_groups(width)
    blocks = [(1, 1), (1, 0), (0, 1), (0, 0)]
    unit = width // (width // 256)

    def span_of(g):
        first, n = groups[g]
        return pl.ds(first * unit, n * unit)

    y_first = (3,)

    def block(g, one, two, cc):
        kx, ky = (two, one) if g in y_first else (one, two)
        return flip(y, ky) * nv + flip(x, kx) * 2 + cc

    def core_copy(g, one, two):
        return copy(part.at[hrow(block(g, one, two, 1 - core)), span_of(g)], core_in.at[one, two, :, span_of(g)],
                    ds.at[0], dr.at[g], b, over_core)

    def over_one(g):
        return (over_y, v) if g in y_first else (b, over_x)

    def over_two(g):
        return (b, over_x) if g in y_first else (over_y, v)

    def one_copy(g, two):
        return copy(x_out.at[two, :, span_of(g)], x_in.at[two, :, span_of(g)], xs.at[0], xr.at[g, two],
                    *over_one(g))

    def two_copy(g):
        return copy(y_out.at[:, span_of(g)], y_in.at[:, span_of(g)], ys.at[0], yr.at[g], *over_two(g))

    def part_group(g):
        first, n = groups[g]

        def columns(j, carry):
            span = pl.ds(pl.multiple_of(j * unit, 128), unit)
            part[:, span] = lax.dot_general(
                delta[0], w_all[span, :], (((1,), (1,)), ((), ())), preferred_element_type=f32)
            return carry

        lax.fori_loop(first, first + n, columns, 0)
        for one, two in blocks:
            core_copy(g, one, two).start()

    hstep = 16

    def over_rows(body):
        def one(n, carry):
            body(pl.multiple_of(n * hstep, hstep))
            return carry

        lax.fori_loop(0, rows // hstep, one, 0)

    def core_sum(g):
        span = span_of(g)
        landed = core_in.at[:, :, :, span]
        copy(landed, landed, ds.at[0], dr.at[g], b, over_core).wait_recv()
        for one, two in blocks:
            start = block(g, one, two, core) * rows

            def add(n):
                here = pl.ds(pl.multiple_of(start + n, hstep), hstep)
                both = part[here, span] + core_in[one, two, pl.ds(n, hstep), span]
                if one:
                    x_out[two, pl.ds(n, hstep), span] = both.astype(bf16)
                else:
                    part[here, span] = both

            over_rows(add)
            if one:
                one_copy(g, two).start()

    def one_sum(g):
        span = span_of(g)
        for two in (1, 0):
            one_copy(g, two).wait_recv()
            start = block(g, 0, two, core) * rows

            def add(n):
                here = pl.ds(pl.multiple_of(start + n, hstep), hstep)
                total = part[here, span] + x_in[two, pl.ds(n, hstep), span].astype(f32)
                if two:
                    y_out[pl.ds(n, hstep), span] = total.astype(bf16)
                else:
                    hid_out[pl.ds(n, hstep), span] = total

            over_rows(add)
            if two:
                two_copy(g).start()

    def two_sum(g):
        span = span_of(g)
        two_copy(g).wait_recv()

        def add(n):
            here = pl.ds(n, hstep)
            hid_out[here, span] += y_in[here, span].astype(f32)

        over_rows(add)

    count = len(groups)

    def plane_copy(k):
        return copy(loss_two, loss_zs.at[z], ms.at[0], mr.at[0], z_peer(k), v)

    def plane_loss():
        loss_all[me] = loss_one[...]
        copy(loss_all.at[others], loss_all.at[others], ls.at[0], lr.at[0], b, over_x).wait_recv()
        hits = loss_all[0]
        for i in range(1, group):
            hits = hits + loss_all[i]
        logs = jnp.sum(weight * jnp.log(partition), axis=1, keepdims=True)
        loss_two[...] = jnp.broadcast_to(jnp.sum(logs, axis=0, keepdims=True), (8, rows)) - hits
        for k in range(1, nz):
            plane_copy(k).start()

    first_piece()
    part_group(0)
    part_group(1)
    plane_loss()
    core_sum(0)
    part_group(2)
    core_sum(1)
    head_piece(1, 0)
    part_group(3)
    core_sum(2)
    head_piece(2, 0)
    relay(2, 0, 0)
    for g in range(4, count):
        part_group(g)
        core_sum(g - 1)
    core_sum(count - 1)
    head_piece(3, 0)
    one_sum(0)

    whole_delta = copy(delta.at[0], delta.at[1], es.at[0], er.at[0], over_y, v)
    whole_delta.wait_recv()
    head_piece(0, 1)
    head_piece(1, 1)
    one_sum(1)
    head_piece(2, 1)
    head_piece(3, 1)
    one_sum(2)
    relay(2, 1, 1)

    copy(w_over, w_over, wys.at[0], wr.at[0, 0], over_y, v).wait_send()
    for n in range(1, nz):
        sent_rows = w_all.at[pl.ds(0, n * slab)]
        for way, slabs_sent in ((0, z + 1), (1, nz - z)):
            going = (slabs_sent == n) & (has_down if way else has_up)
            pl.when(going)(lambda: copy(sent_rows, sent_rows, ws.at[way], wr.at[0, 0], b, over_x).wait_send())
    seven = h_all.at[pl.ds(0, 7 * rows)]
    copy(seven, seven, hs.at[0], hr.at[0], b, over_x).wait_send()
    for got, sem in ((code_got, cs), (stat_all, ss), (loss_all, ls)):
        copy(got.at[others], got.at[others], sem.at[0], sem.at[0], b, over_x).wait_send()
    one_sum(3)
    two_sum(0)
    whole_delta.wait_send()
    copy(core_in, core_in, ds.at[0], dr.at[0], b, over_core).wait_send()
    one_sum(4)
    two_sum(1)
    two_sum(2)
    relay(0, 1, 2)
    for g in range(5, count):
        one_sum(g)
        two_sum(g - 2)

    def r_got(zz, r):
        copy(r_in.at[zz, r], r_in.at[zz, r], rs.at[0], rr.at[zz, r], z_peer(1), v).wait_recv()

    def lanes(r):
        return pl.ds(pl.multiple_of(flip(y, r) * half, 128), half)

    sources = [near, jnp.where(low, 2, 1), far]

    def head_sum(r):
        @pl.when(at_end)
        def _():
            r_got(sources[0], r)

        @pl.when(inside)
        def _():
            for h in range(2):
                mine = r_in.at[sources[0], r, pl.ds(h * piece, piece)]
                copy(mine, mine, rs.at[0], nr.at[r, h], near_end * ny + y, v).wait_recv()

        r_got(sources[1], r)

        def add(n):
            here = pl.ds(n, cstep)
            total = grad_own[r, pl.ds(pl.multiple_of(top + n, 16), cstep), :]
            for k in range(2):
                total = total + r_in[sources[k], r, here, :].astype(f32)
            head_out[here, lanes(r)] = total

        over_cols(add)

        @pl.when(inside)
        def _():
            if r:
                return
            r_got(sources[2], r)

            def last(n):
                here = pl.ds(n, cstep)
                head_out[here, lanes(r)] += r_in[sources[2], r, here, :].astype(f32)

            over_cols(last)

    head_sum(0)
    loss_zs[z] = loss_two[...]
    along = loss_zs.at[pl.ds(0, nz - 1)]
    copy(along, along, ms.at[0], mr.at[0], z_peer(1), v).wait_recv()
    losses = loss_zs[0]
    for i in range(1, nz):
        losses = losses + loss_zs[i]
    loss_out[...] = losses * (1.0 / (tokens * nz))
    copy(along, along, ms.at[0], mr.at[0], z_peer(1), v).wait_send()
    two_sum(count - 2)
    two_sum(count - 1)
    head_sum(1)

    for part_sent, sem in ((x_out, xs), (y_out, ys), (r_in.at[pl.ds(0, nz - 1)], rs)):
        copy(part_sent, part_sent, sem.at[0], sem.at[0], b, over_x).wait_send()


def finish_kernel(head_in, hid_in, loss_in, head_out, hid_out, loss_out, sem):
    parts = sem.shape[1]
    moves = []
    for k, (src, dst) in enumerate(((hid_in, hid_out), (head_in, head_out))):
        size = src.shape[0] // parts
        for n in range(parts):
            here = pl.ds(n * size, size)
            moves.append(pltpu.make_async_copy(src.at[here], dst.at[here], sem.at[k, n]))
    for one in moves:
        one.start()
    loss_out[0, 0] = loss_in[0, 0]
    for one in moves:
        one.wait()


def plane_local(hidden, head_weight, targets, valid_mask):
    nz, ny, nv = 4, 2, 4
    rows, width = hidden.shape
    entries, cols = head_weight.shape
    half = entries // ny
    group = ny * nv
    tokens = rows * group
    shift = cols % 128
    win = -(-(cols + shift) // 128) * 128
    vm = pltpu.VMEM
    dma = pltpu.SemaphoreType.DMA
    count = len(column_groups(width))
    line = vm((8, rows), f32)
    buffers = [
        vm((tokens, width), bf16), vm((width, half), bf16), vm((cols, half), bf16),
        vm((1, rows), jnp.int32), vm((1, rows), jnp.int32), line, vm((group, 8, rows), f32), vm((tokens, 128), f32),
        vm((tokens, half), f32), vm((tokens, half), f32), vm((2, tokens, half), bf16),
        line, vm((group, 8, rows), f32), line, line, vm((group, 8, rows), f32), vm((nz, 8, rows), f32),
        vm((2, win, half), f32), vm((3, win, half), f32), vm((3, 2, win, half), bf16),
        vm((3, cols, half), bf16), vm((nz, 2, cols, half), bf16),
        vm((tokens, width), f32), vm((2, 2, rows, width), f32),
        vm((2, rows, width), bf16), vm((2, rows, width), bf16), vm((rows, width), bf16), vm((rows, width), bf16),
    ]
    sems = [
        dma((5,)), dma((1,)), dma((group,)), dma((2,)), dma((8, 2)), dma((1,)),
        dma((1,)), dma((1,)), dma((1,)), dma((1,)), dma((1,)), dma((1,)), dma((1,)), dma((1,)),
        dma((1,)), dma((1,)), dma((1,)), dma((nz, 2)), dma((2, 2)), dma((4,)),
        dma((1,)), dma((count,)), dma((1,)), dma((count, 2)), dma((1,)), dma((count,)),
    ]
    whole = pl.BlockSpec(memory_space=vm)
    head_t, hidden_grad, loss = pl.pallas_call(
        plane_kernel,
        out_shape=(
            vm((cols, entries), f32),
            vm((rows, width), f32),
            vm((8, rows), f32),
        ),
        in_specs=[pl.BlockSpec(memory_space=pl.ANY)] * 4,
        out_specs=(whole,) * 3,
        scratch_shapes=buffers + sems,
        compiler_params=pltpu.CompilerParams(
            collective_id=1, has_side_effects=True, vmem_limit_bytes=58 * 1024 * 1024),
    )(hidden, jnp.transpose(head_weight), targets[None, :], valid_mask[None, :])
    anywhere = pl.BlockSpec(memory_space=pl.ANY)
    head_t, hidden_grad, loss = pl.pallas_call(
        finish_kernel,
        out_shape=(
            jax.ShapeDtypeStruct((cols, entries), f32),
            jax.ShapeDtypeStruct((rows, width), f32),
            jax.ShapeDtypeStruct((1, 1), f32),
        ),
        in_specs=[whole] * 3,
        out_specs=(anywhere, anywhere, pl.BlockSpec(memory_space=pltpu.SMEM)),
        scratch_shapes=[dma((2, 4))],
        compiler_params=pltpu.CompilerParams(vmem_limit_bytes=1024 * 1024),
    )(head_t, hidden_grad, loss)
    return jnp.transpose(head_t), hidden_grad, loss[0, 0]


def in_planes(nb, nv, hidden, head_weight, targets, valid_mask):
    rows, width = hidden.shape
    entries, cols = head_weight.shape
    fits = nb == 8 and nv == 4 and rows == 128 and width % 256 == 0 and width >= 2048
    return fits and entries % 256 == 0 and entries >= 512 and cols % 32 == 0 and (2 * cols) % 128 == 0


def device(nb, nv, *arrays):
    if in_planes(nb, nv, *arrays):
        return plane_local(*arrays)
    return local(nb, nv, *arrays)


def solution(mesh):
    placed = (
        P(("batch", "vocab"), None),
        P("vocab", "batch"),
        P(("batch", "vocab")),
        P(("batch", "vocab")),
    )
    return jax.shard_map(
        functools.partial(device, mesh.shape["batch"], mesh.shape["vocab"]),
        mesh=mesh,
        in_specs=placed,
        out_specs=(P("vocab", "batch"), P(("batch", "vocab"), None), P()),
        check_vma=False,
    )
```

```python
import functools

import jax
import jax.numpy as jnp
from jax import lax
from jax.experimental import pallas as pl
from jax.experimental.pallas import tpu as pltpu
from jax.sharding import PartitionSpec as P

softcap = 30.0
MESH = pl.DeviceIdType.MESH
f32, bf16 = jnp.float32, jnp.bfloat16


def chunk_of(length, most):
    return max(s for s in range(16, most + 1, 16) if length % s == 0)


def kernel(sizes, h_in, w_in, code_in, head_out, hid_out, loss_out, h_all, w_all, code_got, code_all,
           logits, delta, stat_own, stat_all, loss_own, loss_all, grad, grad_send, r_in,
           part, core_in, x_out, x_in, y_out, y_in, far_own, far_in, *sems):
    nz, ny, nx, nv = sizes
    (own_sem, hs, hf, hd, hr, ws_up, ws_dn, ws_y, wr, cs, cr, ss, sr, ls, lr,
     rs, rr, ds, dr, xs, xr, ys, yr, fs, fr) = sems
    nb = nz * ny
    rows, width = h_in.shape
    cols, half = w_in.shape[1:]
    group = ny * nv
    tokens = rows * group
    entries = ny * half
    b, v = lax.axis_index("batch"), lax.axis_index("vocab")
    z, y = lax.div(b, ny), lax.rem(b, ny)
    x, core = lax.div(v, 2), lax.rem(v, 2)
    other = x * 2 + 1 - core
    me = y * nv + v

    def at(bb, vv):
        return {"batch": bb, "vocab": vv}

    def copy(src, dst, send, recv, bb, vv):
        return pltpu.make_async_remote_copy(
            src_ref=src, dst_ref=dst, send_sem=send, recv_sem=recv, device_id=at(bb, vv), device_id_type=MESH)

    def hrow(i):
        return pl.ds(pl.multiple_of(i * rows, 16), rows)

    def wrow(i):
        return pl.ds(pl.multiple_of(i * cols, 16), cols)

    def turn_y(k):
        return lax.rem(y + k, ny)

    def turn_x(k):
        return lax.rem(x + k, nx)

    peers = [(k, j) for k in range(ny) for j in range(nv) if k or j]

    def peer(n):
        k, j = peers[n]
        return z * ny + turn_y(k), lax.rem(v + j, nv), turn_y(k) * nv + lax.rem(v + j, nv)

    barrier = pltpu.get_barrier_semaphore()
    for k in range(1, nb):
        pl.semaphore_signal(barrier, inc=1, device_id=at(lax.rem(b + k, nb), v), device_id_type=MESH)
    met = [n for n in range(len(peers)) if peers[n][1]]
    for n in met:
        bb, vv, _ = peer(n)
        pl.semaphore_signal(barrier, inc=1, device_id=at(bb, vv), device_id_type=MESH)
    pl.semaphore_wait(barrier, nb - 1 + len(met))

    def w_z(zz, yy, up, own=False):
        i = zz * ny + yy
        dst = w_all.at[wrow(i)]
        sem = (ws_up if up else ws_dn).at[i]
        return copy(w_in.at[y] if own else dst, dst, sem, wr.at[i], b + ny if up else b - ny, v)

    def w_y(k):
        return copy(w_in.at[turn_y(k)], w_all.at[wrow(b)], ws_y.at[k - 1], wr.at[b], z * ny + turn_y(k), v)

    def w_got(zz, yy):
        w_z(zz, yy, True).wait_recv()

    has_up, has_down = z + 1 < nz, z >= 1

    def h_send(n_src, sem, bb, vv, own=False):
        dst = h_all.at[hrow(n_src)]
        return copy(h_in if own else dst, dst, sem, hr.at[n_src], bb, vv)

    def h_x(k):
        return h_send(me, hs.at[k - 1], b, turn_x(k) * 2 + core, True)

    def h_y(k):
        return h_send(me, hs.at[nx + k - 1], z * ny + turn_y(k), v, True)

    def h_xy(kx, ky):
        return h_send(y * nv + turn_x(kx) * 2 + core, hf.at[kx, ky], z * ny + turn_y(ky), v)

    def h_yx(kx, ky):
        return h_send(turn_y(ky) * nv + v, hf.at[kx, ky], b, turn_x(kx) * 2 + core)

    def h_core(kx, ky):
        i = turn_y(ky) * nv + turn_x(kx) * 2 + core
        return h_send(i, hd.at[kx, ky], b, other, kx == 0 and ky == 0)

    def h_got(kx, ky, cc):
        i = turn_y(ky) * nv + turn_x(kx) * 2 + cc
        h_send(i, hd.at[kx, ky], b, other).wait_recv()

    def code_copy(n):
        bb, vv, _ = peer(n)
        return copy(code_in, code_got.at[me], cs.at[n], cr.at[me], bb, vv)

    for k in range(1, ny):
        w_y(k).start()
    pl.when(has_up)(lambda: w_z(z, y, True, True).start())
    pl.when(has_down)(lambda: w_z(z, y, False, True).start())
    for k in range(1, nx):
        h_x(k).start()
    for k in range(1, ny):
        h_y(k).start()
    for n in range(len(peers)):
        code_copy(n).start()
    h_core(0, 0).start()
    local = [
        pltpu.make_async_copy(w_in.at[y], w_all.at[wrow(b)], own_sem.at[0]),
        pltpu.make_async_copy(h_in, h_all.at[hrow(me)], own_sem.at[1]),
    ]
    for one in local:
        one.start()

    for k in range(1, ny):
        w_got(z, turn_y(k))
        pl.when(has_up)(lambda: w_z(z, turn_y(k), True).start())
        pl.when(has_down)(lambda: w_z(z, turn_y(k), False).start())

    def h_pass():
        for kx in range(1, nx):
            h_got(kx, 0, core)
            for ky in range(1, ny):
                pl.when(core == 0)(lambda: h_xy(kx, ky).start())
            h_core(kx, 0).start()
        for ky in range(1, ny):
            h_got(0, ky, core)
            for kx in range(1, nx):
                pl.when(core == 1)(lambda: h_yx(kx, ky).start())
            h_core(0, ky).start()

    def h_rest():
        for kx in range(1, nx):
            for ky in range(1, ny):
                h_got(kx, ky, core)
                h_core(kx, ky).start()

    for k in range(1, nz):
        for j in range(ny):
            yy = turn_y(j)

            @pl.when(z - k >= 0)
            def _():
                w_got(z - k, yy)
                pl.when(has_up)(lambda: w_z(z - k, yy, True).start())

            @pl.when(z + k < nz)
            def _():
                w_got(z + k, yy)
                pl.when(has_down)(lambda: w_z(z + k, yy, False).start())
        if k == 1:
            h_pass()
        if k == min(2, nz - 1):
            h_rest()

    for one in local:
        one.wait()
    for kx in range(nx):
        for ky in range(ny):
            h_got(kx, ky, 1 - core)
    code_got[me] = code_in[...]
    for n in range(len(peers)):
        bb, vv, i = peer(n)
        copy(code_in, code_got.at[i], cs.at[n], cr.at[i], bb, vv).wait_recv()
    for i in range(group):
        code_all[i * rows:(i + 1) * rows, :] = jnp.transpose(jnp.concatenate([code_got[i]] * 16, axis=0))

    step = chunk_of(tokens, 256)
    lanes = lax.broadcasted_iota(jnp.int32, (step, 128), 1)
    first = v * entries + y * half

    def span_of(n):
        return pl.ds(pl.multiple_of(n * step, step), step)

    def hits(n):
        ids = lax.broadcasted_iota(jnp.int32, (step, half), 1) + first
        return ids == code_all[span_of(n), 0:1].astype(jnp.int32)

    for n in range(tokens // step):
        span = pl.ds(n * step, step)
        scores = jnp.dot(h_all[span, :], w_all[...], preferred_element_type=f32)
        capped = softcap * jnp.tanh(scores * (1.0 / softcap))
        logits[span, :] = capped
        total = jnp.sum(jnp.exp(capped), axis=1, keepdims=True)
        hit_sum = jnp.sum(jnp.where(hits(n), capped, 0.0), axis=1, keepdims=True)
        turned = jnp.transpose(jnp.where(lax.rem(lanes, 8) < 4, total, hit_sum))
        stat_own[:, n * step:(n + 1) * step] = turned[0:8]

    def stat_copy(n):
        bb, vv, _ = peer(n)
        return copy(stat_own, stat_all.at[me], ss.at[n], sr.at[me], bb, vv)

    for n in range(len(peers)):
        stat_copy(n).start()
    for n in range(len(peers)):
        bb, vv, i = peer(n)
        copy(stat_own, stat_all.at[i], ss.at[n], sr.at[i], bb, vv).wait_recv()
    stats = stat_own[...]
    for n in range(len(peers)):
        stats = stats + stat_all[peer(n)[2]]

    loss = jnp.zeros((1, 1), f32)
    for n in range(tokens // step):
        span = pl.ds(n * step, step)
        weight = (code_all[span, 0:1] >= 0).astype(f32)
        back = jnp.transpose(jnp.concatenate([stats[:, n * step:(n + 1) * step]] * 16, axis=0))
        partition, target_logit = back[:, 0:1], back[:, 4:5]
        loss = loss + jnp.sum(weight * (jnp.log(partition) - target_logit), axis=0, keepdims=True)
        capped = logits[span, :]
        slope = 1.0 - (capped * (1.0 / softcap)) ** 2
        delta[span, :] = ((jnp.exp(capped) * (weight / partition) - jnp.where(hits(n), weight, 0.0)) * slope
                          ).astype(bf16)
    loss_own[...] = jnp.broadcast_to(loss, loss_own.shape)

    def loss_copy(k):
        return copy(loss_own, loss_all.at[b], ls.at[k - 1], lr.at[b], lax.rem(b + k, nb), v)

    def r_copy(zz, yy):
        i = zz * ny + yy
        return copy(grad_send.at[wrow(i)], r_in.at[z, y], rs.at[i], rr.at[b], i, v)

    def grad_share(span):
        return lax.dot_general(h_all[:, span], delta[...], (((0,), (0,)), ((), ())), preferred_element_type=f32)

    slab = ny * cols
    relay = nz == 4 and slab % 128 == 0
    turn = jnp.where(z * 2 >= nz, 1, nz - 1)
    order = [lax.rem(z + turn * k, nz) for k in range(1, nz)] + [z]
    at_end = (z == 0) | (z == nz - 1)
    far = jnp.where(z * 2 >= nz, 0, nz - 1)
    near = jnp.where(z * 2 >= nz, z - 1, z + 1)

    def far_copy(yy):
        return copy(grad_send.at[wrow(far * ny + yy)], far_in.at[yy], fs.at[yy], fr.at[yy], near * ny + y, v)

    def direct(zz):
        return jnp.logical_not(at_end & (zz == far))
    if slab % 128 == 0:
        mine = y * cols
        for n in range(nz):
            zz = order[n]
            span = pl.ds(pl.multiple_of(zz * slab, 128), slab)
            share = grad_share(span)
            held = relay and n == 1
            if n == nz - 1:
                grad[...] = share
            if held:
                @pl.when(jnp.logical_not(at_end))
                def _():
                    far_own[...] = share

                @pl.when(at_end)
                def _():
                    grad_send[span, :] = share.astype(bf16)
                    for k in range(ny):
                        r_copy(zz, turn_y(k)).start()
            else:
                grad_send[span, :] = share.astype(bf16)
                for k in range(ny):
                    yy = turn_y(k)
                    if relay and n == 0:
                        pl.when(at_end)(lambda: far_copy(yy).start())
                        pl.when(jnp.logical_not(at_end))(lambda: r_copy(zz, yy).start())
                    elif n < nz - 1 or k:
                        r_copy(zz, yy).start()
    else:
        mine = b * cols
        wide = chunk_of(width, 256)

        def grad_step(j, carry):
            span = pl.ds(pl.multiple_of(j * wide, wide), wide)
            share = grad_share(span)
            grad[span, :] = share
            grad_send[span, :] = share.astype(bf16)
            return carry

        lax.fori_loop(0, width // wide, grad_step, 0)
        for n in range(nz):
            for k in range(ny):
                if n < nz - 1 or k:
                    r_copy(order[n], turn_y(k)).start()
    for k in range(1, nb):
        loss_copy(k).start()

    wide = chunk_of(width, 256)

    def part_step(j, carry):
        span = pl.ds(pl.multiple_of(j * wide, wide), wide)
        part[:, span] = lax.dot_general(
            delta[...], w_all[span, :], (((1,), (1,)), ((), ())), preferred_element_type=f32)
        return carry

    lax.fori_loop(0, width // wide, part_step, 0)

    def core_copy(kx, ky):
        i = turn_y(ky) * nv + turn_x(kx) * 2 + 1 - core
        return copy(part.at[hrow(i)], core_in.at[kx, ky], ds.at[kx, ky], dr.at[kx, ky], b, other)

    def x_copy(kx, ky):
        return copy(x_out.at[kx - 1, ky], x_in.at[kx - 1, ky], xs.at[kx, ky], xr.at[kx, ky],
                    b, turn_x(kx) * 2 + core)

    def y_copy(ky):
        return copy(y_out.at[ky - 1], y_in.at[ky - 1], ys.at[ky], yr.at[ky], z * ny + turn_y(ky), v)

    ways = [(kx % nx, ky % ny) for kx in range(1, nx + 1) for ky in range(1, ny + 1)]
    for kx, ky in ways:
        core_copy(kx, ky).start()
    hstep = 16

    def over_rows(start, body):
        def one(r, carry):
            body(pl.ds(pl.multiple_of(r * hstep, hstep), hstep),
                 pl.ds(pl.multiple_of(start + r * hstep, hstep), hstep))
            return carry

        lax.fori_loop(0, rows // hstep, one, 0)

    def start_of(kx, ky):
        return (turn_y(ky) * nv + turn_x(kx) * 2 + core) * rows

    for kx, ky in ways:
        core_copy(kx, ky).wait_recv()

        def core_sum(span, here):
            both = part[here, :] + core_in[kx, ky, span, :]
            if kx:
                x_out[kx - 1, ky, span, :] = both.astype(bf16)
            else:
                part[here, :] = both

        over_rows(start_of(kx, ky), core_sum)
        if kx:
            x_copy(kx, ky).start()

    cstep = chunk_of(cols, 64)

    def over_cols(body):
        def one(r, carry):
            body(pl.multiple_of(r * cstep, 16))
            return carry

        lax.fori_loop(0, cols // cstep, one, 0)

    if relay:
        @pl.when(jnp.logical_not(at_end))
        def _():
            for k in range(ny):
                yy = turn_y(k)
                far_copy(yy).wait_recv()

                def far_sum(r):
                    here = pl.ds(pl.multiple_of(yy * cols + r, 16), cstep)
                    there = pl.ds(pl.multiple_of((far * ny + yy) * cols + r, 16), cstep)
                    grad_send[there, :] = (far_own[here, :] + far_in[yy, pl.ds(r, cstep), :].astype(f32)).astype(bf16)

                over_cols(far_sum)
                r_copy(far, yy).start()

    for ky in [k % ny for k in range(1, ny + 1)]:
        for kx in range(1, nx):
            x_copy(kx, ky).wait_recv()

        def x_sum(span, here):
            total = part[here, :]
            for kx in range(1, nx):
                total = total + x_in[kx - 1, ky, span, :].astype(f32)
            if ky:
                y_out[ky - 1, span, :] = total.astype(bf16)
            else:
                hid_out[span, :] = total

        over_rows(start_of(0, ky), x_sum)
        if ky:
            y_copy(ky).start()

    def r_got(zz, yy):
        i = zz * ny + yy
        copy(grad_send.at[wrow(i)], r_in.at[zz, yy], rs.at[i], rr.at[i], i, v).wait_recv()

    for k in range(1, ny):
        r_got(z, turn_y(k))

    def first_sum(r):
        head_out[y, pl.ds(r, cstep), :] = grad[pl.ds(pl.multiple_of(mine + r, 16), cstep), :]
        for k in range(1, ny):
            head_out[turn_y(k), pl.ds(r, cstep), :] = r_in[z, turn_y(k), pl.ds(r, cstep), :].astype(f32)

    over_cols(first_sum)
    hops = [jnp.where(z * 2 >= nz, lax.rem(z + nz - n, nz), lax.rem(z + n, nz)) for n in range(1, nz)]
    for n in range(1, nz):
        zz = hops[n - 1]
        if n == nz - 1:
            for ky in range(1, ny):
                y_copy(ky).wait_recv()

                def y_sum(span, here):
                    hid_out[span, :] += y_in[ky - 1, span, :].astype(f32)

                over_rows(0, y_sum)

        def more_sum(r):
            for k in range(ny):
                head_out[turn_y(k), pl.ds(r, cstep), :] += r_in[zz, turn_y(k), pl.ds(r, cstep), :].astype(f32)

        def arrived():
            for k in range(ny):
                r_got(zz, turn_y(k))
            over_cols(more_sum)

        if relay:
            pl.when(direct(zz))(arrived)
        else:
            arrived()

    losses = loss_own[...]
    for k in range(1, nb):
        i = lax.rem(b + k, nb)
        copy(loss_own, loss_all.at[i], ls.at[k - 1], lr.at[i], i, v).wait_recv()
        losses = losses + loss_all[i]
    loss_out[...] = losses * (1.0 / (tokens * nb))

    for j in range(ny):
        yy = turn_y(j)
        pl.when(has_up)(lambda: w_z(z, yy, True, j == 0).wait_send())
        pl.when(has_down)(lambda: w_z(z, yy, False, j == 0).wait_send())
        for k in range(1, nz):
            @pl.when(z - k >= 0)
            def _():
                pl.when(has_up)(lambda: w_z(z - k, yy, True).wait_send())

            @pl.when(z + k < nz)
            def _():
                pl.when(has_down)(lambda: w_z(z + k, yy, False).wait_send())
    for k in range(1, ny):
        w_y(k).wait_send()
        h_y(k).wait_send()
        y_copy(k).wait_send()
    for k in range(1, nx):
        h_x(k).wait_send()
        for ky in range(1, ny):
            pl.when(core == 0)(lambda: h_xy(k, ky).wait_send())
            pl.when(core == 1)(lambda: h_yx(k, ky).wait_send())
    for kx, ky in ways:
        h_core(kx, ky).wait_send()
        core_copy(kx, ky).wait_send()
        if kx:
            x_copy(kx, ky).wait_send()
    for n in range(len(peers)):
        code_copy(n).wait_send()
        stat_copy(n).wait_send()
    for k in range(1, nb):
        loss_copy(k).wait_send()
    for n in range(nz):
        for k in range(ny):
            yy = turn_y(k)
            if relay and n == 0:
                pl.when(at_end)(lambda: far_copy(yy).wait_send())
                pl.when(jnp.logical_not(at_end))(lambda: r_copy(order[n], yy).wait_send())
            elif n < nz - 1 or k:
                r_copy(order[n], yy).wait_send()


def local(nb, nv, hidden, head_weight, targets, valid_mask):
    nx = nv // 2
    ny = nx if nx <= 2 and nb % nx == 0 else 1
    nz = nb // ny
    rows, width = hidden.shape
    entries, cols = head_weight.shape
    half = entries // ny
    group = ny * nv
    tokens = rows * group
    code = jnp.broadcast_to(jnp.where(valid_mask != 0, targets, -1).astype(f32)[None, :], (8, rows))
    weight = jnp.transpose(head_weight.reshape(ny, half, cols), (0, 2, 1))
    vm = pltpu.VMEM
    dma = pltpu.SemaphoreType.DMA
    slab = ny * cols
    ly, lx = max(ny - 1, 1), max(nx - 1, 1)
    buffers = [
        vm((tokens, width), bf16), vm((width, half), bf16), vm((group, 8, rows), f32), vm((tokens, 128), f32),
        vm((tokens, half), f32), vm((tokens, half), bf16),
        vm((8, tokens), f32), vm((group, 8, tokens), f32), vm((8, 128), f32), vm((nb, 8, 128), f32),
        vm((slab if slab % 128 == 0 else width, half), f32), vm((width, half), bf16), vm((nz, ny, cols, half), bf16),
        vm((tokens, width), f32), vm((nx, ny, rows, width), f32),
        vm((lx, ny, rows, width), bf16), vm((lx, ny, rows, width), bf16),
        vm((ly, rows, width), bf16), vm((ly, rows, width), bf16),
        vm((slab if nz == 4 else 16, half), f32), vm((ny, cols if nz == 4 else 16, half), bf16),
    ]
    sems = [
        dma((2,)), dma((nx + ny,)), dma((nx, ny)), dma((nx, ny)), dma((group,)), dma((nb,)), dma((nb,)),
        dma((ly,)), dma((nb,)), dma((group,)), dma((group,)), dma((group,)), dma((group,)), dma((nb,)), dma((nb,)),
        dma((nb,)), dma((nb,)), dma((nx, ny)), dma((nx, ny)), dma((nx, ny)), dma((nx, ny)), dma((ny,)), dma((ny,)),
        dma((ny,)), dma((ny,)),
    ]
    whole = pl.BlockSpec(memory_space=vm)
    head_t, hidden_grad, loss = pl.pallas_call(
        functools.partial(kernel, (nz, ny, nx, nv)),
        out_shape=(
            jax.ShapeDtypeStruct((ny, cols, half), f32),
            jax.ShapeDtypeStruct((rows, width), f32),
            jax.ShapeDtypeStruct((8, 128), f32),
        ),
        in_specs=[whole] * 3,
        out_specs=(whole,) * 3,
        scratch_shapes=buffers + sems,
        compiler_params=pltpu.CompilerParams(
            collective_id=0, has_side_effects=True, vmem_limit_bytes=67043328),
    )(hidden, weight, code)
    return jnp.transpose(head_t, (0, 2, 1)).reshape(entries, cols), hidden_grad, loss[0, 0]


def column_groups(width):
    units = width // 256
    sizes, left = [1, 2], units - 5
    while left > 0:
        sizes.append(min(3, left))
        left -= sizes[-1]
    sizes += [1, 1]
    starts = [sum(sizes[:n]) for n in range(len(sizes))]
    return [(s, n) for s, n in zip(starts, sizes)]


def plane_kernel(h_in, w_in, ids_in, mask_in, head_out, hid_out, loss_out, h_all, w_all, w_over, ids_own, mask_own,
                 code_own, code_got, code_all,
                 logits, expo, delta, stat_own, stat_all, loss_one, loss_two, loss_all, loss_zs,
                 grad_own, held, grad_send, far_in, r_in, part, core_in, x_out, x_in, y_out, y_in, *sems):
    (own_sem, hs, hr, ws, wr, wys, cs, cr, ss, sr, ls, lr, ms, mr,
     es, rs, rr, nr, fr, ds, xs, xr, ys) = sems
    nz, ny, nv = 4, 2, 4
    nb = nz * ny
    rows, width = h_in.shape
    cols, half = w_in.shape[0], w_in.shape[1] // ny
    piece = cols // 2
    group = ny * nv
    tokens = rows * group
    slab = ny * cols
    shift, lo = cols % 128, cols - cols % 128
    win = -(-(cols + shift) // 128) * 128
    b, v = lax.axis_index("batch"), lax.axis_index("vocab")
    z, y = lax.div(b, ny), lax.rem(b, ny)
    x, core = lax.div(v, 2), lax.rem(v, 2)
    me = y * nv + v
    low = z * 2 < nz
    at_end = (z == 0) | (z == nz - 1)
    inside = jnp.logical_not(at_end)

    def flip(a, k):
        return 1 - a if k else a

    def copy(src, dst, send, recv, bb, vv):
        return pltpu.make_async_remote_copy(
            src_ref=src, dst_ref=dst, send_sem=send, recv_sem=recv,
            device_id={"batch": bb, "vocab": vv}, device_id_type=MESH)

    def hrow(i):
        return pl.ds(pl.multiple_of(i * rows, 16), rows)

    over_x, over_y, over_core = (1 - x) * 2 + core, z * ny + 1 - y, x * 2 + 1 - core
    peers = [(ky, kx, kc) for ky in range(2) for kx in range(2) for kc in range(2) if ky or kx or kc]

    def peer(n):
        ky, kx, kc = peers[n]
        yy, vv = flip(y, ky), flip(x, kx) * 2 + flip(core, kc)
        return z * ny + yy, vv, yy * nv + vv

    def z_peer(k):
        return lax.rem(z + k, nz) * ny + y

    has_up, has_down = z + 1 < nz, z >= 1
    barrier = pltpu.get_barrier_semaphore()

    def greet(bb, vv):
        pl.semaphore_signal(barrier, inc=1, device_id={"batch": bb, "vocab": vv}, device_id_type=MESH)

    pl.when(has_up)(lambda: greet(b + ny, v))
    pl.when(has_down)(lambda: greet(b - ny, v))
    greet(over_y, v)
    greet(b, over_x)
    greet(b, over_core)
    first = pl.ds(pl.multiple_of(y * half, 128), half)
    second = pl.ds(pl.multiple_of((1 - y) * half, 128), half)
    local = [
        pltpu.make_async_copy(w_in.at[:, second], w_over, own_sem.at[0]),
        pltpu.make_async_copy(w_in.at[:, first], w_all.at[pl.ds(pl.multiple_of(b * cols, 16), cols)], own_sem.at[1]),
        pltpu.make_async_copy(ids_in, ids_own, own_sem.at[2]),
        pltpu.make_async_copy(mask_in, mask_own, own_sem.at[3]),
        pltpu.make_async_copy(h_in, h_all.at[hrow(me)], own_sem.at[4]),
    ]
    for one in local:
        one.start()
    for one in local:
        one.wait()
    code = jnp.where(mask_own[...] != 0, ids_own[...], -1).astype(f32)
    code_own[...] = jnp.broadcast_to(code, code_own.shape)
    pl.semaphore_wait(barrier, jnp.where(inside, 5, 4))

    def w_ref(i, h):
        return w_all.at[pl.ds(pl.multiple_of(i * cols + h * piece, 16), piece)]

    def w_z(i, h, up):
        return copy(w_ref(i, h), w_ref(i, h), ws.at[0 if up else 1],
                    wr.at[i, h], b + ny if up else b - ny, v)

    def w_pass(i, h, up):
        return copy(w_ref(i, h), w_ref(i, h), ws.at[jnp.where(up, 0, 1)], wr.at[i, h], jnp.where(up, b + ny, b - ny), v)

    def w_y(h):
        return copy(w_over.at[pl.ds(h * piece, piece)], w_ref(b, h), wys.at[0], wr.at[b, h], over_y, v)

    def w_got(i, h):
        copy(w_ref(i, h), w_ref(i, h), wys.at[0], wr.at[i, h], over_y, v).wait_recv()

    near = z + 1 - 2 * lax.rem(z, 2)
    slabs = [z, near, jnp.where(low, 2, 1), jnp.where(low, 3, 0)]

    def h_send(i, bb, vv):
        return copy(h_all.at[hrow(i)], h_all.at[hrow(i)], hs.at[0], hr.at[i], bb, vv)

    def h_x():
        return h_send(me, b, over_x)

    def h_y():
        return h_send(me, over_y, v)

    def h_xy():
        return h_send(y * nv + over_x, over_y, v)

    def h_yx():
        return h_send((1 - y) * nv + v, b, over_x)

    def h_core(kx, ky):
        i = flip(y, ky) * nv + flip(x, kx) * 2 + core
        return h_send(i, b, over_core)

    def h_got(kx, ky, cc):
        i = flip(y, ky) * nv + flip(x, kx) * 2 + cc
        h_send(i, b, over_core).wait_recv()

    def code_copy(n):
        bb, vv, _ = peer(n)
        return copy(code_own, code_got.at[me], cs.at[0], cr.at[0], bb, vv)

    for h in range(2):
        w_y(h).start()
    for h in range(2):
        pl.when(has_up)(lambda: w_z(b, h, True).start())
        pl.when(has_down)(lambda: w_z(b, h, False).start())
    h_x().start()
    h_y().start()
    h_core(0, 0).start()

    def send_codes(count):
        for n in range(len(peers)):
            if sum(peers[n]) == count:
                code_copy(n).start()

    send_codes(1)
    for h in range(2):
        i = z * ny + 1 - y
        w_got(i, h)
        pl.when(has_up)(lambda: w_z(i, h, True).start())
        pl.when(has_down)(lambda: w_z(i, h, False).start())

    def w_slab(zz, onward, which=(0, 1)):
        for k in which:
            for h in range(2):
                i = zz * ny + flip(y, k)
                w_got(i, h)
                if onward:
                    w_pass(i, h, zz < z).start()

    @pl.when(at_end)
    def _():
        w_slab(slabs[1], False)

    @pl.when(inside)
    def _():
        w_slab(slabs[1], True)
        w_slab(slabs[2], True)

    h_got(1, 0, core)
    pl.when(core == 0)(lambda: h_xy().start())
    h_core(1, 0).start()
    h_got(0, 1, core)
    pl.when(core == 1)(lambda: h_yx().start())
    h_core(0, 1).start()
    send_codes(2)

    @pl.when(at_end)
    def _():
        w_slab(slabs[2], False)

    @pl.when(inside)
    def _():
        w_slab(slabs[3], True)

    h_got(1, 1, core)
    h_core(1, 1).start()
    send_codes(3)
    for kx in range(2):
        for ky in range(2):
            h_got(kx, ky, 1 - core)

    step = 2 * rows
    steps = tokens // step
    lines = lax.broadcasted_iota(jnp.int32, (8, rows), 0)

    def scores(n, zz, at=0, wide=slab):
        here = pl.ds(pl.multiple_of(zz * slab + at, 128), wide)
        there = pl.ds(pl.multiple_of(zz * slab + at, 16), wide)
        return jnp.dot(h_all[n * step:(n + 1) * step, here], w_all[there, :], preferred_element_type=f32)

    for j in range(nz - 1):
        for n in range(steps):
            span = pl.ds(n * step, step)
            if j:
                logits[span, :] += scores(n, slabs[j])
            else:
                logits[span, :] = scores(n, slabs[j])

    code_got[me] = code_own[...]
    others = pl.ds(0, group - 1)
    copy(code_got.at[others], code_got.at[others], cs.at[0], cr.at[0], b, over_x).wait_recv()
    for i in range(group):
        code_all[i * rows:(i + 1) * rows, :] = jnp.transpose(jnp.concatenate([code_got[i]] * (rows // 8), axis=0))

    early = lo
    pl.when(at_end)(lambda: w_slab(slabs[3], False, (0,)))
    for n in range(steps):
        logits[n * step:(n + 1) * step, :] += scores(n, slabs[3], y * (slab - early), early)
    pl.when(at_end)(lambda: w_slab(slabs[3], False, (1,)))

    sums = jnp.zeros((8, rows), f32)
    for n in range(steps):
        span = pl.ds(n * step, step)
        capped = softcap * jnp.tanh((logits[span, :] + scores(n, slabs[3], (1 - y) * early, slab - early)) * (1.0 / softcap))
        raised = jnp.exp(capped)
        logits[span, :] = capped
        expo[span, :] = raised
        total = jnp.broadcast_to(jnp.sum(raised, axis=1, keepdims=True), (step, 128))
        for k in range(2):
            turned = jnp.transpose(total[k * rows:(k + 1) * rows])
            sums = jnp.where(lines == 2 * n + k, turned[0:8], sums)
    stat_own[...] = sums

    def stat_copy(n):
        bb, vv, _ = peer(n)
        return copy(stat_own, stat_all.at[me], ss.at[0], sr.at[0], bb, vv)

    for n in range(len(peers)):
        stat_copy(n).start()

    ids = (lax.broadcasted_iota(jnp.int32, (step, half), 1) + (v * ny + y) * half).astype(f32)
    hit_total = jnp.zeros((step, 1), f32)
    for n in range(steps):
        span = pl.ds(n * step, step)
        capped = logits[span, :]
        hit = ids == code_all[span, 0:1]
        slope = 1.0 - (capped * (1.0 / softcap)) ** 2
        expo[span, :] = expo[span, :] * slope
        logits[span, :] = jnp.where(hit, slope, 0.0)
        hit_total = hit_total + jnp.sum(jnp.where(hit, capped, 0.0), axis=1, keepdims=True)
    hit_total = jnp.sum(hit_total, axis=0, keepdims=True)
    loss_one[...] = jnp.broadcast_to(hit_total, loss_one.shape)

    def hit_copy(n):
        bb, vv, _ = peer(n)
        return copy(loss_one, loss_all.at[me], ls.at[0], lr.at[0], bb, vv)

    for n in range(len(peers)):
        hit_copy(n).start()
    code_rows = jnp.zeros((8, rows), f32)
    for i in range(group):
        code_rows = jnp.where(lines == i, code_got[i], code_rows)
    weight = (code_rows >= 0).astype(f32)

    stat_all[me] = sums
    copy(stat_all.at[others], stat_all.at[others], ss.at[0], sr.at[0], b, over_x).wait_recv()
    partition = stat_all[0]
    for i in range(1, group):
        partition = partition + stat_all[i]
    scale = weight / partition

    def delta_copy(n):
        span = pl.ds(n * step, step)
        return copy(delta.at[0, span], delta.at[1, span], es.at[0], cr.at[0], over_y, v)

    for n in range(steps):
        for k in range(2):
            i = 2 * n + k
            span = pl.ds(i * rows, rows)
            by_row = jnp.transpose(jnp.broadcast_to(scale[i:i + 1, :], (rows, rows)))
            factor = jnp.concatenate([by_row] * (half // rows), axis=1)
            delta[0, span, :] = (expo[span, :] * factor - logits[span, :]).astype(bf16)
        delta_copy(n).start()

    near_end = jnp.where(low, 1, 2)
    far = jnp.where(low, nz - 1, 0)
    across = jnp.where(low, 2, 1)
    targets = [jnp.where(at_end, far, across), jnp.where(at_end, across, near), jnp.where(at_end, near_end, far), z]
    top = y * shift

    def grad_share(zz, r, first, wide):
        here = pl.ds(pl.multiple_of(zz * slab + y * lo, 128), win)
        return lax.dot_general(h_all[:, here], delta[r, :, first:first + wide], (((0,), (0,)), ((), ())), preferred_element_type=f32)

    def sent(k, r):
        return grad_send.at[k, r, pl.ds(pl.multiple_of(top, 16), cols)]

    def r_copy(k, r):
        return copy(sent(k, r), r_in.at[z, r], rs.at[0], rr.at[z, r], targets[k] * ny + y, v)

    def far_copy(r):
        return copy(sent(0, r), far_in.at[r], rs.at[0], fr.at[r], near_end * ny + y, v)

    bounds = [(0, 128), (128, half - 128)]

    def far_part(n):
        here = pl.ds(*bounds[n])
        return copy(grad_send.at[0, 0, pl.ds(pl.multiple_of(top, 16), cols), here], far_in.at[0, :, here],
                    rs.at[0], fr.at[(0, 2)[n]], near_end * ny + y, v)

    def cross_copy():
        return copy(sent(1, 1), far_in.at[2], rs.at[0], fr.at[3], near_end * ny + y, v)

    def near_copy(r, h):
        src = grad_send.at[2, r, pl.ds(pl.multiple_of(top + h * piece, 16), piece)]
        return copy(src, r_in.at[z, r, pl.ds(h * piece, piece)], rs.at[0], nr.at[r, h], near_end * ny + y, v)

    def first_piece():
        for n in range(2):
            first, wide = bounds[n]
            grad_send[0, 0, :, first:first + wide] = grad_share(targets[0], 0, first, wide).astype(bf16)
            pl.when(at_end)(lambda: far_part(n).start())
        pl.when(inside)(lambda: r_copy(0, 0).start())

    def head_piece(k, r):
        share = grad_share(targets[k], r, 0, half)
        if k == nz - 1:
            grad_own[r] = share
        elif k == 2:
            @pl.when(at_end)
            def _():
                grad_send[k, r] = share.astype(bf16)
                near_copy(r, 0).start()
                if r:
                    near_copy(0, 1).start()
                    near_copy(1, 1).start()

            @pl.when(inside)
            def _():
                held[r] = share
        elif k == 0:
            @pl.when(at_end)
            def _():
                grad_send[k, r] = share.astype(bf16)
                far_copy(r).start()

            @pl.when(inside)
            def _():
                held[2] = share
        else:
            grad_send[k, r] = share.astype(bf16)
            if r:
                pl.when(at_end)(lambda: cross_copy().start())
                pl.when(inside)(lambda: r_copy(k, r).start())
            else:
                r_copy(k, r).start()

    cstep = chunk_of(cols, 64)

    def over_cols(body):
        def one(n, carry):
            body(pl.multiple_of(n * cstep, 16))
            return carry

        lax.fori_loop(0, cols // cstep, one, 0)

    def relay(k, r, slot):
        @pl.when(inside)
        def _():
            if r == 0:
                for n in range(2):
                    far_part(n).wait_recv()
            elif k:
                far_copy(r).wait_recv()
            else:
                cross_copy().wait_recv()

            def add(n):
                here = pl.ds(pl.multiple_of(top + n, 16), cstep)
                there = pl.ds(n, cstep)
                grad_send[k, r, here, :] = (held[slot, here, :] + far_in[slot, there, :].astype(f32)).astype(bf16)

            over_cols(add)
            r_copy(k, r).start()

    groups = column_groups(width)
    blocks = [(1, 1), (1, 0), (0, 1), (0, 0)]
    unit = width // (width // 256)

    def span_of(g):
        first, n = groups[g]
        return pl.ds(first * unit, n * unit)

    y_first = (3,)

    def block(g, one, two, cc):
        kx, ky = (two, one) if g in y_first else (one, two)
        return flip(y, ky) * nv + flip(x, kx) * 2 + cc

    def core_copy(g, one, two):
        return copy(part.at[hrow(block(g, one, two, 1 - core)), span_of(g)], core_in.at[one, two, :, span_of(g)],
                    ds.at[0], wr.at[g, 0], b, over_core)

    def over_one(g):
        return (over_y, v) if g in y_first else (b, over_x)

    def over_two(g):
        return (b, over_x) if g in y_first else (over_y, v)

    def one_copy(g, two):
        return copy(x_out.at[two, :, span_of(g)], x_in.at[two, :, span_of(g)], xs.at[0], (hr if two else xr).at[g],
                    *over_one(g))

    def two_copy(g):
        return copy(y_out.at[:, span_of(g)], y_in.at[:, span_of(g)], ys.at[0], wr.at[g, 1], *over_two(g))

    def part_group(g):
        first, n = groups[g]

        def columns(j, carry):
            span = pl.ds(pl.multiple_of(j * unit, 128), unit)
            part[:, span] = lax.dot_general(
                delta[0], w_all[span, :], (((1,), (1,)), ((), ())), preferred_element_type=f32)
            return carry

        lax.fori_loop(first, first + n, columns, 0)
        for one, two in blocks:
            core_copy(g, one, two).start()

    hstep = 16

    def over_rows(body):
        def one(n, carry):
            body(pl.multiple_of(n * hstep, hstep))
            return carry

        lax.fori_loop(0, rows // hstep, one, 0)

    def core_sum(g):
        span = span_of(g)
        landed = core_in.at[:, :, :, span]
        copy(landed, landed, ds.at[0], wr.at[g, 0], b, over_core).wait_recv()
        for one, two in blocks:
            start = block(g, one, two, core) * rows

            def add(n):
                here = pl.ds(pl.multiple_of(start + n, hstep), hstep)
                both = part[here, span] + core_in[one, two, pl.ds(n, hstep), span]
                if one:
                    x_out[two, pl.ds(n, hstep), span] = both.astype(bf16)
                else:
                    part[here, span] = both

            over_rows(add)
            if one:
                one_copy(g, two).start()

    def one_sum(g):
        span = span_of(g)
        for two in (1, 0):
            one_copy(g, two).wait_recv()
            start = block(g, 0, two, core) * rows

            def add(n):
                here = pl.ds(pl.multiple_of(start + n, hstep), hstep)
                total = part[here, span] + x_in[two, pl.ds(n, hstep), span].astype(f32)
                if two:
                    y_out[pl.ds(n, hstep), span] = total.astype(bf16)
                else:
                    hid_out[pl.ds(n, hstep), span] = total

            over_rows(add)
            if two:
                two_copy(g).start()

    def two_sum(g):
        span = span_of(g)
        two_copy(g).wait_recv()

        def add(n):
            here = pl.ds(n, hstep)
            hid_out[here, span] += y_in[here, span].astype(f32)

        over_rows(add)

    count = len(groups)

    def plane_copy(k):
        return copy(loss_two, loss_zs.at[z], ms.at[0], mr.at[0], z_peer(k), v)

    def plane_loss():
        loss_all[me] = loss_one[...]
        copy(loss_all.at[others], loss_all.at[others], ls.at[0], lr.at[0], b, over_x).wait_recv()
        hits = loss_all[0]
        for i in range(1, group):
            hits = hits + loss_all[i]
        logs = jnp.sum(weight * jnp.log(partition), axis=1, keepdims=True)
        loss_two[...] = jnp.broadcast_to(jnp.sum(logs, axis=0, keepdims=True), (8, rows)) - hits
        for k in range(1, nz):
            plane_copy(k).start()

    first_piece()
    part_group(0)
    part_group(1)
    plane_loss()
    core_sum(0)
    part_group(2)
    core_sum(1)
    head_piece(1, 0)
    part_group(3)
    core_sum(2)
    head_piece(2, 0)
    relay(2, 0, 0)
    for g in range(4, count):
        part_group(g)
        core_sum(g - 1)
    core_sum(count - 1)
    head_piece(3, 0)
    one_sum(0)

    whole_delta = copy(delta.at[0], delta.at[1], es.at[0], cr.at[0], over_y, v)
    whole_delta.wait_recv()
    head_piece(0, 1)
    head_piece(1, 1)
    one_sum(1)
    head_piece(2, 1)
    head_piece(3, 1)
    one_sum(2)
    relay(2, 1, 1)

    copy(w_over, w_over, wys.at[0], wr.at[0, 0], over_y, v).wait_send()
    for n in range(1, nz):
        sent_rows = w_all.at[pl.ds(0, n * slab)]
        for way, slabs_sent in ((0, z + 1), (1, nz - z)):
            going = (slabs_sent == n) & (has_down if way else has_up)
            pl.when(going)(lambda: copy(sent_rows, sent_rows, ws.at[way], wr.at[0, 0], b, over_x).wait_send())
    seven = h_all.at[pl.ds(0, 7 * rows)]
    copy(seven, seven, hs.at[0], hr.at[0], b, over_x).wait_send()
    for got, sem in ((code_got, cs), (stat_all, ss), (loss_all, ls)):
        copy(got.at[others], got.at[others], sem.at[0], sem.at[0], b, over_x).wait_send()
    one_sum(3)
    two_sum(0)
    whole_delta.wait_send()
    copy(core_in, core_in, ds.at[0], wr.at[0, 0], b, over_core).wait_send()
    one_sum(4)
    two_sum(1)
    two_sum(2)
    relay(0, 1, 2)
    for g in range(5, count):
        one_sum(g)
        two_sum(g - 2)

    def r_got(zz, r):
        copy(r_in.at[zz, r], r_in.at[zz, r], rs.at[0], rr.at[zz, r], z_peer(1), v).wait_recv()

    def lanes(r):
        return pl.ds(pl.multiple_of(flip(y, r) * half, 128), half)

    sources = [near, jnp.where(low, 2, 1), far]

    def head_sum(r):
        @pl.when(at_end)
        def _():
            r_got(sources[0], r)

        @pl.when(inside)
        def _():
            for h in range(2):
                mine = r_in.at[sources[0], r, pl.ds(h * piece, piece)]
                copy(mine, mine, rs.at[0], nr.at[r, h], near_end * ny + y, v).wait_recv()

        r_got(sources[1], r)

        def add(n):
            here = pl.ds(n, cstep)
            total = grad_own[r, pl.ds(pl.multiple_of(top + n, 16), cstep), :]
            for k in range(2):
                total = total + r_in[sources[k], r, here, :].astype(f32)
            head_out[here, lanes(r)] = total

        over_cols(add)

        @pl.when(inside)
        def _():
            if r:
                return
            r_got(sources[2], r)

            def last(n):
                here = pl.ds(n, cstep)
                head_out[here, lanes(r)] += r_in[sources[2], r, here, :].astype(f32)

            over_cols(last)

    head_sum(0)
    loss_zs[z] = loss_two[...]
    along = loss_zs.at[pl.ds(0, nz - 1)]
    copy(along, along, ms.at[0], mr.at[0], z_peer(1), v).wait_recv()
    losses = loss_zs[0]
    for i in range(1, nz):
        losses = losses + loss_zs[i]
    loss_out[...] = losses * (1.0 / (tokens * nz))
    copy(along, along, ms.at[0], mr.at[0], z_peer(1), v).wait_send()
    two_sum(count - 2)
    two_sum(count - 1)
    head_sum(1)

    for part_sent, sem in ((x_out, xs), (y_out, ys), (r_in.at[pl.ds(0, nz - 1)], rs)):
        copy(part_sent, part_sent, sem.at[0], sem.at[0], b, over_x).wait_send()


def finish_kernel(head_in, hid_in, loss_in, head_out, hid_out, loss_out, sem):
    parts = sem.shape[1]
    moves = []
    for k, (src, dst) in enumerate(((hid_in, hid_out), (head_in, head_out))):
        size = src.shape[0] // parts
        for n in range(parts):
            here = pl.ds(n * size, size)
            moves.append(pltpu.make_async_copy(src.at[here], dst.at[here], sem.at[k, n]))
    for one in moves:
        one.start()
    loss_out[0, 0] = loss_in[0, 0]
    for one in moves:
        one.wait()


def plane_local(hidden, head_weight, targets, valid_mask):
    nz, ny, nv = 4, 2, 4
    rows, width = hidden.shape
    entries, cols = head_weight.shape
    half = entries // ny
    group = ny * nv
    tokens = rows * group
    shift = cols % 128
    win = -(-(cols + shift) // 128) * 128
    vm = pltpu.VMEM
    dma = pltpu.SemaphoreType.DMA
    count = len(column_groups(width))
    line = vm((8, rows), f32)
    buffers = [
        vm((tokens, width), bf16), vm((width, half), bf16), vm((cols, half), bf16),
        vm((1, rows), jnp.int32), vm((1, rows), jnp.int32), line, vm((group, 8, rows), f32), vm((tokens, 128), f32),
        vm((tokens, half), f32), vm((tokens, half), f32), vm((2, tokens, half), bf16),
        line, vm((group, 8, rows), f32), line, line, vm((group, 8, rows), f32), vm((nz, 8, rows), f32),
        vm((2, win, half), f32), vm((3, win, half), f32), vm((3, 2, win, half), bf16),
        vm((3, cols, half), bf16), vm((nz, 2, cols, half), bf16),
        vm((tokens, width), f32), vm((2, 2, rows, width), f32),
        vm((2, rows, width), bf16), vm((2, rows, width), bf16), vm((rows, width), bf16), vm((rows, width), bf16),
    ]
    sems = [
        dma((5,)), dma((1,)), dma((group,)), dma((2,)), dma((8, 2)), dma((1,)),
        dma((1,)), dma((1,)), dma((1,)), dma((1,)), dma((1,)), dma((1,)), dma((1,)), dma((1,)),
        dma((1,)), dma((1,)), dma((nz, 2)), dma((2, 2)), dma((4,)),
        dma((1,)), dma((1,)), dma((count,)), dma((1,)),
    ]
    whole = pl.BlockSpec(memory_space=vm)
    head_t, hidden_grad, loss = pl.pallas_call(
        plane_kernel,
        out_shape=(
            vm((cols, entries), f32),
            vm((rows, width), f32),
            vm((8, rows), f32),
        ),
        in_specs=[pl.BlockSpec(memory_space=pl.ANY)] * 4,
        out_specs=(whole,) * 3,
        scratch_shapes=buffers + sems,
        compiler_params=pltpu.CompilerParams(
            collective_id=1, has_side_effects=True, vmem_limit_bytes=58 * 1024 * 1024),
    )(hidden, jnp.transpose(head_weight), targets[None, :], valid_mask[None, :])
    anywhere = pl.BlockSpec(memory_space=pl.ANY)
    head_t, hidden_grad, loss = pl.pallas_call(
        finish_kernel,
        out_shape=(
            jax.ShapeDtypeStruct((cols, entries), f32),
            jax.ShapeDtypeStruct((rows, width), f32),
            jax.ShapeDtypeStruct((1, 1), f32),
        ),
        in_specs=[whole] * 3,
        out_specs=(anywhere, anywhere, pl.BlockSpec(memory_space=pltpu.SMEM)),
        scratch_shapes=[dma((2, 4))],
        compiler_params=pltpu.CompilerParams(vmem_limit_bytes=1024 * 1024),
    )(head_t, hidden_grad, loss)
    return jnp.transpose(head_t), hidden_grad, loss[0, 0]


def in_planes(nb, nv, hidden, head_weight, targets, valid_mask):
    rows, width = hidden.shape
    entries, cols = head_weight.shape
    fits = nb == 8 and nv == 4 and rows == 128 and width % 256 == 0 and width >= 2048
    fits = fits and len(column_groups(width)) <= 8
    return fits and entries % 256 == 0 and entries >= 512 and cols % 32 == 0 and (2 * cols) % 128 == 0


def device(nb, nv, *arrays):
    if in_planes(nb, nv, *arrays):
        return plane_local(*arrays)
    return local(nb, nv, *arrays)


def solution(mesh):
    placed = (
        P(("batch", "vocab"), None),
        P("vocab", "batch"),
        P(("batch", "vocab")),
        P(("batch", "vocab")),
    )
    return jax.shard_map(
        functools.partial(device, mesh.shape["batch"], mesh.shape["vocab"]),
        mesh=mesh,
        in_specs=placed,
        out_specs=(P("vocab", "batch"), P(("batch", "vocab"), None), P()),
        check_vma=False,
    )
```

```python
import functools

import jax
import jax.numpy as jnp
from jax import lax
from jax.experimental import pallas as pl
from jax.experimental.pallas import tpu as pltpu
from jax.sharding import PartitionSpec as P

softcap = 30.0
MESH = pl.DeviceIdType.MESH
f32, bf16 = jnp.float32, jnp.bfloat16


def chunk_of(length, most):
    return max(s for s in range(16, most + 1, 16) if length % s == 0)


def kernel(sizes, h_in, w_in, code_in, head_out, hid_out, loss_out, h_all, w_all, code_got, code_all,
           logits, delta, stat_own, stat_all, loss_own, loss_all, grad, grad_send, r_in,
           part, core_in, x_out, x_in, y_out, y_in, far_own, far_in, *sems):
    nz, ny, nx, nv = sizes
    (own_sem, hs, hf, hd, hr, ws_up, ws_dn, ws_y, wr, cs, cr, ss, sr, ls, lr,
     rs, rr, ds, dr, xs, xr, ys, yr, fs, fr) = sems
    nb = nz * ny
    rows, width = h_in.shape
    cols, half = w_in.shape[1:]
    group = ny * nv
    tokens = rows * group
    entries = ny * half
    b, v = lax.axis_index("batch"), lax.axis_index("vocab")
    z, y = lax.div(b, ny), lax.rem(b, ny)
    x, core = lax.div(v, 2), lax.rem(v, 2)
    other = x * 2 + 1 - core
    me = y * nv + v

    def at(bb, vv):
        return {"batch": bb, "vocab": vv}

    def copy(src, dst, send, recv, bb, vv):
        return pltpu.make_async_remote_copy(
            src_ref=src, dst_ref=dst, send_sem=send, recv_sem=recv, device_id=at(bb, vv), device_id_type=MESH)

    def hrow(i):
        return pl.ds(pl.multiple_of(i * rows, 16), rows)

    def wrow(i):
        return pl.ds(pl.multiple_of(i * cols, 16), cols)

    def turn_y(k):
        return lax.rem(y + k, ny)

    def turn_x(k):
        return lax.rem(x + k, nx)

    peers = [(k, j) for k in range(ny) for j in range(nv) if k or j]

    def peer(n):
        k, j = peers[n]
        return z * ny + turn_y(k), lax.rem(v + j, nv), turn_y(k) * nv + lax.rem(v + j, nv)

    barrier = pltpu.get_barrier_semaphore()
    for k in range(1, nb):
        pl.semaphore_signal(barrier, inc=1, device_id=at(lax.rem(b + k, nb), v), device_id_type=MESH)
    met = [n for n in range(len(peers)) if peers[n][1]]
    for n in met:
        bb, vv, _ = peer(n)
        pl.semaphore_signal(barrier, inc=1, device_id=at(bb, vv), device_id_type=MESH)
    pl.semaphore_wait(barrier, nb - 1 + len(met))

    def w_z(zz, yy, up, own=False):
        i = zz * ny + yy
        dst = w_all.at[wrow(i)]
        sem = (ws_up if up else ws_dn).at[i]
        return copy(w_in.at[y] if own else dst, dst, sem, wr.at[i], b + ny if up else b - ny, v)

    def w_y(k):
        return copy(w_in.at[turn_y(k)], w_all.at[wrow(b)], ws_y.at[k - 1], wr.at[b], z * ny + turn_y(k), v)

    def w_got(zz, yy):
        w_z(zz, yy, True).wait_recv()

    has_up, has_down = z + 1 < nz, z >= 1

    def h_send(n_src, sem, bb, vv, own=False):
        dst = h_all.at[hrow(n_src)]
        return copy(h_in if own else dst, dst, sem, hr.at[n_src], bb, vv)

    def h_x(k):
        return h_send(me, hs.at[k - 1], b, turn_x(k) * 2 + core, True)

    def h_y(k):
        return h_send(me, hs.at[nx + k - 1], z * ny + turn_y(k), v, True)

    def h_xy(kx, ky):
        return h_send(y * nv + turn_x(kx) * 2 + core, hf.at[kx, ky], z * ny + turn_y(ky), v)

    def h_yx(kx, ky):
        return h_send(turn_y(ky) * nv + v, hf.at[kx, ky], b, turn_x(kx) * 2 + core)

    def h_core(kx, ky):
        i = turn_y(ky) * nv + turn_x(kx) * 2 + core
        return h_send(i, hd.at[kx, ky], b, other, kx == 0 and ky == 0)

    def h_got(kx, ky, cc):
        i = turn_y(ky) * nv + turn_x(kx) * 2 + cc
        h_send(i, hd.at[kx, ky], b, other).wait_recv()

    def code_copy(n):
        bb, vv, _ = peer(n)
        return copy(code_in, code_got.at[me], cs.at[n], cr.at[me], bb, vv)

    for k in range(1, ny):
        w_y(k).start()
    pl.when(has_up)(lambda: w_z(z, y, True, True).start())
    pl.when(has_down)(lambda: w_z(z, y, False, True).start())
    for k in range(1, nx):
        h_x(k).start()
    for k in range(1, ny):
        h_y(k).start()
    for n in range(len(peers)):
        code_copy(n).start()
    h_core(0, 0).start()
    local = [
        pltpu.make_async_copy(w_in.at[y], w_all.at[wrow(b)], own_sem.at[0]),
        pltpu.make_async_copy(h_in, h_all.at[hrow(me)], own_sem.at[1]),
    ]
    for one in local:
        one.start()

    for k in range(1, ny):
        w_got(z, turn_y(k))
        pl.when(has_up)(lambda: w_z(z, turn_y(k), True).start())
        pl.when(has_down)(lambda: w_z(z, turn_y(k), False).start())

    def h_pass():
        for kx in range(1, nx):
            h_got(kx, 0, core)
            for ky in range(1, ny):
                pl.when(core == 0)(lambda: h_xy(kx, ky).start())
            h_core(kx, 0).start()
        for ky in range(1, ny):
            h_got(0, ky, core)
            for kx in range(1, nx):
                pl.when(core == 1)(lambda: h_yx(kx, ky).start())
            h_core(0, ky).start()

    def h_rest():
        for kx in range(1, nx):
            for ky in range(1, ny):
                h_got(kx, ky, core)
                h_core(kx, ky).start()

    for k in range(1, nz):
        for j in range(ny):
            yy = turn_y(j)

            @pl.when(z - k >= 0)
            def _():
                w_got(z - k, yy)
                pl.when(has_up)(lambda: w_z(z - k, yy, True).start())

            @pl.when(z + k < nz)
            def _():
                w_got(z + k, yy)
                pl.when(has_down)(lambda: w_z(z + k, yy, False).start())
        if k == 1:
            h_pass()
        if k == min(2, nz - 1):
            h_rest()

    for one in local:
        one.wait()
    for kx in range(nx):
        for ky in range(ny):
            h_got(kx, ky, 1 - core)
    code_got[me] = code_in[...]
    for n in range(len(peers)):
        bb, vv, i = peer(n)
        copy(code_in, code_got.at[i], cs.at[n], cr.at[i], bb, vv).wait_recv()
    for i in range(group):
        code_all[i * rows:(i + 1) * rows, :] = jnp.transpose(jnp.concatenate([code_got[i]] * 16, axis=0))

    step = chunk_of(tokens, 256)
    lanes = lax.broadcasted_iota(jnp.int32, (step, 128), 1)
    first = v * entries + y * half

    def span_of(n):
        return pl.ds(pl.multiple_of(n * step, step), step)

    def hits(n):
        ids = lax.broadcasted_iota(jnp.int32, (step, half), 1) + first
        return ids == code_all[span_of(n), 0:1].astype(jnp.int32)

    for n in range(tokens // step):
        span = pl.ds(n * step, step)
        scores = jnp.dot(h_all[span, :], w_all[...], preferred_element_type=f32)
        capped = softcap * jnp.tanh(scores * (1.0 / softcap))
        logits[span, :] = capped
        total = jnp.sum(jnp.exp(capped), axis=1, keepdims=True)
        hit_sum = jnp.sum(jnp.where(hits(n), capped, 0.0), axis=1, keepdims=True)
        turned = jnp.transpose(jnp.where(lax.rem(lanes, 8) < 4, total, hit_sum))
        stat_own[:, n * step:(n + 1) * step] = turned[0:8]

    def stat_copy(n):
        bb, vv, _ = peer(n)
        return copy(stat_own, stat_all.at[me], ss.at[n], sr.at[me], bb, vv)

    for n in range(len(peers)):
        stat_copy(n).start()
    for n in range(len(peers)):
        bb, vv, i = peer(n)
        copy(stat_own, stat_all.at[i], ss.at[n], sr.at[i], bb, vv).wait_recv()
    stats = stat_own[...]
    for n in range(len(peers)):
        stats = stats + stat_all[peer(n)[2]]

    loss = jnp.zeros((1, 1), f32)
    for n in range(tokens // step):
        span = pl.ds(n * step, step)
        weight = (code_all[span, 0:1] >= 0).astype(f32)
        back = jnp.transpose(jnp.concatenate([stats[:, n * step:(n + 1) * step]] * 16, axis=0))
        partition, target_logit = back[:, 0:1], back[:, 4:5]
        loss = loss + jnp.sum(weight * (jnp.log(partition) - target_logit), axis=0, keepdims=True)
        capped = logits[span, :]
        slope = 1.0 - (capped * (1.0 / softcap)) ** 2
        delta[span, :] = ((jnp.exp(capped) * (weight / partition) - jnp.where(hits(n), weight, 0.0)) * slope
                          ).astype(bf16)
    loss_own[...] = jnp.broadcast_to(loss, loss_own.shape)

    def loss_copy(k):
        return copy(loss_own, loss_all.at[b], ls.at[k - 1], lr.at[b], lax.rem(b + k, nb), v)

    def r_copy(zz, yy):
        i = zz * ny + yy
        return copy(grad_send.at[wrow(i)], r_in.at[z, y], rs.at[i], rr.at[b], i, v)

    def grad_share(span):
        return lax.dot_general(h_all[:, span], delta[...], (((0,), (0,)), ((), ())), preferred_element_type=f32)

    slab = ny * cols
    relay = nz == 4 and slab % 128 == 0
    turn = jnp.where(z * 2 >= nz, 1, nz - 1)
    order = [lax.rem(z + turn * k, nz) for k in range(1, nz)] + [z]
    at_end = (z == 0) | (z == nz - 1)
    far = jnp.where(z * 2 >= nz, 0, nz - 1)
    near = jnp.where(z * 2 >= nz, z - 1, z + 1)

    def far_copy(yy):
        return copy(grad_send.at[wrow(far * ny + yy)], far_in.at[yy], fs.at[yy], fr.at[yy], near * ny + y, v)

    def direct(zz):
        return jnp.logical_not(at_end & (zz == far))
    if slab % 128 == 0:
        mine = y * cols
        for n in range(nz):
            zz = order[n]
            span = pl.ds(pl.multiple_of(zz * slab, 128), slab)
            share = grad_share(span)
            held = relay and n == 1
            if n == nz - 1:
                grad[...] = share
            if held:
                @pl.when(jnp.logical_not(at_end))
                def _():
                    far_own[...] = share

                @pl.when(at_end)
                def _():
                    grad_send[span, :] = share.astype(bf16)
                    for k in range(ny):
                        r_copy(zz, turn_y(k)).start()
            else:
                grad_send[span, :] = share.astype(bf16)
                for k in range(ny):
                    yy = turn_y(k)
                    if relay and n == 0:
                        pl.when(at_end)(lambda: far_copy(yy).start())
                        pl.when(jnp.logical_not(at_end))(lambda: r_copy(zz, yy).start())
                    elif n < nz - 1 or k:
                        r_copy(zz, yy).start()
    else:
        mine = b * cols
        wide = chunk_of(width, 256)

        def grad_step(j, carry):
            span = pl.ds(pl.multiple_of(j * wide, wide), wide)
            share = grad_share(span)
            grad[span, :] = share
            grad_send[span, :] = share.astype(bf16)
            return carry

        lax.fori_loop(0, width // wide, grad_step, 0)
        for n in range(nz):
            for k in range(ny):
                if n < nz - 1 or k:
                    r_copy(order[n], turn_y(k)).start()
    for k in range(1, nb):
        loss_copy(k).start()

    wide = chunk_of(width, 256)

    def part_step(j, carry):
        span = pl.ds(pl.multiple_of(j * wide, wide), wide)
        part[:, span] = lax.dot_general(
            delta[...], w_all[span, :], (((1,), (1,)), ((), ())), preferred_element_type=f32)
        return carry

    lax.fori_loop(0, width // wide, part_step, 0)

    def core_copy(kx, ky):
        i = turn_y(ky) * nv + turn_x(kx) * 2 + 1 - core
        return copy(part.at[hrow(i)], core_in.at[kx, ky], ds.at[kx, ky], dr.at[kx, ky], b, other)

    def x_copy(kx, ky):
        return copy(x_out.at[kx - 1, ky], x_in.at[kx - 1, ky], xs.at[kx, ky], xr.at[kx, ky],
                    b, turn_x(kx) * 2 + core)

    def y_copy(ky):
        return copy(y_out.at[ky - 1], y_in.at[ky - 1], ys.at[ky], yr.at[ky], z * ny + turn_y(ky), v)

    ways = [(kx % nx, ky % ny) for kx in range(1, nx + 1) for ky in range(1, ny + 1)]
    for kx, ky in ways:
        core_copy(kx, ky).start()
    hstep = 16

    def over_rows(start, body):
        def one(r, carry):
            body(pl.ds(pl.multiple_of(r * hstep, hstep), hstep),
                 pl.ds(pl.multiple_of(start + r * hstep, hstep), hstep))
            return carry

        lax.fori_loop(0, rows // hstep, one, 0)

    def start_of(kx, ky):
        return (turn_y(ky) * nv + turn_x(kx) * 2 + core) * rows

    for kx, ky in ways:
        core_copy(kx, ky).wait_recv()

        def core_sum(span, here):
            both = part[here, :] + core_in[kx, ky, span, :]
            if kx:
                x_out[kx - 1, ky, span, :] = both.astype(bf16)
            else:
                part[here, :] = both

        over_rows(start_of(kx, ky), core_sum)
        if kx:
            x_copy(kx, ky).start()

    cstep = chunk_of(cols, 64)

    def over_cols(body):
        def one(r, carry):
            body(pl.multiple_of(r * cstep, 16))
            return carry

        lax.fori_loop(0, cols // cstep, one, 0)

    if relay:
        @pl.when(jnp.logical_not(at_end))
        def _():
            for k in range(ny):
                yy = turn_y(k)
                far_copy(yy).wait_recv()

                def far_sum(r):
                    here = pl.ds(pl.multiple_of(yy * cols + r, 16), cstep)
                    there = pl.ds(pl.multiple_of((far * ny + yy) * cols + r, 16), cstep)
                    grad_send[there, :] = (far_own[here, :] + far_in[yy, pl.ds(r, cstep), :].astype(f32)).astype(bf16)

                over_cols(far_sum)
                r_copy(far, yy).start()

    for ky in [k % ny for k in range(1, ny + 1)]:
        for kx in range(1, nx):
            x_copy(kx, ky).wait_recv()

        def x_sum(span, here):
            total = part[here, :]
            for kx in range(1, nx):
                total = total + x_in[kx - 1, ky, span, :].astype(f32)
            if ky:
                y_out[ky - 1, span, :] = total.astype(bf16)
            else:
                hid_out[span, :] = total

        over_rows(start_of(0, ky), x_sum)
        if ky:
            y_copy(ky).start()

    def r_got(zz, yy):
        i = zz * ny + yy
        copy(grad_send.at[wrow(i)], r_in.at[zz, yy], rs.at[i], rr.at[i], i, v).wait_recv()

    for k in range(1, ny):
        r_got(z, turn_y(k))

    def first_sum(r):
        head_out[y, pl.ds(r, cstep), :] = grad[pl.ds(pl.multiple_of(mine + r, 16), cstep), :]
        for k in range(1, ny):
            head_out[turn_y(k), pl.ds(r, cstep), :] = r_in[z, turn_y(k), pl.ds(r, cstep), :].astype(f32)

    over_cols(first_sum)
    hops = [jnp.where(z * 2 >= nz, lax.rem(z + nz - n, nz), lax.rem(z + n, nz)) for n in range(1, nz)]
    for n in range(1, nz):
        zz = hops[n - 1]
        if n == nz - 1:
            for ky in range(1, ny):
                y_copy(ky).wait_recv()

                def y_sum(span, here):
                    hid_out[span, :] += y_in[ky - 1, span, :].astype(f32)

                over_rows(0, y_sum)

        def more_sum(r):
            for k in range(ny):
                head_out[turn_y(k), pl.ds(r, cstep), :] += r_in[zz, turn_y(k), pl.ds(r, cstep), :].astype(f32)

        def arrived():
            for k in range(ny):
                r_got(zz, turn_y(k))
            over_cols(more_sum)

        if relay:
            pl.when(direct(zz))(arrived)
        else:
            arrived()

    losses = loss_own[...]
    for k in range(1, nb):
        i = lax.rem(b + k, nb)
        copy(loss_own, loss_all.at[i], ls.at[k - 1], lr.at[i], i, v).wait_recv()
        losses = losses + loss_all[i]
    loss_out[...] = losses * (1.0 / (tokens * nb))

    for j in range(ny):
        yy = turn_y(j)
        pl.when(has_up)(lambda: w_z(z, yy, True, j == 0).wait_send())
        pl.when(has_down)(lambda: w_z(z, yy, False, j == 0).wait_send())
        for k in range(1, nz):
            @pl.when(z - k >= 0)
            def _():
                pl.when(has_up)(lambda: w_z(z - k, yy, True).wait_send())

            @pl.when(z + k < nz)
            def _():
                pl.when(has_down)(lambda: w_z(z + k, yy, False).wait_send())
    for k in range(1, ny):
        w_y(k).wait_send()
        h_y(k).wait_send()
        y_copy(k).wait_send()
    for k in range(1, nx):
        h_x(k).wait_send()
        for ky in range(1, ny):
            pl.when(core == 0)(lambda: h_xy(k, ky).wait_send())
            pl.when(core == 1)(lambda: h_yx(k, ky).wait_send())
    for kx, ky in ways:
        h_core(kx, ky).wait_send()
        core_copy(kx, ky).wait_send()
        if kx:
            x_copy(kx, ky).wait_send()
    for n in range(len(peers)):
        code_copy(n).wait_send()
        stat_copy(n).wait_send()
    for k in range(1, nb):
        loss_copy(k).wait_send()
    for n in range(nz):
        for k in range(ny):
            yy = turn_y(k)
            if relay and n == 0:
                pl.when(at_end)(lambda: far_copy(yy).wait_send())
                pl.when(jnp.logical_not(at_end))(lambda: r_copy(order[n], yy).wait_send())
            elif n < nz - 1 or k:
                r_copy(order[n], yy).wait_send()


def local(nb, nv, hidden, head_weight, targets, valid_mask):
    nx = nv // 2
    ny = nx if nx <= 2 and nb % nx == 0 else 1
    nz = nb // ny
    rows, width = hidden.shape
    entries, cols = head_weight.shape
    half = entries // ny
    group = ny * nv
    tokens = rows * group
    code = jnp.broadcast_to(jnp.where(valid_mask != 0, targets, -1).astype(f32)[None, :], (8, rows))
    weight = jnp.transpose(head_weight.reshape(ny, half, cols), (0, 2, 1))
    vm = pltpu.VMEM
    dma = pltpu.SemaphoreType.DMA
    slab = ny * cols
    ly, lx = max(ny - 1, 1), max(nx - 1, 1)
    buffers = [
        vm((tokens, width), bf16), vm((width, half), bf16), vm((group, 8, rows), f32), vm((tokens, 128), f32),
        vm((tokens, half), f32), vm((tokens, half), bf16),
        vm((8, tokens), f32), vm((group, 8, tokens), f32), vm((8, 128), f32), vm((nb, 8, 128), f32),
        vm((slab if slab % 128 == 0 else width, half), f32), vm((width, half), bf16), vm((nz, ny, cols, half), bf16),
        vm((tokens, width), f32), vm((nx, ny, rows, width), f32),
        vm((lx, ny, rows, width), bf16), vm((lx, ny, rows, width), bf16),
        vm((ly, rows, width), bf16), vm((ly, rows, width), bf16),
        vm((slab if nz == 4 else 16, half), f32), vm((ny, cols if nz == 4 else 16, half), bf16),
    ]
    sems = [
        dma((2,)), dma((nx + ny,)), dma((nx, ny)), dma((nx, ny)), dma((group,)), dma((nb,)), dma((nb,)),
        dma((ly,)), dma((nb,)), dma((group,)), dma((group,)), dma((group,)), dma((group,)), dma((nb,)), dma((nb,)),
        dma((nb,)), dma((nb,)), dma((nx, ny)), dma((nx, ny)), dma((nx, ny)), dma((nx, ny)), dma((ny,)), dma((ny,)),
        dma((ny,)), dma((ny,)),
    ]
    whole = pl.BlockSpec(memory_space=vm)
    head_t, hidden_grad, loss = pl.pallas_call(
        functools.partial(kernel, (nz, ny, nx, nv)),
        out_shape=(
            jax.ShapeDtypeStruct((ny, cols, half), f32),
            jax.ShapeDtypeStruct((rows, width), f32),
            jax.ShapeDtypeStruct((8, 128), f32),
        ),
        in_specs=[whole] * 3,
        out_specs=(whole,) * 3,
        scratch_shapes=buffers + sems,
        compiler_params=pltpu.CompilerParams(
            collective_id=0, has_side_effects=True, vmem_limit_bytes=67043328),
    )(hidden, weight, code)
    return jnp.transpose(head_t, (0, 2, 1)).reshape(entries, cols), hidden_grad, loss[0, 0]


def column_groups(width):
    left = width // 256 - 11
    sizes = [1, 2, 3, 2]
    while left > 0:
        sizes.append(min(3, left))
        left -= sizes[-1]
    sizes += [2, 1]
    starts = [sum(sizes[:n]) for n in range(len(sizes))]
    return [(s, n) for s, n in zip(starts, sizes)]


def plane_kernel(h_in, w_in, ids_in, mask_in, head_out, hid_out, loss_out, h_all, w_all, w_over, ids_own, mask_own,
                 code_own, code_got, code_all,
                 logits, expo, delta, stat_own, stat_all, loss_one, loss_two, loss_all, loss_zs,
                 grad_own, held, grad_send, far_in, r_in, h_end, d_end, part, core_in, x_out, x_in, y_out, y_in, *sems):
    (own_sem, hs, hr, ws, wr, wys, cs, cr, ss, sr, ls, lr, ms, mr,
     es, er, rs, rr, fr, zs, zr, us, ur, ds, xs, xr, ys) = sems
    nz, ny, nv = 4, 2, 4
    nb = nz * ny
    rows, width = h_in.shape
    cols, half = w_in.shape[0], w_in.shape[1] // ny
    piece = cols // 2
    group = ny * nv
    tokens = rows * group
    slab = ny * cols
    shift, lo = cols % 128, cols - cols % 128
    win = -(-(cols + shift) // 128) * 128
    b, v = lax.axis_index("batch"), lax.axis_index("vocab")
    z, y = lax.div(b, ny), lax.rem(b, ny)
    x, core = lax.div(v, 2), lax.rem(v, 2)
    me = y * nv + v
    low = z * 2 < nz
    at_end = (z == 0) | (z == nz - 1)
    inside = jnp.logical_not(at_end)

    def flip(a, k):
        return 1 - a if k else a

    def copy(src, dst, send, recv, bb, vv):
        return pltpu.make_async_remote_copy(
            src_ref=src, dst_ref=dst, send_sem=send, recv_sem=recv,
            device_id={"batch": bb, "vocab": vv}, device_id_type=MESH)

    def hrow(i):
        return pl.ds(pl.multiple_of(i * rows, 16), rows)

    far = jnp.where(low, nz - 1, 0)
    across = jnp.where(low, 2, 1)
    near_end = jnp.where(low, 1, 2)
    over_x, over_y, over_core = (1 - x) * 2 + core, z * ny + 1 - y, x * 2 + 1 - core
    peers = [(ky, kx, kc) for ky in range(2) for kx in range(2) for kc in range(2) if ky or kx or kc]

    def peer(n):
        ky, kx, kc = peers[n]
        yy, vv = flip(y, ky), flip(x, kx) * 2 + flip(core, kc)
        return z * ny + yy, vv, yy * nv + vv

    def z_peer(k):
        return lax.rem(z + k, nz) * ny + y

    has_up, has_down = z + 1 < nz, z >= 1
    barrier = pltpu.get_barrier_semaphore()

    def greet(bb, vv):
        pl.semaphore_signal(barrier, inc=1, device_id={"batch": bb, "vocab": vv}, device_id_type=MESH)

    pl.when(has_up)(lambda: greet(b + ny, v))
    pl.when(has_down)(lambda: greet(b - ny, v))
    greet(over_y, v)
    greet(b, over_x)
    greet(b, over_core)
    first = pl.ds(pl.multiple_of(y * half, 128), half)
    second = pl.ds(pl.multiple_of((1 - y) * half, 128), half)
    local = [
        pltpu.make_async_copy(w_in.at[:, second], w_over, own_sem.at[0]),
        pltpu.make_async_copy(w_in.at[:, first], w_all.at[pl.ds(pl.multiple_of(b * cols, 16), cols)], own_sem.at[1]),
        pltpu.make_async_copy(ids_in, ids_own, own_sem.at[2]),
        pltpu.make_async_copy(mask_in, mask_own, own_sem.at[3]),
        pltpu.make_async_copy(h_in, h_all.at[hrow(me)], own_sem.at[4]),
    ]
    for one in local:
        one.start()
    for one in local:
        one.wait()
    code = jnp.where(mask_own[...] != 0, ids_own[...], -1).astype(f32)
    code_own[...] = jnp.broadcast_to(code, code_own.shape)
    pl.semaphore_wait(barrier, jnp.where(inside, 5, 4))

    def w_ref(i, h):
        return w_all.at[pl.ds(pl.multiple_of(i * cols + h * piece, 16), piece)]

    def w_z(i, h, up):
        return copy(w_ref(i, h), w_ref(i, h), ws.at[0 if up else 1],
                    wr.at[i, h], b + ny if up else b - ny, v)

    def w_pass(i, h, up):
        return copy(w_ref(i, h), w_ref(i, h), ws.at[jnp.where(up, 0, 1)], wr.at[i, h], jnp.where(up, b + ny, b - ny), v)

    def w_y(h):
        return copy(w_over.at[pl.ds(h * piece, piece)], w_ref(b, h), wys.at[0], wr.at[b, h], over_y, v)

    def w_got(i, h):
        copy(w_ref(i, h), w_ref(i, h), wys.at[0], wr.at[i, h], over_y, v).wait_recv()

    near = z + 1 - 2 * lax.rem(z, 2)
    slabs = [z, near, jnp.where(low, 2, 1), jnp.where(low, 3, 0)]

    def h_send(i, bb, vv):
        return copy(h_all.at[hrow(i)], h_all.at[hrow(i)], hs.at[0], hr.at[i], bb, vv)

    def h_x():
        return h_send(me, b, over_x)

    def h_y():
        return h_send(me, over_y, v)

    def h_xy():
        return h_send(y * nv + over_x, over_y, v)

    def h_yx():
        return h_send((1 - y) * nv + v, b, over_x)

    def h_core(kx, ky):
        i = flip(y, ky) * nv + flip(x, kx) * 2 + core
        return h_send(i, b, over_core)

    def h_got(kx, ky, cc):
        i = flip(y, ky) * nv + flip(x, kx) * 2 + cc
        h_send(i, b, over_core).wait_recv()

    def window(zz):
        return pl.ds(pl.multiple_of(zz * slab + y * lo, 128), win)

    def mine_of(kx, ky):
        return flip(y, ky) * nv + flip(x, kx) * 2 + core

    def h_out(kx, ky, j):
        i = mine_of(kx, ky)
        return copy(h_all.at[hrow(i), window((far, across, near_end)[j])], h_end.at[hrow(i), pl.ds(j * win, win)],
                    us.at[0], ur.at[i], near_end * ny + y, v)

    def send_out(kx, ky):
        @pl.when(at_end)
        def _():
            for j in range(3):
                h_out(kx, ky, j).start()

    def end_copy(i):
        return copy(h_end.at[hrow(i)], h_end.at[hrow(i)], us.at[0], ur.at[i], b, over_core)

    def share_end(kx, ky):
        @pl.when(inside)
        def _():
            end_copy(mine_of(kx, ky)).wait_recv()
            end_copy(mine_of(kx, ky)).start()

    def code_copy(n):
        bb, vv, _ = peer(n)
        return copy(code_own, code_got.at[me], cs.at[0], cr.at[0], bb, vv)

    for h in range(2):
        w_y(h).start()
    for h in range(2):
        pl.when(has_up)(lambda: w_z(b, h, True).start())
        pl.when(has_down)(lambda: w_z(b, h, False).start())
    h_x().start()
    h_y().start()
    h_core(0, 0).start()

    def send_codes(count):
        for n in range(len(peers)):
            if sum(peers[n]) == count:
                code_copy(n).start()

    send_codes(1)
    for h in range(2):
        i = z * ny + 1 - y
        w_got(i, h)
        pl.when(has_up)(lambda: w_z(i, h, True).start())
        pl.when(has_down)(lambda: w_z(i, h, False).start())
    send_out(0, 0)

    def w_slab(zz, onward, which=(0, 1)):
        for k in which:
            for h in range(2):
                i = zz * ny + flip(y, k)
                w_got(i, h)
                if onward:
                    w_pass(i, h, zz < z).start()

    @pl.when(at_end)
    def _():
        w_slab(slabs[1], False)

    @pl.when(inside)
    def _():
        w_slab(slabs[1], True)
        w_slab(slabs[2], True)

    h_got(1, 0, core)
    pl.when(core == 0)(lambda: h_xy().start())
    h_core(1, 0).start()
    send_out(1, 0)
    h_got(0, 1, core)
    pl.when(core == 1)(lambda: h_yx().start())
    h_core(0, 1).start()
    send_out(0, 1)
    send_codes(2)

    @pl.when(at_end)
    def _():
        w_slab(slabs[2], False)

    @pl.when(inside)
    def _():
        w_slab(slabs[3], True)

    h_got(1, 1, core)
    h_core(1, 1).start()
    send_out(1, 1)
    send_codes(3)
    for kx in range(2):
        for ky in range(2):
            h_got(kx, ky, 1 - core)

    step = 2 * rows
    steps = tokens // step
    lines = lax.broadcasted_iota(jnp.int32, (8, rows), 0)

    def scores(n, zz, at=0, wide=slab):
        here = pl.ds(pl.multiple_of(zz * slab + at, 128), wide)
        there = pl.ds(pl.multiple_of(zz * slab + at, 16), wide)
        return jnp.dot(h_all[n * step:(n + 1) * step, here], w_all[there, :], preferred_element_type=f32)

    for j in range(nz - 1):
        for n in range(steps):
            span = pl.ds(n * step, step)
            if j:
                logits[span, :] += scores(n, slabs[j])
            else:
                logits[span, :] = scores(n, slabs[j])

    code_got[me] = code_own[...]
    others = pl.ds(0, group - 1)
    copy(code_got.at[others], code_got.at[others], cs.at[0], cr.at[0], b, over_x).wait_recv()
    for i in range(group):
        code_all[i * rows:(i + 1) * rows, :] = jnp.transpose(jnp.concatenate([code_got[i]] * (rows // 8), axis=0))

    early = lo
    pl.when(at_end)(lambda: w_slab(slabs[3], False, (0,)))
    for n in range(steps):
        logits[n * step:(n + 1) * step, :] += scores(n, slabs[3], y * (slab - early), early)
    pl.when(at_end)(lambda: w_slab(slabs[3], False, (1,)))

    sums = jnp.zeros((8, rows), f32)
    for n in range(steps):
        span = pl.ds(n * step, step)
        capped = softcap * jnp.tanh((logits[span, :] + scores(n, slabs[3], (1 - y) * early, slab - early)) * (1.0 / softcap))
        raised = jnp.exp(capped)
        logits[span, :] = capped
        expo[span, :] = raised
        total = jnp.broadcast_to(jnp.sum(raised, axis=1, keepdims=True), (step, 128))
        for k in range(2):
            turned = jnp.transpose(total[k * rows:(k + 1) * rows])
            sums = jnp.where(lines == 2 * n + k, turned[0:8], sums)
    stat_own[...] = sums

    def stat_copy(n):
        bb, vv, _ = peer(n)
        return copy(stat_own, stat_all.at[me], ss.at[0], sr.at[0], bb, vv)

    for n in range(len(peers)):
        stat_copy(n).start()

    ids = (lax.broadcasted_iota(jnp.int32, (step, half), 1) + (v * ny + y) * half).astype(f32)
    hit_total = jnp.zeros((step, 1), f32)
    for n in range(steps):
        span = pl.ds(n * step, step)
        capped = logits[span, :]
        hit = ids == code_all[span, 0:1]
        slope = 1.0 - (capped * (1.0 / softcap)) ** 2
        expo[span, :] = expo[span, :] * slope
        logits[span, :] = jnp.where(hit, slope, 0.0)
        hit_total = hit_total + jnp.sum(jnp.where(hit, capped, 0.0), axis=1, keepdims=True)
    hit_total = jnp.sum(hit_total, axis=0, keepdims=True)
    loss_one[...] = jnp.broadcast_to(hit_total, loss_one.shape)

    def hit_copy(n):
        bb, vv, _ = peer(n)
        return copy(loss_one, loss_all.at[me], ls.at[0], lr.at[0], bb, vv)

    for n in range(len(peers)):
        hit_copy(n).start()
    code_rows = jnp.zeros((8, rows), f32)
    for i in range(group):
        code_rows = jnp.where(lines == i, code_got[i], code_rows)
    weight = (code_rows >= 0).astype(f32)

    share_end(0, 0)
    share_end(1, 0)
    stat_all[me] = sums
    copy(stat_all.at[others], stat_all.at[others], ss.at[0], sr.at[0], b, over_x).wait_recv()
    partition = stat_all[0]
    for i in range(1, group):
        partition = partition + stat_all[i]
    scale = weight / partition

    lane_parts = [pl.ds(0, half - 128), pl.ds(half - 128, 128)]

    def delta_copy(p):
        here = lane_parts[p]
        return copy(delta.at[0, :, here], delta.at[1, :, here], es.at[0], (cr, er)[p].at[0], over_y, v)

    for n in range(steps):
        for k in range(2):
            i = 2 * n + k
            span = pl.ds(i * rows, rows)
            by_row = jnp.transpose(jnp.broadcast_to(scale[i:i + 1, :], (rows, rows)))
            factor = jnp.concatenate([by_row] * (half // rows), axis=1)
            delta[0, span, :] = (expo[span, :] * factor - logits[span, :]).astype(bf16)
    for p in range(2):
        delta_copy(p).start()

    chunks = range(half // 128)

    def chunk_of_delta(n):
        here = pl.ds(n * 128, 128)
        return copy(delta.at[0, :, here], d_end.at[:, here], zs.at[0], zr.at[n], near_end * ny + y, v)

    for n in chunks:
        pl.when(at_end)(lambda: chunk_of_delta(n).start())

    targets = [jnp.where(at_end, far, across), jnp.where(at_end, across, near), jnp.where(at_end, near_end, far), z]
    top = y * shift

    def over_tokens(left, right):
        return lax.dot_general(left, right, (((0,), (0,)), ((), ())), preferred_element_type=f32)

    def grad_share(zz, r):
        return over_tokens(h_all[:, window(zz)], delta[r])

    def sent(k, r):
        return grad_send.at[k, r, pl.ds(pl.multiple_of(top, 16), cols)]

    def r_copy(k, r):
        return copy(sent(k, r), r_in.at[z * 2 + r], rs.at[0], rr.at[z, r], targets[k] * ny + y, v)

    def relay_copy(n, p):
        src = grad_send.at[n, 1, pl.ds(pl.multiple_of(top, 16), cols), lane_parts[p]]
        return copy(src, far_in.at[n, :, lane_parts[p]], rs.at[0], fr.at[n, p], near_end * ny + y, v)

    def part_copy(k, p):
        src = grad_send.at[k, 1, pl.ds(pl.multiple_of(top, 16), cols), lane_parts[p]]
        return copy(src, r_in.at[z * 2 + 1, :, lane_parts[p]], rs.at[0], rr.at[z, 1], targets[k] * ny + y, v)

    def chunk_copy(k, n):
        here = pl.ds(n * 128, 128)
        src = grad_send.at[k, 0, pl.ds(pl.multiple_of(top, 16), cols), here]
        return copy(src, r_in.at[z * 2, :, here], rs.at[0], rr.at[z, 0], targets[k] * ny + y, v)

    def to_end():
        @pl.when(inside)
        def _():
            grad_send[1, 0] = grad_share(near, 0).astype(bf16)
            r_copy(1, 0).start()

    def keep():
        @pl.when(inside)
        def _():
            held[0] = grad_share(across, 0)
            held[1] = grad_share(far, 0)

    def chunk(n):
        first = n * 128

        @pl.when(inside)
        def _():
            if n == 0:
                for kx in range(2):
                    for ky in range(2):
                        end_copy(flip(y, ky) * nv + flip(x, kx) * 2 + 1 - core).wait_recv()
            chunk_of_delta(n).wait_recv()
            right = d_end[:, first:first + 128]
            for k, slot, j in ((0, 0, 1), (2, 1, 0)):
                share = held[slot, :, first:first + 128] + over_tokens(h_end[:, j * win:(j + 1) * win], right)
                grad_send[k, 0, :, first:first + 128] = share.astype(bf16)
                chunk_copy(k, n).start()
            grad_own[0, :, first:first + 128] += over_tokens(h_end[:, 2 * win:3 * win], right)

    def head_part(k, p):
        here = lane_parts[p]
        share = over_tokens(h_all[:, window(targets[k])], delta[1, :, here])
        if k:
            grad_send[k, 1, :, here] = share.astype(bf16)
            pl.when(at_end)(lambda: relay_copy(1, p).start())
            pl.when(inside)(lambda: part_copy(k, p).start())
        else:
            @pl.when(at_end)
            def _():
                grad_send[k, 1, :, here] = share.astype(bf16)
                relay_copy(0, p).start()

            @pl.when(inside)
            def _():
                held[0, :, here] = share

    def head_rest():
        share = grad_share(targets[2], 1)

        @pl.when(at_end)
        def _():
            grad_send[2, 1] = share.astype(bf16)
            r_copy(2, 1).start()

        @pl.when(inside)
        def _():
            held[1] = share

    cstep = chunk_of(cols, 64)

    def over_cols(body):
        def one(n, carry):
            body(pl.multiple_of(n * cstep, 16))
            return carry

        lax.fori_loop(0, cols // cstep, one, 0)

    def relay(k, n, p):
        lane = lane_parts[p]

        @pl.when(inside)
        def _():
            relay_copy(n, p).wait_recv()

            def add(m):
                here = pl.ds(pl.multiple_of(top + m, 16), cstep)
                there = pl.ds(m, cstep)
                grad_send[k, 1, here, lane] = (
                    held[k // 2, here, lane] + far_in[n, there, lane].astype(f32)).astype(bf16)

            over_cols(add)
            part_copy(k, p).start()

    groups = column_groups(width)
    blocks = [(1, 1), (1, 0), (0, 1), (0, 0)]
    unit = width // (width // 256)

    def span_of(g):
        first, n = groups[g]
        return pl.ds(first * unit, n * unit)

    y_first = (3,)

    def block(g, one, two, cc):
        kx, ky = (two, one) if g in y_first else (one, two)
        return flip(y, ky) * nv + flip(x, kx) * 2 + cc

    def core_copy(g, one, two):
        return copy(part.at[hrow(block(g, one, two, 1 - core)), span_of(g)], core_in.at[one, two, :, span_of(g)],
                    ds.at[0], wr.at[g, 0], b, over_core)

    def over_one(g):
        return (over_y, v) if g in y_first else (b, over_x)

    def over_two(g):
        return (b, over_x) if g in y_first else (over_y, v)

    def one_copy(g, two):
        return copy(x_out.at[two, :, span_of(g)], x_in.at[two, :, span_of(g)], xs.at[0], (hr if two else xr).at[g],
                    *over_one(g))

    def two_copy(g):
        return copy(y_out.at[:, span_of(g)], y_in.at[:, span_of(g)], ys.at[0], wr.at[g, 1], *over_two(g))

    def part_group(g):
        first, n = groups[g]

        def columns(j, carry):
            span = pl.ds(pl.multiple_of(j * unit, 128), unit)
            part[:, span] = lax.dot_general(
                delta[0], w_all[span, :], (((1,), (1,)), ((), ())), preferred_element_type=f32)
            return carry

        lax.fori_loop(first, first + n, columns, 0)
        for one, two in blocks:
            core_copy(g, one, two).start()

    hstep = 16

    def over_rows(body):
        def one(n, carry):
            body(pl.multiple_of(n * hstep, hstep))
            return carry

        lax.fori_loop(0, rows // hstep, one, 0)

    def core_sum(g):
        span = span_of(g)
        landed = core_in.at[:, :, :, span]
        copy(landed, landed, ds.at[0], wr.at[g, 0], b, over_core).wait_recv()
        for one, two in blocks:
            start = block(g, one, two, core) * rows

            def add(n):
                here = pl.ds(pl.multiple_of(start + n, hstep), hstep)
                both = part[here, span] + core_in[one, two, pl.ds(n, hstep), span]
                if one:
                    x_out[two, pl.ds(n, hstep), span] = both.astype(bf16)
                else:
                    part[here, span] = both

            over_rows(add)
            if one:
                one_copy(g, two).start()

    def one_sum(g):
        span = span_of(g)
        for two in (1, 0):
            one_copy(g, two).wait_recv()
            start = block(g, 0, two, core) * rows

            def add(n):
                here = pl.ds(pl.multiple_of(start + n, hstep), hstep)
                total = part[here, span] + x_in[two, pl.ds(n, hstep), span].astype(f32)
                if two:
                    y_out[pl.ds(n, hstep), span] = total.astype(bf16)
                else:
                    hid_out[pl.ds(n, hstep), span] = total

            over_rows(add)
            if two:
                two_copy(g).start()

    def two_sum(g):
        span = span_of(g)
        two_copy(g).wait_recv()

        def add(n):
            here = pl.ds(n, hstep)
            hid_out[here, span] += y_in[here, span].astype(f32)

        over_rows(add)

    count = len(groups)

    def plane_copy(k):
        return copy(loss_two, loss_zs.at[z], ms.at[0], mr.at[0], z_peer(k), v)

    def plane_loss():
        loss_all[me] = loss_one[...]
        copy(loss_all.at[others], loss_all.at[others], ls.at[0], lr.at[0], b, over_x).wait_recv()
        hits = loss_all[0]
        for i in range(1, group):
            hits = hits + loss_all[i]
        logs = jnp.sum(weight * jnp.log(partition), axis=1, keepdims=True)
        loss_two[...] = jnp.broadcast_to(jnp.sum(logs, axis=0, keepdims=True), (8, rows)) - hits
        for k in range(1, nz):
            plane_copy(k).start()

    part_group(0)
    part_group(1)
    to_end()
    plane_loss()
    core_sum(0)
    part_group(2)
    core_sum(1)
    share_end(0, 1)
    keep()
    part_group(3)
    core_sum(2)
    share_end(1, 1)
    grad_own[0] = grad_share(z, 0)
    part_group(4)
    core_sum(3)
    chunk(0)
    for g in range(5, count):
        part_group(g)
        core_sum(g - 1)
    core_sum(count - 1)
    for n in chunks[1:-1]:
        chunk(n)
    one_sum(0)

    delta_copy(0).wait_recv()
    head_part(0, 0)
    head_part(1, 0)
    chunk(len(chunks) - 1)
    delta_copy(1).wait_recv()
    head_part(0, 1)
    head_part(1, 1)
    one_sum(1)
    head_rest()
    grad_own[1] = grad_share(z, 1)
    one_sum(2)
    relay(2, 0, 0)

    copy(w_over, w_over, wys.at[0], wr.at[0, 0], over_y, v).wait_send()
    for n in range(1, nz):
        sent_rows = w_all.at[pl.ds(0, n * slab)]
        for way, slabs_sent in ((0, z + 1), (1, nz - z)):
            going = (slabs_sent == n) & (has_down if way else has_up)
            pl.when(going)(lambda: copy(sent_rows, sent_rows, ws.at[way], wr.at[0, 0], b, over_x).wait_send())
    seven = h_all.at[pl.ds(0, 7 * rows)]
    copy(seven, seven, hs.at[0], hr.at[0], b, over_x).wait_send()
    for got, sem in ((code_got, cs), (stat_all, ss), (loss_all, ls)):
        copy(got.at[others], got.at[others], sem.at[0], sem.at[0], b, over_x).wait_send()
    one_sum(3)
    two_sum(0)
    copy(delta.at[0], delta.at[1], es.at[0], cr.at[0], over_y, v).wait_send()
    relay(0, 1, 0)
    copy(core_in, core_in, ds.at[0], wr.at[0, 0], b, over_core).wait_send()
    one_sum(4)
    two_sum(1)
    relay(2, 0, 1)
    relay(0, 1, 1)
    for g in range(5, count):
        one_sum(g)
    two_sum(2)
    for g in range(4, count - 1):
        two_sum(g)

    def r_got(zz, r):
        whole = r_in.at[zz * 2 + r]
        copy(whole, whole, rs.at[0], rr.at[zz, r], z_peer(1), v).wait_recv()

    def lanes(r):
        return pl.ds(pl.multiple_of(flip(y, r) * half, 128), half)

    def head_sum(r):
        r_got(across, r)

        def add(n):
            here = pl.ds(n, cstep)
            total = grad_own[r, pl.ds(pl.multiple_of(top + n, 16), cstep), :]
            head_out[here, lanes(r)] = total + r_in[across * 2 + r, here, :].astype(f32)

        over_cols(add)

        def by_near():
            r_got(near, r)

            def last(n):
                here = pl.ds(n, cstep)
                head_out[here, lanes(r)] += r_in[near * 2 + r, here, :].astype(f32)

            over_cols(last)

        if r:
            by_near()
        else:
            pl.when(at_end)(by_near)

    head_sum(0)
    loss_zs[z] = loss_two[...]
    along = loss_zs.at[pl.ds(0, nz - 1)]
    copy(along, along, ms.at[0], mr.at[0], z_peer(1), v).wait_recv()
    losses = loss_zs[0]
    for i in range(1, nz):
        losses = losses + loss_zs[i]
    loss_out[...] = losses * (1.0 / (tokens * nz))
    copy(along, along, ms.at[0], mr.at[0], z_peer(1), v).wait_send()
    two_sum(3)
    two_sum(count - 1)
    head_sum(1)

    rows_out = h_end.at[pl.ds(0, tokens // 2)]
    for part_sent, sem in ((x_out, xs), (y_out, ys), (rows_out, us)):
        copy(part_sent, part_sent, sem.at[0], sem.at[0], b, over_x).wait_send()

    @pl.when(at_end)
    def _():
        for part_sent, sem in ((d_end, zs), (r_in.at[pl.ds(0, 3)], rs)):
            copy(part_sent, part_sent, sem.at[0], sem.at[0], b, over_x).wait_send()

    @pl.when(inside)
    def _():
        six = r_in.at[pl.ds(0, 6)]
        copy(six, six, rs.at[0], rs.at[0], b, over_x).wait_send()


def finish_kernel(head_in, hid_in, loss_in, head_out, hid_out, loss_out, sem):
    parts = sem.shape[1]
    moves = []
    for k, (src, dst) in enumerate(((hid_in, hid_out), (head_in, head_out))):
        size = src.shape[0] // parts
        for n in range(parts):
            here = pl.ds(n * size, size)
            moves.append(pltpu.make_async_copy(src.at[here], dst.at[here], sem.at[k, n]))
    for one in moves:
        one.start()
    loss_out[0, 0] = loss_in[0, 0]
    for one in moves:
        one.wait()


def plane_local(hidden, head_weight, targets, valid_mask):
    nz, ny, nv = 4, 2, 4
    rows, width = hidden.shape
    entries, cols = head_weight.shape
    half = entries // ny
    group = ny * nv
    tokens = rows * group
    shift = cols % 128
    win = -(-(cols + shift) // 128) * 128
    vm = pltpu.VMEM
    dma = pltpu.SemaphoreType.DMA
    count = len(column_groups(width))
    line = vm((8, rows), f32)
    buffers = [
        vm((tokens, width), bf16), vm((width, half), bf16), vm((cols, half), bf16),
        vm((1, rows), jnp.int32), vm((1, rows), jnp.int32), line, vm((group, 8, rows), f32), vm((tokens, 128), f32),
        vm((tokens, half), f32), vm((tokens, half), f32), vm((2, tokens, half), bf16),
        line, vm((group, 8, rows), f32), line, line, vm((group, 8, rows), f32), vm((nz, 8, rows), f32),
        vm((2, win, half), f32), vm((2, win, half), f32), vm((3, 2, win, half), bf16),
        vm((2, cols, half), bf16), vm((nz * 2, cols, half), bf16), vm((tokens, 3 * win), bf16), vm((tokens, half), bf16),
        vm((tokens, width), f32), vm((2, 2, rows, width), f32),
        vm((2, rows, width), bf16), vm((2, rows, width), bf16), vm((rows, width), bf16), vm((rows, width), bf16),
    ]
    sems = [
        dma((5,)), dma((1,)), dma((group,)), dma((2,)), dma((8, 2)), dma((1,)),
        dma((1,)), dma((1,)), dma((1,)), dma((1,)), dma((1,)), dma((1,)), dma((1,)), dma((1,)),
        dma((1,)), dma((1,)), dma((1,)), dma((nz, 2)), dma((2, 2)), dma((1,)), dma((half // 128,)), dma((1,)), dma((group,)),
        dma((1,)), dma((1,)), dma((count,)), dma((1,)),
    ]
    whole = pl.BlockSpec(memory_space=vm)
    head_t, hidden_grad, loss = pl.pallas_call(
        plane_kernel,
        out_shape=(
            vm((cols, entries), f32),
            vm((rows, width), f32),
            vm((8, rows), f32),
        ),
        in_specs=[pl.BlockSpec(memory_space=pl.ANY)] * 4,
        out_specs=(whole,) * 3,
        scratch_shapes=buffers + sems,
        compiler_params=pltpu.CompilerParams(
            collective_id=1, has_side_effects=True, vmem_limit_bytes=58 * 1024 * 1024),
    )(hidden, jnp.transpose(head_weight), targets[None, :], valid_mask[None, :])
    anywhere = pl.BlockSpec(memory_space=pl.ANY)
    head_t, hidden_grad, loss = pl.pallas_call(
        finish_kernel,
        out_shape=(
            jax.ShapeDtypeStruct((cols, entries), f32),
            jax.ShapeDtypeStruct((rows, width), f32),
            jax.ShapeDtypeStruct((1, 1), f32),
        ),
        in_specs=[whole] * 3,
        out_specs=(anywhere, anywhere, pl.BlockSpec(memory_space=pltpu.SMEM)),
        scratch_shapes=[dma((2, 4))],
        compiler_params=pltpu.CompilerParams(vmem_limit_bytes=1024 * 1024),
    )(head_t, hidden_grad, loss)
    return jnp.transpose(head_t), hidden_grad, loss[0, 0]


def in_planes(nb, nv, hidden, head_weight, targets, valid_mask):
    rows, width = hidden.shape
    entries, cols = head_weight.shape
    fits = nb == 8 and nv == 4 and rows == 128 and width % 256 == 0 and width >= 3072
    fits = fits and len(column_groups(width)) <= 8
    return fits and entries % 256 == 0 and entries >= 512 and cols % 32 == 0 and (2 * cols) % 128 == 0


def device(nb, nv, *arrays):
    if in_planes(nb, nv, *arrays):
        return plane_local(*arrays)
    return local(nb, nv, *arrays)


def solution(mesh):
    placed = (
        P(("batch", "vocab"), None),
        P("vocab", "batch"),
        P(("batch", "vocab")),
        P(("batch", "vocab")),
    )
    return jax.shard_map(
        functools.partial(device, mesh.shape["batch"], mesh.shape["vocab"]),
        mesh=mesh,
        in_specs=placed,
        out_specs=(P("vocab", "batch"), P(("batch", "vocab"), None), P()),
        check_vma=False,
    )
```

```python
import functools

import jax
import jax.numpy as jnp
from jax import lax
from jax.experimental import pallas as pl
from jax.experimental.pallas import tpu as pltpu
from jax.sharding import PartitionSpec as P

softcap = 30.0
MESH = pl.DeviceIdType.MESH
f32, bf16 = jnp.float32, jnp.bfloat16


def chunk_of(length, most):
    return max(s for s in range(16, most + 1, 16) if length % s == 0)


def kernel(sizes, h_in, w_in, code_in, head_out, hid_out, loss_out, h_all, w_all, code_got, code_all,
           logits, delta, stat_own, stat_all, loss_own, loss_all, grad, grad_send, r_in,
           part, core_in, x_out, x_in, y_out, y_in, far_own, far_in, *sems):
    nz, ny, nx, nv = sizes
    (own_sem, hs, hf, hd, hr, ws_up, ws_dn, ws_y, wr, cs, cr, ss, sr, ls, lr,
     rs, rr, ds, dr, xs, xr, ys, yr, fs, fr) = sems
    nb = nz * ny
    rows, width = h_in.shape
    cols, half = w_in.shape[1:]
    group = ny * nv
    tokens = rows * group
    entries = ny * half
    b, v = lax.axis_index("batch"), lax.axis_index("vocab")
    z, y = lax.div(b, ny), lax.rem(b, ny)
    x, core = lax.div(v, 2), lax.rem(v, 2)
    other = x * 2 + 1 - core
    me = y * nv + v

    def at(bb, vv):
        return {"batch": bb, "vocab": vv}

    def copy(src, dst, send, recv, bb, vv):
        return pltpu.make_async_remote_copy(
            src_ref=src, dst_ref=dst, send_sem=send, recv_sem=recv, device_id=at(bb, vv), device_id_type=MESH)

    def hrow(i):
        return pl.ds(pl.multiple_of(i * rows, 16), rows)

    def wrow(i):
        return pl.ds(pl.multiple_of(i * cols, 16), cols)

    def turn_y(k):
        return lax.rem(y + k, ny)

    def turn_x(k):
        return lax.rem(x + k, nx)

    peers = [(k, j) for k in range(ny) for j in range(nv) if k or j]

    def peer(n):
        k, j = peers[n]
        return z * ny + turn_y(k), lax.rem(v + j, nv), turn_y(k) * nv + lax.rem(v + j, nv)

    barrier = pltpu.get_barrier_semaphore()
    for k in range(1, nb):
        pl.semaphore_signal(barrier, inc=1, device_id=at(lax.rem(b + k, nb), v), device_id_type=MESH)
    met = [n for n in range(len(peers)) if peers[n][1]]
    for n in met:
        bb, vv, _ = peer(n)
        pl.semaphore_signal(barrier, inc=1, device_id=at(bb, vv), device_id_type=MESH)
    pl.semaphore_wait(barrier, nb - 1 + len(met))

    def w_z(zz, yy, up, own=False):
        i = zz * ny + yy
        dst = w_all.at[wrow(i)]
        sem = (ws_up if up else ws_dn).at[i]
        return copy(w_in.at[y] if own else dst, dst, sem, wr.at[i], b + ny if up else b - ny, v)

    def w_y(k):
        return copy(w_in.at[turn_y(k)], w_all.at[wrow(b)], ws_y.at[k - 1], wr.at[b], z * ny + turn_y(k), v)

    def w_got(zz, yy):
        w_z(zz, yy, True).wait_recv()

    has_up, has_down = z + 1 < nz, z >= 1

    def h_send(n_src, sem, bb, vv, own=False):
        dst = h_all.at[hrow(n_src)]
        return copy(h_in if own else dst, dst, sem, hr.at[n_src], bb, vv)

    def h_x(k):
        return h_send(me, hs.at[k - 1], b, turn_x(k) * 2 + core, True)

    def h_y(k):
        return h_send(me, hs.at[nx + k - 1], z * ny + turn_y(k), v, True)

    def h_xy(kx, ky):
        return h_send(y * nv + turn_x(kx) * 2 + core, hf.at[kx, ky], z * ny + turn_y(ky), v)

    def h_yx(kx, ky):
        return h_send(turn_y(ky) * nv + v, hf.at[kx, ky], b, turn_x(kx) * 2 + core)

    def h_core(kx, ky):
        i = turn_y(ky) * nv + turn_x(kx) * 2 + core
        return h_send(i, hd.at[kx, ky], b, other, kx == 0 and ky == 0)

    def h_got(kx, ky, cc):
        i = turn_y(ky) * nv + turn_x(kx) * 2 + cc
        h_send(i, hd.at[kx, ky], b, other).wait_recv()

    def code_copy(n):
        bb, vv, _ = peer(n)
        return copy(code_in, code_got.at[me], cs.at[n], cr.at[me], bb, vv)

    for k in range(1, ny):
        w_y(k).start()
    pl.when(has_up)(lambda: w_z(z, y, True, True).start())
    pl.when(has_down)(lambda: w_z(z, y, False, True).start())
    for k in range(1, nx):
        h_x(k).start()
    for k in range(1, ny):
        h_y(k).start()
    for n in range(len(peers)):
        code_copy(n).start()
    h_core(0, 0).start()
    local = [
        pltpu.make_async_copy(w_in.at[y], w_all.at[wrow(b)], own_sem.at[0]),
        pltpu.make_async_copy(h_in, h_all.at[hrow(me)], own_sem.at[1]),
    ]
    for one in local:
        one.start()

    for k in range(1, ny):
        w_got(z, turn_y(k))
        pl.when(has_up)(lambda: w_z(z, turn_y(k), True).start())
        pl.when(has_down)(lambda: w_z(z, turn_y(k), False).start())

    def h_pass():
        for kx in range(1, nx):
            h_got(kx, 0, core)
            for ky in range(1, ny):
                pl.when(core == 0)(lambda: h_xy(kx, ky).start())
            h_core(kx, 0).start()
        for ky in range(1, ny):
            h_got(0, ky, core)
            for kx in range(1, nx):
                pl.when(core == 1)(lambda: h_yx(kx, ky).start())
            h_core(0, ky).start()

    def h_rest():
        for kx in range(1, nx):
            for ky in range(1, ny):
                h_got(kx, ky, core)
                h_core(kx, ky).start()

    for k in range(1, nz):
        for j in range(ny):
            yy = turn_y(j)

            @pl.when(z - k >= 0)
            def _():
                w_got(z - k, yy)
                pl.when(has_up)(lambda: w_z(z - k, yy, True).start())

            @pl.when(z + k < nz)
            def _():
                w_got(z + k, yy)
                pl.when(has_down)(lambda: w_z(z + k, yy, False).start())
        if k == 1:
            h_pass()
        if k == min(2, nz - 1):
            h_rest()

    for one in local:
        one.wait()
    for kx in range(nx):
        for ky in range(ny):
            h_got(kx, ky, 1 - core)
    code_got[me] = code_in[...]
    for n in range(len(peers)):
        bb, vv, i = peer(n)
        copy(code_in, code_got.at[i], cs.at[n], cr.at[i], bb, vv).wait_recv()
    for i in range(group):
        code_all[i * rows:(i + 1) * rows, :] = jnp.transpose(jnp.concatenate([code_got[i]] * 16, axis=0))

    step = chunk_of(tokens, 256)
    lanes = lax.broadcasted_iota(jnp.int32, (step, 128), 1)
    first = v * entries + y * half

    def span_of(n):
        return pl.ds(pl.multiple_of(n * step, step), step)

    def hits(n):
        ids = lax.broadcasted_iota(jnp.int32, (step, half), 1) + first
        return ids == code_all[span_of(n), 0:1].astype(jnp.int32)

    for n in range(tokens // step):
        span = pl.ds(n * step, step)
        scores = jnp.dot(h_all[span, :], w_all[...], preferred_element_type=f32)
        capped = softcap * jnp.tanh(scores * (1.0 / softcap))
        logits[span, :] = capped
        total = jnp.sum(jnp.exp(capped), axis=1, keepdims=True)
        hit_sum = jnp.sum(jnp.where(hits(n), capped, 0.0), axis=1, keepdims=True)
        turned = jnp.transpose(jnp.where(lax.rem(lanes, 8) < 4, total, hit_sum))
        stat_own[:, n * step:(n + 1) * step] = turned[0:8]

    def stat_copy(n):
        bb, vv, _ = peer(n)
        return copy(stat_own, stat_all.at[me], ss.at[n], sr.at[me], bb, vv)

    for n in range(len(peers)):
        stat_copy(n).start()
    for n in range(len(peers)):
        bb, vv, i = peer(n)
        copy(stat_own, stat_all.at[i], ss.at[n], sr.at[i], bb, vv).wait_recv()
    stats = stat_own[...]
    for n in range(len(peers)):
        stats = stats + stat_all[peer(n)[2]]

    loss = jnp.zeros((1, 1), f32)
    for n in range(tokens // step):
        span = pl.ds(n * step, step)
        weight = (code_all[span, 0:1] >= 0).astype(f32)
        back = jnp.transpose(jnp.concatenate([stats[:, n * step:(n + 1) * step]] * 16, axis=0))
        partition, target_logit = back[:, 0:1], back[:, 4:5]
        loss = loss + jnp.sum(weight * (jnp.log(partition) - target_logit), axis=0, keepdims=True)
        capped = logits[span, :]
        slope = 1.0 - (capped * (1.0 / softcap)) ** 2
        delta[span, :] = ((jnp.exp(capped) * (weight / partition) - jnp.where(hits(n), weight, 0.0)) * slope
                          ).astype(bf16)
    loss_own[...] = jnp.broadcast_to(loss, loss_own.shape)

    def loss_copy(k):
        return copy(loss_own, loss_all.at[b], ls.at[k - 1], lr.at[b], lax.rem(b + k, nb), v)

    def r_copy(zz, yy):
        i = zz * ny + yy
        return copy(grad_send.at[wrow(i)], r_in.at[z, y], rs.at[i], rr.at[b], i, v)

    def grad_share(span):
        return lax.dot_general(h_all[:, span], delta[...], (((0,), (0,)), ((), ())), preferred_element_type=f32)

    slab = ny * cols
    relay = nz == 4 and slab % 128 == 0
    turn = jnp.where(z * 2 >= nz, 1, nz - 1)
    order = [lax.rem(z + turn * k, nz) for k in range(1, nz)] + [z]
    at_end = (z == 0) | (z == nz - 1)
    far = jnp.where(z * 2 >= nz, 0, nz - 1)
    near = jnp.where(z * 2 >= nz, z - 1, z + 1)

    def far_copy(yy):
        return copy(grad_send.at[wrow(far * ny + yy)], far_in.at[yy], fs.at[yy], fr.at[yy], near * ny + y, v)

    def direct(zz):
        return jnp.logical_not(at_end & (zz == far))
    if slab % 128 == 0:
        mine = y * cols
        for n in range(nz):
            zz = order[n]
            span = pl.ds(pl.multiple_of(zz * slab, 128), slab)
            share = grad_share(span)
            held = relay and n == 1
            if n == nz - 1:
                grad[...] = share
            if held:
                @pl.when(jnp.logical_not(at_end))
                def _():
                    far_own[...] = share

                @pl.when(at_end)
                def _():
                    grad_send[span, :] = share.astype(bf16)
                    for k in range(ny):
                        r_copy(zz, turn_y(k)).start()
            else:
                grad_send[span, :] = share.astype(bf16)
                for k in range(ny):
                    yy = turn_y(k)
                    if relay and n == 0:
                        pl.when(at_end)(lambda: far_copy(yy).start())
                        pl.when(jnp.logical_not(at_end))(lambda: r_copy(zz, yy).start())
                    elif n < nz - 1 or k:
                        r_copy(zz, yy).start()
    else:
        mine = b * cols
        wide = chunk_of(width, 256)

        def grad_step(j, carry):
            span = pl.ds(pl.multiple_of(j * wide, wide), wide)
            share = grad_share(span)
            grad[span, :] = share
            grad_send[span, :] = share.astype(bf16)
            return carry

        lax.fori_loop(0, width // wide, grad_step, 0)
        for n in range(nz):
            for k in range(ny):
                if n < nz - 1 or k:
                    r_copy(order[n], turn_y(k)).start()
    for k in range(1, nb):
        loss_copy(k).start()

    wide = chunk_of(width, 256)

    def part_step(j, carry):
        span = pl.ds(pl.multiple_of(j * wide, wide), wide)
        part[:, span] = lax.dot_general(
            delta[...], w_all[span, :], (((1,), (1,)), ((), ())), preferred_element_type=f32)
        return carry

    lax.fori_loop(0, width // wide, part_step, 0)

    def core_copy(kx, ky):
        i = turn_y(ky) * nv + turn_x(kx) * 2 + 1 - core
        return copy(part.at[hrow(i)], core_in.at[kx, ky], ds.at[kx, ky], dr.at[kx, ky], b, other)

    def x_copy(kx, ky):
        return copy(x_out.at[kx - 1, ky], x_in.at[kx - 1, ky], xs.at[kx, ky], xr.at[kx, ky],
                    b, turn_x(kx) * 2 + core)

    def y_copy(ky):
        return copy(y_out.at[ky - 1], y_in.at[ky - 1], ys.at[ky], yr.at[ky], z * ny + turn_y(ky), v)

    ways = [(kx % nx, ky % ny) for kx in range(1, nx + 1) for ky in range(1, ny + 1)]
    for kx, ky in ways:
        core_copy(kx, ky).start()
    hstep = 16

    def over_rows(start, body):
        def one(r, carry):
            body(pl.ds(pl.multiple_of(r * hstep, hstep), hstep),
                 pl.ds(pl.multiple_of(start + r * hstep, hstep), hstep))
            return carry

        lax.fori_loop(0, rows // hstep, one, 0)

    def start_of(kx, ky):
        return (turn_y(ky) * nv + turn_x(kx) * 2 + core) * rows

    for kx, ky in ways:
        core_copy(kx, ky).wait_recv()

        def core_sum(span, here):
            both = part[here, :] + core_in[kx, ky, span, :]
            if kx:
                x_out[kx - 1, ky, span, :] = both.astype(bf16)
            else:
                part[here, :] = both

        over_rows(start_of(kx, ky), core_sum)
        if kx:
            x_copy(kx, ky).start()

    cstep = chunk_of(cols, 64)

    def over_cols(body):
        def one(r, carry):
            body(pl.multiple_of(r * cstep, 16))
            return carry

        lax.fori_loop(0, cols // cstep, one, 0)

    if relay:
        @pl.when(jnp.logical_not(at_end))
        def _():
            for k in range(ny):
                yy = turn_y(k)
                far_copy(yy).wait_recv()

                def far_sum(r):
                    here = pl.ds(pl.multiple_of(yy * cols + r, 16), cstep)
                    there = pl.ds(pl.multiple_of((far * ny + yy) * cols + r, 16), cstep)
                    grad_send[there, :] = (far_own[here, :] + far_in[yy, pl.ds(r, cstep), :].astype(f32)).astype(bf16)

                over_cols(far_sum)
                r_copy(far, yy).start()

    for ky in [k % ny for k in range(1, ny + 1)]:
        for kx in range(1, nx):
            x_copy(kx, ky).wait_recv()

        def x_sum(span, here):
            total = part[here, :]
            for kx in range(1, nx):
                total = total + x_in[kx - 1, ky, span, :].astype(f32)
            if ky:
                y_out[ky - 1, span, :] = total.astype(bf16)
            else:
                hid_out[span, :] = total

        over_rows(start_of(0, ky), x_sum)
        if ky:
            y_copy(ky).start()

    def r_got(zz, yy):
        i = zz * ny + yy
        copy(grad_send.at[wrow(i)], r_in.at[zz, yy], rs.at[i], rr.at[i], i, v).wait_recv()

    for k in range(1, ny):
        r_got(z, turn_y(k))

    def first_sum(r):
        head_out[y, pl.ds(r, cstep), :] = grad[pl.ds(pl.multiple_of(mine + r, 16), cstep), :]
        for k in range(1, ny):
            head_out[turn_y(k), pl.ds(r, cstep), :] = r_in[z, turn_y(k), pl.ds(r, cstep), :].astype(f32)

    over_cols(first_sum)
    hops = [jnp.where(z * 2 >= nz, lax.rem(z + nz - n, nz), lax.rem(z + n, nz)) for n in range(1, nz)]
    for n in range(1, nz):
        zz = hops[n - 1]
        if n == nz - 1:
            for ky in range(1, ny):
                y_copy(ky).wait_recv()

                def y_sum(span, here):
                    hid_out[span, :] += y_in[ky - 1, span, :].astype(f32)

                over_rows(0, y_sum)

        def more_sum(r):
            for k in range(ny):
                head_out[turn_y(k), pl.ds(r, cstep), :] += r_in[zz, turn_y(k), pl.ds(r, cstep), :].astype(f32)

        def arrived():
            for k in range(ny):
                r_got(zz, turn_y(k))
            over_cols(more_sum)

        if relay:
            pl.when(direct(zz))(arrived)
        else:
            arrived()

    losses = loss_own[...]
    for k in range(1, nb):
        i = lax.rem(b + k, nb)
        copy(loss_own, loss_all.at[i], ls.at[k - 1], lr.at[i], i, v).wait_recv()
        losses = losses + loss_all[i]
    loss_out[...] = losses * (1.0 / (tokens * nb))

    for j in range(ny):
        yy = turn_y(j)
        pl.when(has_up)(lambda: w_z(z, yy, True, j == 0).wait_send())
        pl.when(has_down)(lambda: w_z(z, yy, False, j == 0).wait_send())
        for k in range(1, nz):
            @pl.when(z - k >= 0)
            def _():
                pl.when(has_up)(lambda: w_z(z - k, yy, True).wait_send())

            @pl.when(z + k < nz)
            def _():
                pl.when(has_down)(lambda: w_z(z + k, yy, False).wait_send())
    for k in range(1, ny):
        w_y(k).wait_send()
        h_y(k).wait_send()
        y_copy(k).wait_send()
    for k in range(1, nx):
        h_x(k).wait_send()
        for ky in range(1, ny):
            pl.when(core == 0)(lambda: h_xy(k, ky).wait_send())
            pl.when(core == 1)(lambda: h_yx(k, ky).wait_send())
    for kx, ky in ways:
        h_core(kx, ky).wait_send()
        core_copy(kx, ky).wait_send()
        if kx:
            x_copy(kx, ky).wait_send()
    for n in range(len(peers)):
        code_copy(n).wait_send()
        stat_copy(n).wait_send()
    for k in range(1, nb):
        loss_copy(k).wait_send()
    for n in range(nz):
        for k in range(ny):
            yy = turn_y(k)
            if relay and n == 0:
                pl.when(at_end)(lambda: far_copy(yy).wait_send())
                pl.when(jnp.logical_not(at_end))(lambda: r_copy(order[n], yy).wait_send())
            elif n < nz - 1 or k:
                r_copy(order[n], yy).wait_send()


def local(nb, nv, hidden, head_weight, targets, valid_mask):
    nx = nv // 2
    ny = nx if nx <= 2 and nb % nx == 0 else 1
    nz = nb // ny
    rows, width = hidden.shape
    entries, cols = head_weight.shape
    half = entries // ny
    group = ny * nv
    tokens = rows * group
    code = jnp.broadcast_to(jnp.where(valid_mask != 0, targets, -1).astype(f32)[None, :], (8, rows))
    weight = jnp.transpose(head_weight.reshape(ny, half, cols), (0, 2, 1))
    vm = pltpu.VMEM
    dma = pltpu.SemaphoreType.DMA
    slab = ny * cols
    ly, lx = max(ny - 1, 1), max(nx - 1, 1)
    buffers = [
        vm((tokens, width), bf16), vm((width, half), bf16), vm((group, 8, rows), f32), vm((tokens, 128), f32),
        vm((tokens, half), f32), vm((tokens, half), bf16),
        vm((8, tokens), f32), vm((group, 8, tokens), f32), vm((8, 128), f32), vm((nb, 8, 128), f32),
        vm((slab if slab % 128 == 0 else width, half), f32), vm((width, half), bf16), vm((nz, ny, cols, half), bf16),
        vm((tokens, width), f32), vm((nx, ny, rows, width), f32),
        vm((lx, ny, rows, width), bf16), vm((lx, ny, rows, width), bf16),
        vm((ly, rows, width), bf16), vm((ly, rows, width), bf16),
        vm((slab if nz == 4 else 16, half), f32), vm((ny, cols if nz == 4 else 16, half), bf16),
    ]
    sems = [
        dma((2,)), dma((nx + ny,)), dma((nx, ny)), dma((nx, ny)), dma((group,)), dma((nb,)), dma((nb,)),
        dma((ly,)), dma((nb,)), dma((group,)), dma((group,)), dma((group,)), dma((group,)), dma((nb,)), dma((nb,)),
        dma((nb,)), dma((nb,)), dma((nx, ny)), dma((nx, ny)), dma((nx, ny)), dma((nx, ny)), dma((ny,)), dma((ny,)),
        dma((ny,)), dma((ny,)),
    ]
    whole = pl.BlockSpec(memory_space=vm)
    head_t, hidden_grad, loss = pl.pallas_call(
        functools.partial(kernel, (nz, ny, nx, nv)),
        out_shape=(
            jax.ShapeDtypeStruct((ny, cols, half), f32),
            jax.ShapeDtypeStruct((rows, width), f32),
            jax.ShapeDtypeStruct((8, 128), f32),
        ),
        in_specs=[whole] * 3,
        out_specs=(whole,) * 3,
        scratch_shapes=buffers + sems,
        compiler_params=pltpu.CompilerParams(
            collective_id=0, has_side_effects=True, vmem_limit_bytes=67043328),
    )(hidden, weight, code)
    return jnp.transpose(head_t, (0, 2, 1)).reshape(entries, cols), hidden_grad, loss[0, 0]


def column_groups(width):
    left = width // 256 - 11
    sizes = [1, 2, 3, 2]
    while left > 0:
        sizes.append(min(3, left))
        left -= sizes[-1]
    sizes += [2, 1]
    starts = [sum(sizes[:n]) for n in range(len(sizes))]
    return [(s, n) for s, n in zip(starts, sizes)]


def plane_kernel(h_in, w_in, ids_in, mask_in, head_out, hid_out, loss_out, h_all, w_all, w_over, ids_own, mask_own,
                 code_own, code_got, code_all,
                 logits, expo, delta, stat_own, stat_all, loss_one, loss_two, loss_all, loss_zs,
                 grad_own, held, grad_send, far_in, r_in, h_end, d_end, part, core_in, x_out, x_in, y_out, y_in, *sems):
    (own_sem, hs, hr, ws, wr, wys, cs, cr, ss, sr, ls, lr, ms, mr,
     es, er, rs, rr, fr, zs, zr, us, ur, ds, xs, xr, ys) = sems
    nz, ny, nv = 4, 2, 4
    nb = nz * ny
    rows, width = h_in.shape
    cols, half = w_in.shape[0], w_in.shape[1] // ny
    piece = cols // 2
    group = ny * nv
    tokens = rows * group
    slab = ny * cols
    shift, lo = cols % 128, cols - cols % 128
    win = -(-(cols + shift) // 128) * 128
    b, v = lax.axis_index("batch"), lax.axis_index("vocab")
    z, y = lax.div(b, ny), lax.rem(b, ny)
    x, core = lax.div(v, 2), lax.rem(v, 2)
    me = y * nv + v
    low = z * 2 < nz
    at_end = (z == 0) | (z == nz - 1)
    inside = jnp.logical_not(at_end)

    def flip(a, k):
        return 1 - a if k else a

    def copy(src, dst, send, recv, bb, vv):
        return pltpu.make_async_remote_copy(
            src_ref=src, dst_ref=dst, send_sem=send, recv_sem=recv,
            device_id={"batch": bb, "vocab": vv}, device_id_type=MESH)

    def hrow(i):
        return pl.ds(pl.multiple_of(i * rows, 16), rows)

    far = jnp.where(low, nz - 1, 0)
    across = jnp.where(low, 2, 1)
    near_end = jnp.where(low, 1, 2)
    over_x, over_y, over_core = (1 - x) * 2 + core, z * ny + 1 - y, x * 2 + 1 - core
    peers = [(ky, kx, kc) for ky in range(2) for kx in range(2) for kc in range(2) if ky or kx or kc]

    def peer(n):
        ky, kx, kc = peers[n]
        yy, vv = flip(y, ky), flip(x, kx) * 2 + flip(core, kc)
        return z * ny + yy, vv, yy * nv + vv

    def z_peer(k):
        return lax.rem(z + k, nz) * ny + y

    has_up, has_down = z + 1 < nz, z >= 1
    barrier = pltpu.get_barrier_semaphore()

    def greet(bb, vv):
        pl.semaphore_signal(barrier, inc=1, device_id={"batch": bb, "vocab": vv}, device_id_type=MESH)

    pl.when(has_up)(lambda: greet(b + ny, v))
    pl.when(has_down)(lambda: greet(b - ny, v))
    greet(over_y, v)
    greet(b, over_x)
    greet(b, over_core)
    first = pl.ds(pl.multiple_of(y * half, 128), half)
    second = pl.ds(pl.multiple_of((1 - y) * half, 128), half)
    local = [
        pltpu.make_async_copy(w_in.at[:, second], w_over, own_sem.at[0]),
        pltpu.make_async_copy(w_in.at[:, first], w_all.at[pl.ds(pl.multiple_of(b * cols, 16), cols)], own_sem.at[1]),
        pltpu.make_async_copy(ids_in, ids_own, own_sem.at[2]),
        pltpu.make_async_copy(mask_in, mask_own, own_sem.at[3]),
        pltpu.make_async_copy(h_in, h_all.at[hrow(me)], own_sem.at[4]),
    ]
    for one in local:
        one.start()
    for one in local[:2]:
        one.wait()
    pl.semaphore_wait(barrier, jnp.where(inside, 5, 4))

    def w_ref(i, h):
        return w_all.at[pl.ds(pl.multiple_of(i * cols + h * piece, 16), piece)]

    def w_z(i, h, up):
        return copy(w_ref(i, h), w_ref(i, h), ws.at[0 if up else 1],
                    wr.at[i, h], b + ny if up else b - ny, v)

    def w_pass(i, h, up):
        return copy(w_ref(i, h), w_ref(i, h), ws.at[jnp.where(up, 0, 1)], wr.at[i, h], jnp.where(up, b + ny, b - ny), v)

    def w_y(h):
        return copy(w_over.at[pl.ds(h * piece, piece)], w_ref(b, h), wys.at[0], wr.at[b, h], over_y, v)

    def w_got(i, h):
        copy(w_ref(i, h), w_ref(i, h), wys.at[0], wr.at[i, h], over_y, v).wait_recv()

    near = z + 1 - 2 * lax.rem(z, 2)
    slabs = [z, near, jnp.where(low, 2, 1), jnp.where(low, 3, 0)]

    def h_send(i, bb, vv):
        return copy(h_all.at[hrow(i)], h_all.at[hrow(i)], hs.at[0], hr.at[i], bb, vv)

    def h_x():
        return h_send(me, b, over_x)

    def h_y():
        return h_send(me, over_y, v)

    def h_xy():
        return h_send(y * nv + over_x, over_y, v)

    def h_yx():
        return h_send((1 - y) * nv + v, b, over_x)

    def h_core(kx, ky):
        i = flip(y, ky) * nv + flip(x, kx) * 2 + core
        return h_send(i, b, over_core)

    def h_got(kx, ky, cc):
        i = flip(y, ky) * nv + flip(x, kx) * 2 + cc
        h_send(i, b, over_core).wait_recv()

    def window(zz):
        return pl.ds(pl.multiple_of(zz * slab + y * lo, 128), win)

    def mine_of(kx, ky):
        return flip(y, ky) * nv + flip(x, kx) * 2 + core

    def h_out(kx, ky, j):
        i = mine_of(kx, ky)
        return copy(h_all.at[hrow(i), window((far, across, near_end)[j])], h_end.at[hrow(i), pl.ds(j * win, win)],
                    us.at[0], ur.at[i], near_end * ny + y, v)

    def send_out(kx, ky):
        @pl.when(at_end)
        def _():
            for j in range(3):
                h_out(kx, ky, j).start()

    def end_copy(i):
        return copy(h_end.at[hrow(i)], h_end.at[hrow(i)], us.at[0], ur.at[i], b, over_core)

    def share_end(kx, ky):
        @pl.when(inside)
        def _():
            end_copy(mine_of(kx, ky)).wait_recv()
            end_copy(mine_of(kx, ky)).start()

    def code_copy(n):
        bb, vv, _ = peer(n)
        return copy(code_own, code_got.at[me], cs.at[0], cr.at[0], bb, vv)

    for h in range(2):
        w_y(h).start()
    for h in range(2):
        pl.when(has_up)(lambda: w_z(b, h, True).start())
        pl.when(has_down)(lambda: w_z(b, h, False).start())
    for one in local[2:]:
        one.wait()
    code = jnp.where(mask_own[...] != 0, ids_own[...], -1).astype(f32)
    code_own[...] = jnp.broadcast_to(code, code_own.shape)
    h_x().start()
    h_y().start()
    h_core(0, 0).start()

    def send_codes(count):
        for n in range(len(peers)):
            if sum(peers[n]) == count:
                code_copy(n).start()

    send_codes(1)
    for h in range(2):
        i = z * ny + 1 - y
        w_got(i, h)
        pl.when(has_up)(lambda: w_z(i, h, True).start())
        pl.when(has_down)(lambda: w_z(i, h, False).start())
    send_out(0, 0)

    def w_slab(zz, onward, which=(0, 1)):
        for k in which:
            for h in range(2):
                i = zz * ny + flip(y, k)
                w_got(i, h)
                if onward:
                    w_pass(i, h, zz < z).start()

    @pl.when(at_end)
    def _():
        w_slab(slabs[1], False)

    @pl.when(inside)
    def _():
        w_slab(slabs[1], True)
        w_slab(slabs[2], True)

    h_got(1, 0, core)
    pl.when(core == 0)(lambda: h_xy().start())
    h_core(1, 0).start()
    send_out(1, 0)
    h_got(0, 1, core)
    pl.when(core == 1)(lambda: h_yx().start())
    h_core(0, 1).start()
    send_out(0, 1)
    send_codes(2)

    @pl.when(at_end)
    def _():
        w_slab(slabs[2], False)

    @pl.when(inside)
    def _():
        w_slab(slabs[3], True)

    h_got(1, 1, core)
    h_core(1, 1).start()
    send_out(1, 1)
    send_codes(3)
    for kx in range(2):
        for ky in range(2):
            h_got(kx, ky, 1 - core)

    step = 2 * rows
    steps = tokens // step
    lines = lax.broadcasted_iota(jnp.int32, (8, rows), 0)

    def scores(n, zz, at=0, wide=slab):
        here = pl.ds(pl.multiple_of(zz * slab + at, 128), wide)
        there = pl.ds(pl.multiple_of(zz * slab + at, 16), wide)
        return jnp.dot(h_all[n * step:(n + 1) * step, here], w_all[there, :], preferred_element_type=f32)

    for j in range(nz - 1):
        for n in range(steps):
            span = pl.ds(n * step, step)
            if j:
                logits[span, :] += scores(n, slabs[j])
            else:
                logits[span, :] = scores(n, slabs[j])

    code_got[me] = code_own[...]
    others = pl.ds(0, group - 1)
    copy(code_got.at[others], code_got.at[others], cs.at[0], cr.at[0], b, over_x).wait_recv()
    for i in range(group):
        code_all[i * rows:(i + 1) * rows, :] = jnp.transpose(jnp.concatenate([code_got[i]] * (rows // 8), axis=0))

    early = lo
    pl.when(at_end)(lambda: w_slab(slabs[3], False, (0,)))
    for n in range(steps):
        logits[n * step:(n + 1) * step, :] += scores(n, slabs[3], y * (slab - early), early)
    pl.when(at_end)(lambda: w_slab(slabs[3], False, (1,)))

    sums = jnp.zeros((8, rows), f32)
    for n in range(steps):
        span = pl.ds(n * step, step)
        capped = softcap * jnp.tanh((logits[span, :] + scores(n, slabs[3], (1 - y) * early, slab - early)) * (1.0 / softcap))
        raised = jnp.exp(capped)
        logits[span, :] = capped
        expo[span, :] = raised
        total = jnp.broadcast_to(jnp.sum(raised, axis=1, keepdims=True), (step, 128))
        for k in range(2):
            turned = jnp.transpose(total[k * rows:(k + 1) * rows])
            sums = jnp.where(lines == 2 * n + k, turned[0:8], sums)
    stat_own[...] = sums

    def stat_copy(n):
        bb, vv, _ = peer(n)
        return copy(stat_own, stat_all.at[me], ss.at[0], sr.at[0], bb, vv)

    for n in range(len(peers)):
        stat_copy(n).start()

    ids = (lax.broadcasted_iota(jnp.int32, (step, half), 1) + (v * ny + y) * half).astype(f32)
    hit_total = jnp.zeros((step, 1), f32)
    for n in range(steps):
        span = pl.ds(n * step, step)
        capped = logits[span, :]
        hit = ids == code_all[span, 0:1]
        slope = 1.0 - (capped * (1.0 / softcap)) ** 2
        expo[span, :] = expo[span, :] * slope
        logits[span, :] = jnp.where(hit, slope, 0.0)
        hit_total = hit_total + jnp.sum(jnp.where(hit, capped, 0.0), axis=1, keepdims=True)
    hit_total = jnp.sum(hit_total, axis=0, keepdims=True)
    loss_one[...] = jnp.broadcast_to(hit_total, loss_one.shape)

    def hit_copy(n):
        bb, vv, _ = peer(n)
        return copy(loss_one, loss_all.at[me], ls.at[0], lr.at[0], bb, vv)

    for n in range(len(peers)):
        hit_copy(n).start()
    code_rows = jnp.zeros((8, rows), f32)
    for i in range(group):
        code_rows = jnp.where(lines == i, code_got[i], code_rows)
    weight = (code_rows >= 0).astype(f32)

    share_end(0, 0)
    share_end(1, 0)
    stat_all[me] = sums
    copy(stat_all.at[others], stat_all.at[others], ss.at[0], sr.at[0], b, over_x).wait_recv()
    partition = stat_all[0]
    for i in range(1, group):
        partition = partition + stat_all[i]
    scale = weight / partition

    lane_parts = [pl.ds(0, half - 128), pl.ds(half - 128, 128)]

    def delta_copy(p):
        here = lane_parts[p]
        return copy(delta.at[0, :, here], delta.at[1, :, here], es.at[0], (cr, er)[p].at[0], over_y, v)

    for n in range(steps):
        for k in range(2):
            i = 2 * n + k
            span = pl.ds(i * rows, rows)
            by_row = jnp.transpose(jnp.broadcast_to(scale[i:i + 1, :], (rows, rows)))
            factor = jnp.concatenate([by_row] * (half // rows), axis=1)
            delta[0, span, :] = (expo[span, :] * factor - logits[span, :]).astype(bf16)
    for p in range(2):
        delta_copy(p).start()

    chunks = range(half // 128)

    def chunk_of_delta(n):
        here = pl.ds(n * 128, 128)
        return copy(delta.at[0, :, here], d_end.at[:, here], zs.at[0], zr.at[n], near_end * ny + y, v)

    for n in chunks:
        pl.when(at_end)(lambda: chunk_of_delta(n).start())

    targets = [jnp.where(at_end, far, across), jnp.where(at_end, across, near), jnp.where(at_end, near_end, far), z]
    top = y * shift

    def over_tokens(left, right):
        return lax.dot_general(left, right, (((0,), (0,)), ((), ())), preferred_element_type=f32)

    def grad_share(zz, r):
        return over_tokens(h_all[:, window(zz)], delta[r])

    def sent(k, r):
        return grad_send.at[k, r, pl.ds(pl.multiple_of(top, 16), cols)]

    def r_copy(k, r):
        return copy(sent(k, r), r_in.at[z * 2 + r], rs.at[0], rr.at[z, r], targets[k] * ny + y, v)

    def relay_copy(n, p):
        src = grad_send.at[n, 1, pl.ds(pl.multiple_of(top, 16), cols), lane_parts[p]]
        return copy(src, far_in.at[n, :, lane_parts[p]], rs.at[0], fr.at[n, p], near_end * ny + y, v)

    def part_copy(k, p):
        src = grad_send.at[k, 1, pl.ds(pl.multiple_of(top, 16), cols), lane_parts[p]]
        return copy(src, r_in.at[z * 2 + 1, :, lane_parts[p]], rs.at[0], rr.at[z, 1], targets[k] * ny + y, v)

    def chunk_copy(k, n):
        here = pl.ds(n * 128, 128)
        src = grad_send.at[k, 0, pl.ds(pl.multiple_of(top, 16), cols), here]
        return copy(src, r_in.at[z * 2, :, here], rs.at[0], rr.at[z, 0], targets[k] * ny + y, v)

    def to_end():
        @pl.when(inside)
        def _():
            grad_send[1, 0] = grad_share(near, 0).astype(bf16)
            r_copy(1, 0).start()

    def keep():
        @pl.when(inside)
        def _():
            held[0] = grad_share(across, 0)
            held[1] = grad_share(far, 0)

    def chunk(n):
        first = n * 128

        @pl.when(inside)
        def _():
            if n == 0:
                for kx in range(2):
                    for ky in range(2):
                        end_copy(flip(y, ky) * nv + flip(x, kx) * 2 + 1 - core).wait_recv()
            chunk_of_delta(n).wait_recv()
            right = d_end[:, first:first + 128]
            for k, slot, j in ((0, 0, 1), (2, 1, 0)):
                share = held[slot, :, first:first + 128] + over_tokens(h_end[:, j * win:(j + 1) * win], right)
                grad_send[k, 0, :, first:first + 128] = share.astype(bf16)
                chunk_copy(k, n).start()
            grad_own[0, :, first:first + 128] += over_tokens(h_end[:, 2 * win:3 * win], right)

    def head_part(k, p):
        here = lane_parts[p]
        share = over_tokens(h_all[:, window(targets[k])], delta[1, :, here])
        if k:
            grad_send[k, 1, :, here] = share.astype(bf16)
            pl.when(at_end)(lambda: relay_copy(1, p).start())
            pl.when(inside)(lambda: part_copy(k, p).start())
        else:
            @pl.when(at_end)
            def _():
                grad_send[k, 1, :, here] = share.astype(bf16)
                relay_copy(0, p).start()

            @pl.when(inside)
            def _():
                held[0, :, here] = share

    def head_rest():
        share = grad_share(targets[2], 1)

        @pl.when(at_end)
        def _():
            grad_send[2, 1] = share.astype(bf16)
            r_copy(2, 1).start()

        @pl.when(inside)
        def _():
            held[1] = share

    cstep = chunk_of(cols, 64)

    def over_cols(body):
        def one(n, carry):
            body(pl.multiple_of(n * cstep, 16))
            return carry

        lax.fori_loop(0, cols // cstep, one, 0)

    def relay(k, n, p):
        lane = lane_parts[p]

        @pl.when(inside)
        def _():
            relay_copy(n, p).wait_recv()

            def add(m):
                here = pl.ds(pl.multiple_of(top + m, 16), cstep)
                there = pl.ds(m, cstep)
                grad_send[k, 1, here, lane] = (
                    held[k // 2, here, lane] + far_in[n, there, lane].astype(f32)).astype(bf16)

            over_cols(add)
            part_copy(k, p).start()

    groups = column_groups(width)
    blocks = [(1, 1), (1, 0), (0, 1), (0, 0)]
    unit = width // (width // 256)

    def span_of(g):
        first, n = groups[g]
        return pl.ds(first * unit, n * unit)

    y_first = (3,)

    def block(g, one, two, cc):
        kx, ky = (two, one) if g in y_first else (one, two)
        return flip(y, ky) * nv + flip(x, kx) * 2 + cc

    def core_copy(g, one, two):
        return copy(part.at[hrow(block(g, one, two, 1 - core)), span_of(g)], core_in.at[one, two, :, span_of(g)],
                    ds.at[0], wr.at[g, 0], b, over_core)

    def over_one(g):
        return (over_y, v) if g in y_first else (b, over_x)

    def over_two(g):
        return (b, over_x) if g in y_first else (over_y, v)

    def one_copy(g, two):
        return copy(x_out.at[two, :, span_of(g)], x_in.at[two, :, span_of(g)], xs.at[0], (hr if two else xr).at[g],
                    *over_one(g))

    def two_copy(g):
        return copy(y_out.at[:, span_of(g)], y_in.at[:, span_of(g)], ys.at[0], wr.at[g, 1], *over_two(g))

    def part_group(g):
        first, n = groups[g]

        def columns(j, carry):
            span = pl.ds(pl.multiple_of(j * unit, 128), unit)
            part[:, span] = lax.dot_general(
                delta[0], w_all[span, :], (((1,), (1,)), ((), ())), preferred_element_type=f32)
            return carry

        lax.fori_loop(first, first + n, columns, 0)
        for one, two in blocks:
            core_copy(g, one, two).start()

    hstep = 16

    def over_rows(body):
        def one(n, carry):
            body(pl.multiple_of(n * hstep, hstep))
            return carry

        lax.fori_loop(0, rows // hstep, one, 0)

    def core_sum(g):
        span = span_of(g)
        landed = core_in.at[:, :, :, span]
        copy(landed, landed, ds.at[0], wr.at[g, 0], b, over_core).wait_recv()
        for one, two in blocks:
            start = block(g, one, two, core) * rows

            def add(n):
                here = pl.ds(pl.multiple_of(start + n, hstep), hstep)
                both = part[here, span] + core_in[one, two, pl.ds(n, hstep), span]
                if one:
                    x_out[two, pl.ds(n, hstep), span] = both.astype(bf16)
                else:
                    part[here, span] = both

            over_rows(add)
            if one:
                one_copy(g, two).start()

    def one_sum(g):
        span = span_of(g)
        for two in (1, 0):
            one_copy(g, two).wait_recv()
            start = block(g, 0, two, core) * rows

            def add(n):
                here = pl.ds(pl.multiple_of(start + n, hstep), hstep)
                total = part[here, span] + x_in[two, pl.ds(n, hstep), span].astype(f32)
                if two:
                    y_out[pl.ds(n, hstep), span] = total.astype(bf16)
                else:
                    hid_out[pl.ds(n, hstep), span] = total

            over_rows(add)
            if two:
                two_copy(g).start()

    def two_sum(g):
        span = span_of(g)
        two_copy(g).wait_recv()

        def add(n):
            here = pl.ds(n, hstep)
            hid_out[here, span] += y_in[here, span].astype(f32)

        over_rows(add)

    count = len(groups)

    def plane_copy(k):
        return copy(loss_two, loss_zs.at[z], ms.at[0], mr.at[0], z_peer(k), v)

    def plane_loss():
        loss_all[me] = loss_one[...]
        copy(loss_all.at[others], loss_all.at[others], ls.at[0], lr.at[0], b, over_x).wait_recv()
        hits = loss_all[0]
        for i in range(1, group):
            hits = hits + loss_all[i]
        logs = jnp.sum(weight * jnp.log(partition), axis=1, keepdims=True)
        loss_two[...] = jnp.broadcast_to(jnp.sum(logs, axis=0, keepdims=True), (8, rows)) - hits
        for k in range(1, nz):
            plane_copy(k).start()

    part_group(0)
    part_group(1)
    to_end()
    plane_loss()
    core_sum(0)
    part_group(2)
    core_sum(1)
    share_end(0, 1)
    keep()
    part_group(3)
    core_sum(2)
    share_end(1, 1)
    grad_own[0] = grad_share(z, 0)
    part_group(4)
    core_sum(3)
    chunk(0)
    for g in range(5, count):
        part_group(g)
        core_sum(g - 1)
    core_sum(count - 1)
    for n in chunks[1:-1]:
        chunk(n)
    one_sum(0)

    delta_copy(0).wait_recv()
    head_part(0, 0)
    head_part(1, 0)
    chunk(len(chunks) - 1)
    delta_copy(1).wait_recv()
    head_part(0, 1)
    head_part(1, 1)
    one_sum(1)
    head_rest()
    grad_own[1] = grad_share(z, 1)
    one_sum(2)
    relay(2, 0, 0)

    copy(w_over, w_over, wys.at[0], wr.at[0, 0], over_y, v).wait_send()
    for n in range(1, nz):
        sent_rows = w_all.at[pl.ds(0, n * slab)]
        for way, slabs_sent in ((0, z + 1), (1, nz - z)):
            going = (slabs_sent == n) & (has_down if way else has_up)
            pl.when(going)(lambda: copy(sent_rows, sent_rows, ws.at[way], wr.at[0, 0], b, over_x).wait_send())
    seven = h_all.at[pl.ds(0, 7 * rows)]
    copy(seven, seven, hs.at[0], hr.at[0], b, over_x).wait_send()
    for got, sem in ((code_got, cs), (stat_all, ss), (loss_all, ls)):
        copy(got.at[others], got.at[others], sem.at[0], sem.at[0], b, over_x).wait_send()
    one_sum(3)
    two_sum(0)
    copy(delta.at[0], delta.at[1], es.at[0], cr.at[0], over_y, v).wait_send()
    relay(0, 1, 0)
    copy(core_in, core_in, ds.at[0], wr.at[0, 0], b, over_core).wait_send()
    one_sum(4)
    two_sum(1)
    relay(2, 0, 1)
    relay(0, 1, 1)
    for g in range(5, count):
        one_sum(g)
    two_sum(2)
    for g in range(4, count - 1):
        two_sum(g)

    def r_got(zz, r):
        whole = r_in.at[zz * 2 + r]
        copy(whole, whole, rs.at[0], rr.at[zz, r], z_peer(1), v).wait_recv()

    def lanes(r):
        return pl.ds(pl.multiple_of(flip(y, r) * half, 128), half)

    def head_sum(r):
        r_got(across, r)

        def add(n):
            here = pl.ds(n, cstep)
            total = grad_own[r, pl.ds(pl.multiple_of(top + n, 16), cstep), :]
            head_out[here, lanes(r)] = total + r_in[across * 2 + r, here, :].astype(f32)

        over_cols(add)

        def by_near():
            r_got(near, r)

            def last(n):
                here = pl.ds(n, cstep)
                head_out[here, lanes(r)] += r_in[near * 2 + r, here, :].astype(f32)

            over_cols(last)

        if r:
            by_near()
        else:
            pl.when(at_end)(by_near)

    head_sum(0)
    loss_zs[z] = loss_two[...]
    along = loss_zs.at[pl.ds(0, nz - 1)]
    copy(along, along, ms.at[0], mr.at[0], z_peer(1), v).wait_recv()
    losses = loss_zs[0]
    for i in range(1, nz):
        losses = losses + loss_zs[i]
    loss_out[...] = losses * (1.0 / (tokens * nz))
    copy(along, along, ms.at[0], mr.at[0], z_peer(1), v).wait_send()
    two_sum(3)
    two_sum(count - 1)
    head_sum(1)

    rows_out = h_end.at[pl.ds(0, tokens // 2)]
    for part_sent, sem in ((x_out, xs), (y_out, ys), (rows_out, us)):
        copy(part_sent, part_sent, sem.at[0], sem.at[0], b, over_x).wait_send()

    @pl.when(at_end)
    def _():
        for part_sent, sem in ((d_end, zs), (r_in.at[pl.ds(0, 3)], rs)):
            copy(part_sent, part_sent, sem.at[0], sem.at[0], b, over_x).wait_send()

    @pl.when(inside)
    def _():
        six = r_in.at[pl.ds(0, 6)]
        copy(six, six, rs.at[0], rs.at[0], b, over_x).wait_send()


def finish_kernel(head_in, hid_in, loss_in, head_out, hid_out, loss_out, loss_one, sem):
    moves = [
        pltpu.make_async_copy(hid_in, hid_out, sem.at[0]),
        pltpu.make_async_copy(head_in, head_out, sem.at[1]),
        pltpu.make_async_copy(loss_one, loss_out, sem.at[2]),
    ]
    for one in moves[:2]:
        one.start()
    loss_one[...] = loss_in[0:1, 0:1]
    moves[2].start()
    for one in moves:
        one.wait()


def plane_local(hidden, head_weight, targets, valid_mask):
    nz, ny, nv = 4, 2, 4
    rows, width = hidden.shape
    entries, cols = head_weight.shape
    half = entries // ny
    group = ny * nv
    tokens = rows * group
    shift = cols % 128
    win = -(-(cols + shift) // 128) * 128
    vm = pltpu.VMEM
    dma = pltpu.SemaphoreType.DMA
    count = len(column_groups(width))
    line = vm((8, rows), f32)
    buffers = [
        vm((tokens, width), bf16), vm((width, half), bf16), vm((cols, half), bf16),
        vm((1, rows), jnp.int32), vm((1, rows), jnp.int32), line, vm((group, 8, rows), f32), vm((tokens, 128), f32),
        vm((tokens, half), f32), vm((tokens, half), f32), vm((2, tokens, half), bf16),
        line, vm((group, 8, rows), f32), line, line, vm((group, 8, rows), f32), vm((nz, 8, rows), f32),
        vm((2, win, half), f32), vm((2, win, half), f32), vm((3, 2, win, half), bf16),
        vm((2, cols, half), bf16), vm((nz * 2, cols, half), bf16), vm((tokens, 3 * win), bf16), vm((tokens, half), bf16),
        vm((tokens, width), f32), vm((2, 2, rows, width), f32),
        vm((2, rows, width), bf16), vm((2, rows, width), bf16), vm((rows, width), bf16), vm((rows, width), bf16),
    ]
    sems = [
        dma((5,)), dma((1,)), dma((group,)), dma((2,)), dma((8, 2)), dma((1,)),
        dma((1,)), dma((1,)), dma((1,)), dma((1,)), dma((1,)), dma((1,)), dma((1,)), dma((1,)),
        dma((1,)), dma((1,)), dma((1,)), dma((nz, 2)), dma((2, 2)), dma((1,)), dma((half // 128,)), dma((1,)), dma((group,)),
        dma((1,)), dma((1,)), dma((count,)), dma((1,)),
    ]
    whole = pl.BlockSpec(memory_space=vm)
    head_t, hidden_grad, loss = pl.pallas_call(
        plane_kernel,
        out_shape=(
            vm((cols, entries), f32),
            vm((rows, width), f32),
            vm((8, rows), f32),
        ),
        in_specs=[pl.BlockSpec(memory_space=pl.ANY)] * 4,
        out_specs=(whole,) * 3,
        scratch_shapes=buffers + sems,
        compiler_params=pltpu.CompilerParams(
            collective_id=1, has_side_effects=True, vmem_limit_bytes=58 * 1024 * 1024),
    )(hidden, jnp.transpose(head_weight), targets[None, :], valid_mask[None, :])
    anywhere = pl.BlockSpec(memory_space=pl.ANY)
    head_t, hidden_grad, loss = pl.pallas_call(
        finish_kernel,
        out_shape=(
            jax.ShapeDtypeStruct((cols, entries), f32),
            jax.ShapeDtypeStruct((rows, width), f32),
            jax.ShapeDtypeStruct((1, 1), f32),
        ),
        in_specs=[whole] * 3,
        out_specs=(anywhere,) * 3,
        scratch_shapes=[vm((1, 1), f32), dma((3,))],
        compiler_params=pltpu.CompilerParams(vmem_limit_bytes=1024 * 1024),
    )(head_t, hidden_grad, loss)
    return jnp.transpose(head_t), hidden_grad, loss[0, 0]


def in_planes(nb, nv, hidden, head_weight, targets, valid_mask):
    rows, width = hidden.shape
    entries, cols = head_weight.shape
    fits = nb == 8 and nv == 4 and rows == 128 and width % 256 == 0 and width >= 3072
    fits = fits and len(column_groups(width)) <= 8
    return fits and entries % 256 == 0 and entries >= 512 and cols % 32 == 0 and (2 * cols) % 128 == 0


def device(nb, nv, *arrays):
    if in_planes(nb, nv, *arrays):
        return plane_local(*arrays)
    return local(nb, nv, *arrays)


def solution(mesh):
    placed = (
        P(("batch", "vocab"), None),
        P("vocab", "batch"),
        P(("batch", "vocab")),
        P(("batch", "vocab")),
    )
    return jax.shard_map(
        functools.partial(device, mesh.shape["batch"], mesh.shape["vocab"]),
        mesh=mesh,
        in_specs=placed,
        out_specs=(P("vocab", "batch"), P(("batch", "vocab"), None), P()),
        check_vma=False,
    )
```

```python
import functools

import jax
import jax.numpy as jnp
from jax import lax
from jax.experimental import pallas as pl
from jax.experimental.pallas import tpu as pltpu
from jax.sharding import PartitionSpec as P

softcap = 30.0
MESH = pl.DeviceIdType.MESH
f32, bf16 = jnp.float32, jnp.bfloat16


def chunk_of(length, most):
    return max(s for s in range(16, most + 1, 16) if length % s == 0)


def kernel(sizes, h_in, w_in, code_in, head_out, hid_out, loss_out, h_all, w_all, code_got, code_all,
           logits, delta, stat_own, stat_all, loss_own, loss_all, grad, grad_send, r_in,
           part, core_in, x_out, x_in, y_out, y_in, far_own, far_in, *sems):
    nz, ny, nx, nv = sizes
    (own_sem, hs, hf, hd, hr, ws_up, ws_dn, ws_y, wr, cs, cr, ss, sr, ls, lr,
     rs, rr, ds, dr, xs, xr, ys, yr, fs, fr) = sems
    nb = nz * ny
    rows, width = h_in.shape
    cols, half = w_in.shape[1:]
    group = ny * nv
    tokens = rows * group
    entries = ny * half
    b, v = lax.axis_index("batch"), lax.axis_index("vocab")
    z, y = lax.div(b, ny), lax.rem(b, ny)
    x, core = lax.div(v, 2), lax.rem(v, 2)
    other = x * 2 + 1 - core
    me = y * nv + v

    def at(bb, vv):
        return {"batch": bb, "vocab": vv}

    def copy(src, dst, send, recv, bb, vv):
        return pltpu.make_async_remote_copy(
            src_ref=src, dst_ref=dst, send_sem=send, recv_sem=recv, device_id=at(bb, vv), device_id_type=MESH)

    def hrow(i):
        return pl.ds(pl.multiple_of(i * rows, 16), rows)

    def wrow(i):
        return pl.ds(pl.multiple_of(i * cols, 16), cols)

    def turn_y(k):
        return lax.rem(y + k, ny)

    def turn_x(k):
        return lax.rem(x + k, nx)

    peers = [(k, j) for k in range(ny) for j in range(nv) if k or j]

    def peer(n):
        k, j = peers[n]
        return z * ny + turn_y(k), lax.rem(v + j, nv), turn_y(k) * nv + lax.rem(v + j, nv)

    barrier = pltpu.get_barrier_semaphore()
    for k in range(1, nb):
        pl.semaphore_signal(barrier, inc=1, device_id=at(lax.rem(b + k, nb), v), device_id_type=MESH)
    met = [n for n in range(len(peers)) if peers[n][1]]
    for n in met:
        bb, vv, _ = peer(n)
        pl.semaphore_signal(barrier, inc=1, device_id=at(bb, vv), device_id_type=MESH)
    pl.semaphore_wait(barrier, nb - 1 + len(met))

    def w_z(zz, yy, up, own=False):
        i = zz * ny + yy
        dst = w_all.at[wrow(i)]
        sem = (ws_up if up else ws_dn).at[i]
        return copy(w_in.at[y] if own else dst, dst, sem, wr.at[i], b + ny if up else b - ny, v)

    def w_y(k):
        return copy(w_in.at[turn_y(k)], w_all.at[wrow(b)], ws_y.at[k - 1], wr.at[b], z * ny + turn_y(k), v)

    def w_got(zz, yy):
        w_z(zz, yy, True).wait_recv()

    has_up, has_down = z + 1 < nz, z >= 1

    def h_send(n_src, sem, bb, vv, own=False):
        dst = h_all.at[hrow(n_src)]
        return copy(h_in if own else dst, dst, sem, hr.at[n_src], bb, vv)

    def h_x(k):
        return h_send(me, hs.at[k - 1], b, turn_x(k) * 2 + core, True)

    def h_y(k):
        return h_send(me, hs.at[nx + k - 1], z * ny + turn_y(k), v, True)

    def h_xy(kx, ky):
        return h_send(y * nv + turn_x(kx) * 2 + core, hf.at[kx, ky], z * ny + turn_y(ky), v)

    def h_yx(kx, ky):
        return h_send(turn_y(ky) * nv + v, hf.at[kx, ky], b, turn_x(kx) * 2 + core)

    def h_core(kx, ky):
        i = turn_y(ky) * nv + turn_x(kx) * 2 + core
        return h_send(i, hd.at[kx, ky], b, other, kx == 0 and ky == 0)

    def h_got(kx, ky, cc):
        i = turn_y(ky) * nv + turn_x(kx) * 2 + cc
        h_send(i, hd.at[kx, ky], b, other).wait_recv()

    def code_copy(n):
        bb, vv, _ = peer(n)
        return copy(code_in, code_got.at[me], cs.at[n], cr.at[me], bb, vv)

    for k in range(1, ny):
        w_y(k).start()
    pl.when(has_up)(lambda: w_z(z, y, True, True).start())
    pl.when(has_down)(lambda: w_z(z, y, False, True).start())
    for k in range(1, nx):
        h_x(k).start()
    for k in range(1, ny):
        h_y(k).start()
    for n in range(len(peers)):
        code_copy(n).start()
    h_core(0, 0).start()
    local = [
        pltpu.make_async_copy(w_in.at[y], w_all.at[wrow(b)], own_sem.at[0]),
        pltpu.make_async_copy(h_in, h_all.at[hrow(me)], own_sem.at[1]),
    ]
    for one in local:
        one.start()

    for k in range(1, ny):
        w_got(z, turn_y(k))
        pl.when(has_up)(lambda: w_z(z, turn_y(k), True).start())
        pl.when(has_down)(lambda: w_z(z, turn_y(k), False).start())

    def h_pass():
        for kx in range(1, nx):
            h_got(kx, 0, core)
            for ky in range(1, ny):
                pl.when(core == 0)(lambda: h_xy(kx, ky).start())
            h_core(kx, 0).start()
        for ky in range(1, ny):
            h_got(0, ky, core)
            for kx in range(1, nx):
                pl.when(core == 1)(lambda: h_yx(kx, ky).start())
            h_core(0, ky).start()

    def h_rest():
        for kx in range(1, nx):
            for ky in range(1, ny):
                h_got(kx, ky, core)
                h_core(kx, ky).start()

    for k in range(1, nz):
        for j in range(ny):
            yy = turn_y(j)

            @pl.when(z - k >= 0)
            def _():
                w_got(z - k, yy)
                pl.when(has_up)(lambda: w_z(z - k, yy, True).start())

            @pl.when(z + k < nz)
            def _():
                w_got(z + k, yy)
                pl.when(has_down)(lambda: w_z(z + k, yy, False).start())
        if k == 1:
            h_pass()
        if k == min(2, nz - 1):
            h_rest()

    for one in local:
        one.wait()
    for kx in range(nx):
        for ky in range(ny):
            h_got(kx, ky, 1 - core)
    code_got[me] = code_in[...]
    for n in range(len(peers)):
        bb, vv, i = peer(n)
        copy(code_in, code_got.at[i], cs.at[n], cr.at[i], bb, vv).wait_recv()
    for i in range(group):
        code_all[i * rows:(i + 1) * rows, :] = jnp.transpose(jnp.concatenate([code_got[i]] * 16, axis=0))

    step = chunk_of(tokens, 256)
    lanes = lax.broadcasted_iota(jnp.int32, (step, 128), 1)
    first = v * entries + y * half

    def span_of(n):
        return pl.ds(pl.multiple_of(n * step, step), step)

    def hits(n):
        ids = lax.broadcasted_iota(jnp.int32, (step, half), 1) + first
        return ids == code_all[span_of(n), 0:1].astype(jnp.int32)

    for n in range(tokens // step):
        span = pl.ds(n * step, step)
        scores = jnp.dot(h_all[span, :], w_all[...], preferred_element_type=f32)
        capped = softcap * jnp.tanh(scores * (1.0 / softcap))
        logits[span, :] = capped
        total = jnp.sum(jnp.exp(capped), axis=1, keepdims=True)
        hit_sum = jnp.sum(jnp.where(hits(n), capped, 0.0), axis=1, keepdims=True)
        turned = jnp.transpose(jnp.where(lax.rem(lanes, 8) < 4, total, hit_sum))
        stat_own[:, n * step:(n + 1) * step] = turned[0:8]

    def stat_copy(n):
        bb, vv, _ = peer(n)
        return copy(stat_own, stat_all.at[me], ss.at[n], sr.at[me], bb, vv)

    for n in range(len(peers)):
        stat_copy(n).start()
    for n in range(len(peers)):
        bb, vv, i = peer(n)
        copy(stat_own, stat_all.at[i], ss.at[n], sr.at[i], bb, vv).wait_recv()
    stats = stat_own[...]
    for n in range(len(peers)):
        stats = stats + stat_all[peer(n)[2]]

    loss = jnp.zeros((1, 1), f32)
    for n in range(tokens // step):
        span = pl.ds(n * step, step)
        weight = (code_all[span, 0:1] >= 0).astype(f32)
        back = jnp.transpose(jnp.concatenate([stats[:, n * step:(n + 1) * step]] * 16, axis=0))
        partition, target_logit = back[:, 0:1], back[:, 4:5]
        loss = loss + jnp.sum(weight * (jnp.log(partition) - target_logit), axis=0, keepdims=True)
        capped = logits[span, :]
        slope = 1.0 - (capped * (1.0 / softcap)) ** 2
        delta[span, :] = ((jnp.exp(capped) * (weight / partition) - jnp.where(hits(n), weight, 0.0)) * slope
                          ).astype(bf16)
    loss_own[...] = jnp.broadcast_to(loss, loss_own.shape)

    def loss_copy(k):
        return copy(loss_own, loss_all.at[b], ls.at[k - 1], lr.at[b], lax.rem(b + k, nb), v)

    def r_copy(zz, yy):
        i = zz * ny + yy
        return copy(grad_send.at[wrow(i)], r_in.at[z, y], rs.at[i], rr.at[b], i, v)

    def grad_share(span):
        return lax.dot_general(h_all[:, span], delta[...], (((0,), (0,)), ((), ())), preferred_element_type=f32)

    slab = ny * cols
    relay = nz == 4 and slab % 128 == 0
    turn = jnp.where(z * 2 >= nz, 1, nz - 1)
    order = [lax.rem(z + turn * k, nz) for k in range(1, nz)] + [z]
    at_end = (z == 0) | (z == nz - 1)
    far = jnp.where(z * 2 >= nz, 0, nz - 1)
    near = jnp.where(z * 2 >= nz, z - 1, z + 1)

    def far_copy(yy):
        return copy(grad_send.at[wrow(far * ny + yy)], far_in.at[yy], fs.at[yy], fr.at[yy], near * ny + y, v)

    def direct(zz):
        return jnp.logical_not(at_end & (zz == far))
    if slab % 128 == 0:
        mine = y * cols
        for n in range(nz):
            zz = order[n]
            span = pl.ds(pl.multiple_of(zz * slab, 128), slab)
            share = grad_share(span)
            held = relay and n == 1
            if n == nz - 1:
                grad[...] = share
            if held:
                @pl.when(jnp.logical_not(at_end))
                def _():
                    far_own[...] = share

                @pl.when(at_end)
                def _():
                    grad_send[span, :] = share.astype(bf16)
                    for k in range(ny):
                        r_copy(zz, turn_y(k)).start()
            else:
                grad_send[span, :] = share.astype(bf16)
                for k in range(ny):
                    yy = turn_y(k)
                    if relay and n == 0:
                        pl.when(at_end)(lambda: far_copy(yy).start())
                        pl.when(jnp.logical_not(at_end))(lambda: r_copy(zz, yy).start())
                    elif n < nz - 1 or k:
                        r_copy(zz, yy).start()
    else:
        mine = b * cols
        wide = chunk_of(width, 256)

        def grad_step(j, carry):
            span = pl.ds(pl.multiple_of(j * wide, wide), wide)
            share = grad_share(span)
            grad[span, :] = share
            grad_send[span, :] = share.astype(bf16)
            return carry

        lax.fori_loop(0, width // wide, grad_step, 0)
        for n in range(nz):
            for k in range(ny):
                if n < nz - 1 or k:
                    r_copy(order[n], turn_y(k)).start()
    for k in range(1, nb):
        loss_copy(k).start()

    wide = chunk_of(width, 256)

    def part_step(j, carry):
        span = pl.ds(pl.multiple_of(j * wide, wide), wide)
        part[:, span] = lax.dot_general(
            delta[...], w_all[span, :], (((1,), (1,)), ((), ())), preferred_element_type=f32)
        return carry

    lax.fori_loop(0, width // wide, part_step, 0)

    def core_copy(kx, ky):
        i = turn_y(ky) * nv + turn_x(kx) * 2 + 1 - core
        return copy(part.at[hrow(i)], core_in.at[kx, ky], ds.at[kx, ky], dr.at[kx, ky], b, other)

    def x_copy(kx, ky):
        return copy(x_out.at[kx - 1, ky], x_in.at[kx - 1, ky], xs.at[kx, ky], xr.at[kx, ky],
                    b, turn_x(kx) * 2 + core)

    def y_copy(ky):
        return copy(y_out.at[ky - 1], y_in.at[ky - 1], ys.at[ky], yr.at[ky], z * ny + turn_y(ky), v)

    ways = [(kx % nx, ky % ny) for kx in range(1, nx + 1) for ky in range(1, ny + 1)]
    for kx, ky in ways:
        core_copy(kx, ky).start()
    hstep = 16

    def over_rows(start, body):
        def one(r, carry):
            body(pl.ds(pl.multiple_of(r * hstep, hstep), hstep),
                 pl.ds(pl.multiple_of(start + r * hstep, hstep), hstep))
            return carry

        lax.fori_loop(0, rows // hstep, one, 0)

    def start_of(kx, ky):
        return (turn_y(ky) * nv + turn_x(kx) * 2 + core) * rows

    for kx, ky in ways:
        core_copy(kx, ky).wait_recv()

        def core_sum(span, here):
            both = part[here, :] + core_in[kx, ky, span, :]
            if kx:
                x_out[kx - 1, ky, span, :] = both.astype(bf16)
            else:
                part[here, :] = both

        over_rows(start_of(kx, ky), core_sum)
        if kx:
            x_copy(kx, ky).start()

    cstep = chunk_of(cols, 64)

    def over_cols(body):
        def one(r, carry):
            body(pl.multiple_of(r * cstep, 16))
            return carry

        lax.fori_loop(0, cols // cstep, one, 0)

    if relay:
        @pl.when(jnp.logical_not(at_end))
        def _():
            for k in range(ny):
                yy = turn_y(k)
                far_copy(yy).wait_recv()

                def far_sum(r):
                    here = pl.ds(pl.multiple_of(yy * cols + r, 16), cstep)
                    there = pl.ds(pl.multiple_of((far * ny + yy) * cols + r, 16), cstep)
                    grad_send[there, :] = (far_own[here, :] + far_in[yy, pl.ds(r, cstep), :].astype(f32)).astype(bf16)

                over_cols(far_sum)
                r_copy(far, yy).start()

    for ky in [k % ny for k in range(1, ny + 1)]:
        for kx in range(1, nx):
            x_copy(kx, ky).wait_recv()

        def x_sum(span, here):
            total = part[here, :]
            for kx in range(1, nx):
                total = total + x_in[kx - 1, ky, span, :].astype(f32)
            if ky:
                y_out[ky - 1, span, :] = total.astype(bf16)
            else:
                hid_out[span, :] = total

        over_rows(start_of(0, ky), x_sum)
        if ky:
            y_copy(ky).start()

    def r_got(zz, yy):
        i = zz * ny + yy
        copy(grad_send.at[wrow(i)], r_in.at[zz, yy], rs.at[i], rr.at[i], i, v).wait_recv()

    for k in range(1, ny):
        r_got(z, turn_y(k))

    def first_sum(r):
        head_out[y, pl.ds(r, cstep), :] = grad[pl.ds(pl.multiple_of(mine + r, 16), cstep), :]
        for k in range(1, ny):
            head_out[turn_y(k), pl.ds(r, cstep), :] = r_in[z, turn_y(k), pl.ds(r, cstep), :].astype(f32)

    over_cols(first_sum)
    hops = [jnp.where(z * 2 >= nz, lax.rem(z + nz - n, nz), lax.rem(z + n, nz)) for n in range(1, nz)]
    for n in range(1, nz):
        zz = hops[n - 1]
        if n == nz - 1:
            for ky in range(1, ny):
                y_copy(ky).wait_recv()

                def y_sum(span, here):
                    hid_out[span, :] += y_in[ky - 1, span, :].astype(f32)

                over_rows(0, y_sum)

        def more_sum(r):
            for k in range(ny):
                head_out[turn_y(k), pl.ds(r, cstep), :] += r_in[zz, turn_y(k), pl.ds(r, cstep), :].astype(f32)

        def arrived():
            for k in range(ny):
                r_got(zz, turn_y(k))
            over_cols(more_sum)

        if relay:
            pl.when(direct(zz))(arrived)
        else:
            arrived()

    losses = loss_own[...]
    for k in range(1, nb):
        i = lax.rem(b + k, nb)
        copy(loss_own, loss_all.at[i], ls.at[k - 1], lr.at[i], i, v).wait_recv()
        losses = losses + loss_all[i]
    loss_out[...] = losses * (1.0 / (tokens * nb))

    for j in range(ny):
        yy = turn_y(j)
        pl.when(has_up)(lambda: w_z(z, yy, True, j == 0).wait_send())
        pl.when(has_down)(lambda: w_z(z, yy, False, j == 0).wait_send())
        for k in range(1, nz):
            @pl.when(z - k >= 0)
            def _():
                pl.when(has_up)(lambda: w_z(z - k, yy, True).wait_send())

            @pl.when(z + k < nz)
            def _():
                pl.when(has_down)(lambda: w_z(z + k, yy, False).wait_send())
    for k in range(1, ny):
        w_y(k).wait_send()
        h_y(k).wait_send()
        y_copy(k).wait_send()
    for k in range(1, nx):
        h_x(k).wait_send()
        for ky in range(1, ny):
            pl.when(core == 0)(lambda: h_xy(k, ky).wait_send())
            pl.when(core == 1)(lambda: h_yx(k, ky).wait_send())
    for kx, ky in ways:
        h_core(kx, ky).wait_send()
        core_copy(kx, ky).wait_send()
        if kx:
            x_copy(kx, ky).wait_send()
    for n in range(len(peers)):
        code_copy(n).wait_send()
        stat_copy(n).wait_send()
    for k in range(1, nb):
        loss_copy(k).wait_send()
    for n in range(nz):
        for k in range(ny):
            yy = turn_y(k)
            if relay and n == 0:
                pl.when(at_end)(lambda: far_copy(yy).wait_send())
                pl.when(jnp.logical_not(at_end))(lambda: r_copy(order[n], yy).wait_send())
            elif n < nz - 1 or k:
                r_copy(order[n], yy).wait_send()


def local(nb, nv, hidden, head_weight, targets, valid_mask):
    nx = nv // 2
    ny = nx if nx <= 2 and nb % nx == 0 else 1
    nz = nb // ny
    rows, width = hidden.shape
    entries, cols = head_weight.shape
    half = entries // ny
    group = ny * nv
    tokens = rows * group
    code = jnp.broadcast_to(jnp.where(valid_mask != 0, targets, -1).astype(f32)[None, :], (8, rows))
    weight = jnp.transpose(head_weight.reshape(ny, half, cols), (0, 2, 1))
    vm = pltpu.VMEM
    dma = pltpu.SemaphoreType.DMA
    slab = ny * cols
    ly, lx = max(ny - 1, 1), max(nx - 1, 1)
    buffers = [
        vm((tokens, width), bf16), vm((width, half), bf16), vm((group, 8, rows), f32), vm((tokens, 128), f32),
        vm((tokens, half), f32), vm((tokens, half), bf16),
        vm((8, tokens), f32), vm((group, 8, tokens), f32), vm((8, 128), f32), vm((nb, 8, 128), f32),
        vm((slab if slab % 128 == 0 else width, half), f32), vm((width, half), bf16), vm((nz, ny, cols, half), bf16),
        vm((tokens, width), f32), vm((nx, ny, rows, width), f32),
        vm((lx, ny, rows, width), bf16), vm((lx, ny, rows, width), bf16),
        vm((ly, rows, width), bf16), vm((ly, rows, width), bf16),
        vm((slab if nz == 4 else 16, half), f32), vm((ny, cols if nz == 4 else 16, half), bf16),
    ]
    sems = [
        dma((2,)), dma((nx + ny,)), dma((nx, ny)), dma((nx, ny)), dma((group,)), dma((nb,)), dma((nb,)),
        dma((ly,)), dma((nb,)), dma((group,)), dma((group,)), dma((group,)), dma((group,)), dma((nb,)), dma((nb,)),
        dma((nb,)), dma((nb,)), dma((nx, ny)), dma((nx, ny)), dma((nx, ny)), dma((nx, ny)), dma((ny,)), dma((ny,)),
        dma((ny,)), dma((ny,)),
    ]
    whole = pl.BlockSpec(memory_space=vm)
    head_t, hidden_grad, loss = pl.pallas_call(
        functools.partial(kernel, (nz, ny, nx, nv)),
        out_shape=(
            jax.ShapeDtypeStruct((ny, cols, half), f32),
            jax.ShapeDtypeStruct((rows, width), f32),
            jax.ShapeDtypeStruct((8, 128), f32),
        ),
        in_specs=[whole] * 3,
        out_specs=(whole,) * 3,
        scratch_shapes=buffers + sems,
        compiler_params=pltpu.CompilerParams(
            collective_id=0, has_side_effects=True, vmem_limit_bytes=67043328),
    )(hidden, weight, code)
    return jnp.transpose(head_t, (0, 2, 1)).reshape(entries, cols), hidden_grad, loss[0, 0]


def column_groups(width):
    left = width // 256 - 11
    sizes = [1, 2, 3, 2]
    while left > 0:
        sizes.append(min(3, left))
        left -= sizes[-1]
    sizes += [2, 1]
    starts = [sum(sizes[:n]) for n in range(len(sizes))]
    return [(s, n) for s, n in zip(starts, sizes)]


def plane_kernel(h_in, w_in, ids_in, mask_in, head_out, hid_out, loss_out, h_all, w_all, w_over, ids_own, mask_own,
                 code_own, code_got, code_all,
                 logits, expo, delta, stat_own, stat_all, loss_one, loss_two, loss_all, loss_zs,
                 grad_own, held, grad_send, far_in, r_in, h_end, d_end, part, core_in, x_out, x_in, y_out, y_in, *sems):
    (own_sem, hs, hr, ws, wr, wys, cs, cr, ss, sr, ls, lr, ms, mr,
     es, er, rs, rr, fr, zs, zr, us, ur, ds, xs, xr, ys) = sems
    nz, ny, nv = 4, 2, 4
    nb = nz * ny
    rows, width = h_in.shape
    cols, half = w_in.shape[0], w_in.shape[1] // ny
    piece = cols // 2
    group = ny * nv
    tokens = rows * group
    slab = ny * cols
    shift, lo = cols % 128, cols - cols % 128
    win = -(-(cols + shift) // 128) * 128
    b, v = lax.axis_index("batch"), lax.axis_index("vocab")
    z, y = lax.div(b, ny), lax.rem(b, ny)
    x, core = lax.div(v, 2), lax.rem(v, 2)
    me = y * nv + v
    low = z * 2 < nz
    at_end = (z == 0) | (z == nz - 1)
    inside = jnp.logical_not(at_end)

    def flip(a, k):
        return 1 - a if k else a

    def copy(src, dst, send, recv, bb, vv):
        return pltpu.make_async_remote_copy(
            src_ref=src, dst_ref=dst, send_sem=send, recv_sem=recv,
            device_id={"batch": bb, "vocab": vv}, device_id_type=MESH)

    def hrow(i):
        return pl.ds(pl.multiple_of(i * rows, 16), rows)

    far = jnp.where(low, nz - 1, 0)
    across = jnp.where(low, 2, 1)
    near_end = jnp.where(low, 1, 2)
    over_x, over_y, over_core = (1 - x) * 2 + core, z * ny + 1 - y, x * 2 + 1 - core
    peers = [(ky, kx, kc) for ky in range(2) for kx in range(2) for kc in range(2) if ky or kx or kc]

    def peer(n):
        ky, kx, kc = peers[n]
        yy, vv = flip(y, ky), flip(x, kx) * 2 + flip(core, kc)
        return z * ny + yy, vv, yy * nv + vv

    def z_peer(k):
        return lax.rem(z + k, nz) * ny + y

    has_up, has_down = z + 1 < nz, z >= 1
    barrier = pltpu.get_barrier_semaphore()

    def greet(bb, vv):
        pl.semaphore_signal(barrier, inc=1, device_id={"batch": bb, "vocab": vv}, device_id_type=MESH)

    pl.when(has_up)(lambda: greet(b + ny, v))
    pl.when(has_down)(lambda: greet(b - ny, v))
    greet(over_y, v)
    greet(b, over_x)
    greet(b, over_core)
    first = pl.ds(pl.multiple_of(y * half, 128), half)
    second = pl.ds(pl.multiple_of((1 - y) * half, 128), half)
    local = [
        pltpu.make_async_copy(w_in.at[:, second], w_over, own_sem.at[0]),
        pltpu.make_async_copy(w_in.at[:, first], w_all.at[pl.ds(pl.multiple_of(b * cols, 16), cols)], own_sem.at[1]),
        pltpu.make_async_copy(ids_in, ids_own, own_sem.at[2]),
        pltpu.make_async_copy(mask_in, mask_own, own_sem.at[3]),
        pltpu.make_async_copy(h_in, h_all.at[hrow(me)], own_sem.at[4]),
    ]
    for one in local:
        one.start()
    for one in local[:2]:
        one.wait()
    pl.semaphore_wait(barrier, jnp.where(inside, 5, 4))

    def w_ref(i, h):
        return w_all.at[pl.ds(pl.multiple_of(i * cols + h * piece, 16), piece)]

    def w_z(i, h, up):
        return copy(w_ref(i, h), w_ref(i, h), ws.at[0 if up else 1],
                    wr.at[i, h], b + ny if up else b - ny, v)

    def w_pass(i, h, up):
        return copy(w_ref(i, h), w_ref(i, h), ws.at[jnp.where(up, 0, 1)], wr.at[i, h], jnp.where(up, b + ny, b - ny), v)

    def w_y(h):
        return copy(w_over.at[pl.ds(h * piece, piece)], w_ref(b, h), wys.at[0], wr.at[b, h], over_y, v)

    def w_got(i, h):
        copy(w_ref(i, h), w_ref(i, h), wys.at[0], wr.at[i, h], over_y, v).wait_recv()

    near = z + 1 - 2 * lax.rem(z, 2)
    slabs = [z, near, jnp.where(low, 2, 1), jnp.where(low, 3, 0)]

    def h_send(i, bb, vv):
        return copy(h_all.at[hrow(i)], h_all.at[hrow(i)], hs.at[0], hr.at[i], bb, vv)

    def h_x():
        return h_send(me, b, over_x)

    def h_y():
        return h_send(me, over_y, v)

    def h_xy():
        return h_send(y * nv + over_x, over_y, v)

    def h_yx():
        return h_send((1 - y) * nv + v, b, over_x)

    def h_core(kx, ky):
        i = flip(y, ky) * nv + flip(x, kx) * 2 + core
        return h_send(i, b, over_core)

    def h_got(kx, ky, cc):
        i = flip(y, ky) * nv + flip(x, kx) * 2 + cc
        h_send(i, b, over_core).wait_recv()

    def window(zz):
        return pl.ds(pl.multiple_of(zz * slab + y * lo, 128), win)

    def mine_of(kx, ky):
        return flip(y, ky) * nv + flip(x, kx) * 2 + core

    def h_out(kx, ky, j):
        i = mine_of(kx, ky)
        return copy(h_all.at[hrow(i), window((far, across, near_end)[j])], h_end.at[hrow(i), pl.ds(j * win, win)],
                    us.at[0], ur.at[i], near_end * ny + y, v)

    def send_out(kx, ky):
        @pl.when(at_end)
        def _():
            for j in range(3):
                h_out(kx, ky, j).start()

    def end_copy(i):
        return copy(h_end.at[hrow(i)], h_end.at[hrow(i)], us.at[0], ur.at[i], b, over_core)

    def share_end(kx, ky):
        @pl.when(inside)
        def _():
            end_copy(mine_of(kx, ky)).wait_recv()
            end_copy(mine_of(kx, ky)).start()

    def code_copy(n):
        bb, vv, _ = peer(n)
        return copy(code_own, code_got.at[me], cs.at[0], cr.at[0], bb, vv)

    for h in range(2):
        w_y(h).start()
    for h in range(2):
        pl.when(has_up)(lambda: w_z(b, h, True).start())
        pl.when(has_down)(lambda: w_z(b, h, False).start())
    for one in local[2:]:
        one.wait()
    code = jnp.where(mask_own[...] != 0, ids_own[...], -1).astype(f32)
    code_own[...] = jnp.broadcast_to(code, code_own.shape)
    h_x().start()
    h_y().start()
    h_core(0, 0).start()

    def send_codes(count):
        for n in range(len(peers)):
            if sum(peers[n]) == count:
                code_copy(n).start()

    send_codes(1)
    for h in range(2):
        i = z * ny + 1 - y
        w_got(i, h)
        pl.when(has_up)(lambda: w_z(i, h, True).start())
        pl.when(has_down)(lambda: w_z(i, h, False).start())
    send_out(0, 0)

    def w_slab(zz, onward, which=(0, 1)):
        for k in which:
            for h in range(2):
                i = zz * ny + flip(y, k)
                w_got(i, h)
                if onward:
                    w_pass(i, h, zz < z).start()

    @pl.when(at_end)
    def _():
        w_slab(slabs[1], False)

    @pl.when(inside)
    def _():
        w_slab(slabs[1], True)
        w_slab(slabs[2], True)

    h_got(1, 0, core)
    pl.when(core == 0)(lambda: h_xy().start())
    h_core(1, 0).start()
    send_out(1, 0)
    h_got(0, 1, core)
    pl.when(core == 1)(lambda: h_yx().start())
    h_core(0, 1).start()
    send_out(0, 1)
    send_codes(2)

    @pl.when(at_end)
    def _():
        w_slab(slabs[2], False)

    @pl.when(inside)
    def _():
        w_slab(slabs[3], True)

    h_got(1, 1, core)
    h_core(1, 1).start()
    send_out(1, 1)
    send_codes(3)
    for kx in range(2):
        for ky in range(2):
            h_got(kx, ky, 1 - core)

    step = 2 * rows
    steps = tokens // step
    lines = lax.broadcasted_iota(jnp.int32, (8, rows), 0)

    def scores(n, zz, at=0, wide=slab):
        here = pl.ds(pl.multiple_of(zz * slab + at, 128), wide)
        there = pl.ds(pl.multiple_of(zz * slab + at, 16), wide)
        return jnp.dot(h_all[n * step:(n + 1) * step, here], w_all[there, :], preferred_element_type=f32)

    for j in range(nz - 1):
        for n in range(steps):
            span = pl.ds(n * step, step)
            if j:
                logits[span, :] += scores(n, slabs[j])
            else:
                logits[span, :] = scores(n, slabs[j])

    code_got[me] = code_own[...]
    others = pl.ds(0, group - 1)
    copy(code_got.at[others], code_got.at[others], cs.at[0], cr.at[0], b, over_x).wait_recv()
    for i in range(group):
        code_all[i * rows:(i + 1) * rows, :] = jnp.transpose(jnp.concatenate([code_got[i]] * (rows // 8), axis=0))

    early = lo
    pl.when(at_end)(lambda: w_slab(slabs[3], False, (0,)))
    for n in range(steps):
        logits[n * step:(n + 1) * step, :] += scores(n, slabs[3], y * (slab - early), early)
    pl.when(at_end)(lambda: w_slab(slabs[3], False, (1,)))

    sums = jnp.zeros((8, rows), f32)
    for n in range(steps):
        span = pl.ds(n * step, step)
        capped = softcap * jnp.tanh((logits[span, :] + scores(n, slabs[3], (1 - y) * early, slab - early)) * (1.0 / softcap))
        raised = jnp.exp(capped)
        logits[span, :] = capped
        expo[span, :] = raised
        total = jnp.broadcast_to(jnp.sum(raised, axis=1, keepdims=True), (step, 128))
        for k in range(2):
            turned = jnp.transpose(total[k * rows:(k + 1) * rows])
            sums = jnp.where(lines == 2 * n + k, turned[0:8], sums)
    stat_own[...] = sums

    def stat_copy(n):
        bb, vv, _ = peer(n)
        return copy(stat_own, stat_all.at[me], ss.at[0], sr.at[0], bb, vv)

    for n in range(len(peers)):
        stat_copy(n).start()

    ids = (lax.broadcasted_iota(jnp.int32, (step, half), 1) + (v * ny + y) * half).astype(f32)
    hit_total = jnp.zeros((step, 1), f32)
    for n in range(steps):
        span = pl.ds(n * step, step)
        capped = logits[span, :]
        hit = ids == code_all[span, 0:1]
        slope = 1.0 - (capped * (1.0 / softcap)) ** 2
        expo[span, :] = expo[span, :] * slope
        logits[span, :] = jnp.where(hit, slope, 0.0)
        hit_total = hit_total + jnp.sum(jnp.where(hit, capped, 0.0), axis=1, keepdims=True)
    hit_total = jnp.sum(hit_total, axis=0, keepdims=True)
    loss_one[...] = jnp.broadcast_to(hit_total, loss_one.shape)

    def hit_copy(n):
        bb, vv, _ = peer(n)
        return copy(loss_one, loss_all.at[me], ls.at[0], lr.at[0], bb, vv)

    for n in range(len(peers)):
        hit_copy(n).start()
    code_rows = jnp.zeros((8, rows), f32)
    for i in range(group):
        code_rows = jnp.where(lines == i, code_got[i], code_rows)
    weight = (code_rows >= 0).astype(f32)

    share_end(0, 0)
    share_end(1, 0)
    stat_all[me] = sums
    copy(stat_all.at[others], stat_all.at[others], ss.at[0], sr.at[0], b, over_x).wait_recv()
    partition = stat_all[0]
    for i in range(1, group):
        partition = partition + stat_all[i]
    scale = weight / partition

    lane_parts = [pl.ds(0, 128), pl.ds(128, half - 128)]

    def delta_copy(p):
        here = lane_parts[p]
        return copy(delta.at[0, :, here], delta.at[1, :, here], es.at[0], (cr, er)[p].at[0], over_y, v)

    chunks = range(half // 128)

    def chunk_of_delta(n):
        here = pl.ds(n * 128, 128)
        return copy(delta.at[0, :, here], d_end.at[:, here], zs.at[0], zr.at[n], near_end * ny + y, v)

    by_row = [jnp.transpose(jnp.broadcast_to(scale[i:i + 1, :], (rows, rows))) for i in range(group)]
    for n in chunks:
        here = pl.ds(n * 128, 128)
        for i in range(group):
            span = pl.ds(i * rows, rows)
            delta[0, span, here] = (expo[span, here] * by_row[i] - logits[span, here]).astype(bf16)
        pl.when(at_end)(lambda: chunk_of_delta(n).start())
        if n in (0, half // 128 - 1):
            delta_copy(min(n, 1)).start()

    targets = [jnp.where(at_end, far, across), jnp.where(at_end, across, near), jnp.where(at_end, near_end, far), z]
    top = y * shift

    def over_tokens(left, right):
        return lax.dot_general(left, right, (((0,), (0,)), ((), ())), preferred_element_type=f32)

    def grad_share(zz, r):
        return over_tokens(h_all[:, window(zz)], delta[r])

    def sent(k, r):
        return grad_send.at[k, r, pl.ds(pl.multiple_of(top, 16), cols)]

    def r_copy(k, r):
        return copy(sent(k, r), r_in.at[z * 2 + r], rs.at[0], rr.at[z, r], targets[k] * ny + y, v)

    def relay_copy(n, p):
        src = grad_send.at[n, 1, pl.ds(pl.multiple_of(top, 16), cols), lane_parts[p]]
        return copy(src, far_in.at[n, :, lane_parts[p]], rs.at[0], fr.at[n, p], near_end * ny + y, v)

    def part_copy(k, p):
        src = grad_send.at[k, 1, pl.ds(pl.multiple_of(top, 16), cols), lane_parts[p]]
        return copy(src, r_in.at[z * 2 + 1, :, lane_parts[p]], rs.at[0], rr.at[z, 1], targets[k] * ny + y, v)

    def chunk_copy(k, n):
        here = pl.ds(n * 128, 128)
        src = grad_send.at[k, 0, pl.ds(pl.multiple_of(top, 16), cols), here]
        return copy(src, r_in.at[z * 2, :, here], rs.at[0], rr.at[z, 0], targets[k] * ny + y, v)

    def to_end():
        @pl.when(inside)
        def _():
            grad_send[1, 0] = grad_share(near, 0).astype(bf16)
            r_copy(1, 0).start()

    def keep():
        @pl.when(inside)
        def _():
            held[0] = grad_share(across, 0)
            held[1] = grad_share(far, 0)

    def chunk(n):
        first = n * 128

        @pl.when(inside)
        def _():
            if n == 0:
                for kx in range(2):
                    for ky in range(2):
                        end_copy(flip(y, ky) * nv + flip(x, kx) * 2 + 1 - core).wait_recv()
            chunk_of_delta(n).wait_recv()
            right = d_end[:, first:first + 128]
            for k, slot, j in ((0, 0, 1), (2, 1, 0)):
                share = held[slot, :, first:first + 128] + over_tokens(h_end[:, j * win:(j + 1) * win], right)
                grad_send[k, 0, :, first:first + 128] = share.astype(bf16)
                chunk_copy(k, n).start()
            grad_own[0, :, first:first + 128] += over_tokens(h_end[:, 2 * win:3 * win], right)

    def head_part(k, p):
        here = lane_parts[p]
        share = over_tokens(h_all[:, window(targets[k])], delta[1, :, here])
        if k:
            grad_send[k, 1, :, here] = share.astype(bf16)
            pl.when(at_end)(lambda: relay_copy(1, p).start())
            pl.when(inside)(lambda: part_copy(k, p).start())
        else:
            @pl.when(at_end)
            def _():
                grad_send[k, 1, :, here] = share.astype(bf16)
                relay_copy(0, p).start()

            @pl.when(inside)
            def _():
                held[0, :, here] = share

    def head_rest():
        share = grad_share(targets[2], 1)

        @pl.when(at_end)
        def _():
            grad_send[2, 1] = share.astype(bf16)
            r_copy(2, 1).start()

        @pl.when(inside)
        def _():
            held[1] = share

    cstep = chunk_of(cols, 64)

    def over_cols(body):
        def one(n, carry):
            body(pl.multiple_of(n * cstep, 16))
            return carry

        lax.fori_loop(0, cols // cstep, one, 0)

    def relay(k, n, p):
        lane = lane_parts[p]

        @pl.when(inside)
        def _():
            relay_copy(n, p).wait_recv()

            def add(m):
                here = pl.ds(pl.multiple_of(top + m, 16), cstep)
                there = pl.ds(m, cstep)
                grad_send[k, 1, here, lane] = (
                    held[k // 2, here, lane] + far_in[n, there, lane].astype(f32)).astype(bf16)

            over_cols(add)
            part_copy(k, p).start()

    groups = column_groups(width)
    blocks = [(1, 1), (1, 0), (0, 1), (0, 0)]
    unit = width // (width // 256)

    def span_of(g):
        first, n = groups[g]
        return pl.ds(first * unit, n * unit)

    y_first = (3,)

    def block(g, one, two, cc):
        kx, ky = (two, one) if g in y_first else (one, two)
        return flip(y, ky) * nv + flip(x, kx) * 2 + cc

    def core_copy(g, one, two):
        return copy(part.at[hrow(block(g, one, two, 1 - core)), span_of(g)], core_in.at[one, two, :, span_of(g)],
                    ds.at[0], wr.at[g, 0], b, over_core)

    def over_one(g):
        return (over_y, v) if g in y_first else (b, over_x)

    def over_two(g):
        return (b, over_x) if g in y_first else (over_y, v)

    def one_copy(g, two):
        return copy(x_out.at[two, :, span_of(g)], x_in.at[two, :, span_of(g)], xs.at[0], (hr if two else xr).at[g],
                    *over_one(g))

    def two_copy(g):
        return copy(y_out.at[:, span_of(g)], y_in.at[:, span_of(g)], ys.at[0], wr.at[g, 1], *over_two(g))

    def part_group(g):
        first, n = groups[g]

        def columns(j, carry):
            span = pl.ds(pl.multiple_of(j * unit, 128), unit)
            part[:, span] = lax.dot_general(
                delta[0], w_all[span, :], (((1,), (1,)), ((), ())), preferred_element_type=f32)
            return carry

        lax.fori_loop(first, first + n, columns, 0)
        for one, two in blocks:
            core_copy(g, one, two).start()

    hstep = 16

    def over_rows(body):
        def one(n, carry):
            body(pl.multiple_of(n * hstep, hstep))
            return carry

        lax.fori_loop(0, rows // hstep, one, 0)

    def core_sum(g):
        span = span_of(g)
        landed = core_in.at[:, :, :, span]
        copy(landed, landed, ds.at[0], wr.at[g, 0], b, over_core).wait_recv()
        for one, two in blocks:
            start = block(g, one, two, core) * rows

            def add(n):
                here = pl.ds(pl.multiple_of(start + n, hstep), hstep)
                both = part[here, span] + core_in[one, two, pl.ds(n, hstep), span]
                if one:
                    x_out[two, pl.ds(n, hstep), span] = both.astype(bf16)
                else:
                    part[here, span] = both

            over_rows(add)
            if one:
                one_copy(g, two).start()

    def one_sum(g):
        span = span_of(g)
        for two in (1, 0):
            one_copy(g, two).wait_recv()
            start = block(g, 0, two, core) * rows

            def add(n):
                here = pl.ds(pl.multiple_of(start + n, hstep), hstep)
                total = part[here, span] + x_in[two, pl.ds(n, hstep), span].astype(f32)
                if two:
                    y_out[pl.ds(n, hstep), span] = total.astype(bf16)
                else:
                    hid_out[pl.ds(n, hstep), span] = total

            over_rows(add)
            if two:
                two_copy(g).start()

    def two_sum(g):
        span = span_of(g)
        two_copy(g).wait_recv()

        def add(n):
            here = pl.ds(n, hstep)
            hid_out[here, span] += y_in[here, span].astype(f32)

        over_rows(add)

    count = len(groups)

    def plane_copy(k):
        return copy(loss_two, loss_zs.at[z], ms.at[0], mr.at[0], z_peer(k), v)

    def plane_loss():
        loss_all[me] = loss_one[...]
        copy(loss_all.at[others], loss_all.at[others], ls.at[0], lr.at[0], b, over_x).wait_recv()
        hits = loss_all[0]
        for i in range(1, group):
            hits = hits + loss_all[i]
        logs = jnp.sum(weight * jnp.log(partition), axis=1, keepdims=True)
        loss_two[...] = jnp.broadcast_to(jnp.sum(logs, axis=0, keepdims=True), (8, rows)) - hits
        for k in range(1, nz):
            plane_copy(k).start()

    part_group(0)
    part_group(1)
    to_end()
    plane_loss()
    core_sum(0)
    part_group(2)
    core_sum(1)
    share_end(0, 1)
    keep()
    part_group(3)
    core_sum(2)
    share_end(1, 1)
    grad_own[0] = grad_share(z, 0)
    part_group(4)
    core_sum(3)
    chunk(0)
    for g in range(5, count):
        part_group(g)
        core_sum(g - 1)
    core_sum(count - 1)
    for n in chunks[1:-1]:
        chunk(n)
    one_sum(0)

    delta_copy(0).wait_recv()
    head_part(0, 0)
    head_part(1, 0)
    chunk(len(chunks) - 1)
    delta_copy(1).wait_recv()
    head_part(0, 1)
    head_part(1, 1)
    one_sum(1)
    head_rest()
    grad_own[1] = grad_share(z, 1)
    one_sum(2)
    relay(2, 0, 0)

    copy(w_over, w_over, wys.at[0], wr.at[0, 0], over_y, v).wait_send()
    for n in range(1, nz):
        sent_rows = w_all.at[pl.ds(0, n * slab)]
        for way, slabs_sent in ((0, z + 1), (1, nz - z)):
            going = (slabs_sent == n) & (has_down if way else has_up)
            pl.when(going)(lambda: copy(sent_rows, sent_rows, ws.at[way], wr.at[0, 0], b, over_x).wait_send())
    seven = h_all.at[pl.ds(0, 7 * rows)]
    copy(seven, seven, hs.at[0], hr.at[0], b, over_x).wait_send()
    for got, sem in ((code_got, cs), (stat_all, ss), (loss_all, ls)):
        copy(got.at[others], got.at[others], sem.at[0], sem.at[0], b, over_x).wait_send()
    one_sum(3)
    two_sum(0)
    copy(delta.at[0], delta.at[1], es.at[0], cr.at[0], over_y, v).wait_send()
    relay(0, 1, 0)
    copy(core_in, core_in, ds.at[0], wr.at[0, 0], b, over_core).wait_send()
    one_sum(4)
    two_sum(1)
    relay(2, 0, 1)
    relay(0, 1, 1)
    for g in range(5, count):
        one_sum(g)
    two_sum(2)
    for g in range(4, count - 1):
        two_sum(g)

    def r_got(zz, r):
        whole = r_in.at[zz * 2 + r]
        copy(whole, whole, rs.at[0], rr.at[zz, r], z_peer(1), v).wait_recv()

    def lanes(r):
        return pl.ds(pl.multiple_of(flip(y, r) * half, 128), half)

    def head_sum(r):
        r_got(across, r)

        def add(n):
            here = pl.ds(n, cstep)
            total = grad_own[r, pl.ds(pl.multiple_of(top + n, 16), cstep), :]
            head_out[here, lanes(r)] = total + r_in[across * 2 + r, here, :].astype(f32)

        over_cols(add)

        def by_near():
            r_got(near, r)

            def last(n):
                here = pl.ds(n, cstep)
                head_out[here, lanes(r)] += r_in[near * 2 + r, here, :].astype(f32)

            over_cols(last)

        if r:
            by_near()
        else:
            pl.when(at_end)(by_near)

    head_sum(0)
    loss_zs[z] = loss_two[...]
    along = loss_zs.at[pl.ds(0, nz - 1)]
    copy(along, along, ms.at[0], mr.at[0], z_peer(1), v).wait_recv()
    losses = loss_zs[0]
    for i in range(1, nz):
        losses = losses + loss_zs[i]
    loss_out[...] = losses * (1.0 / (tokens * nz))
    copy(along, along, ms.at[0], mr.at[0], z_peer(1), v).wait_send()
    two_sum(3)
    two_sum(count - 1)
    head_sum(1)

    rows_out = h_end.at[pl.ds(0, tokens // 2)]
    for part_sent, sem in ((x_out, xs), (y_out, ys), (rows_out, us)):
        copy(part_sent, part_sent, sem.at[0], sem.at[0], b, over_x).wait_send()

    @pl.when(at_end)
    def _():
        for part_sent, sem in ((d_end, zs), (r_in.at[pl.ds(0, 3)], rs)):
            copy(part_sent, part_sent, sem.at[0], sem.at[0], b, over_x).wait_send()

    @pl.when(inside)
    def _():
        six = r_in.at[pl.ds(0, 6)]
        copy(six, six, rs.at[0], rs.at[0], b, over_x).wait_send()


def finish_kernel(head_in, hid_in, loss_in, head_out, hid_out, loss_out, loss_one, sem):
    moves = [
        pltpu.make_async_copy(hid_in, hid_out, sem.at[0]),
        pltpu.make_async_copy(head_in, head_out, sem.at[1]),
        pltpu.make_async_copy(loss_one, loss_out, sem.at[2]),
    ]
    for one in moves[:2]:
        one.start()
    loss_one[...] = loss_in[0:1, 0:1]
    moves[2].start()
    for one in moves:
        one.wait()


def plane_local(hidden, head_weight, targets, valid_mask):
    nz, ny, nv = 4, 2, 4
    rows, width = hidden.shape
    entries, cols = head_weight.shape
    half = entries // ny
    group = ny * nv
    tokens = rows * group
    shift = cols % 128
    win = -(-(cols + shift) // 128) * 128
    vm = pltpu.VMEM
    dma = pltpu.SemaphoreType.DMA
    count = len(column_groups(width))
    line = vm((8, rows), f32)
    buffers = [
        vm((tokens, width), bf16), vm((width, half), bf16), vm((cols, half), bf16),
        vm((1, rows), jnp.int32), vm((1, rows), jnp.int32), line, vm((group, 8, rows), f32), vm((tokens, 128), f32),
        vm((tokens, half), f32), vm((tokens, half), f32), vm((2, tokens, half), bf16),
        line, vm((group, 8, rows), f32), line, line, vm((group, 8, rows), f32), vm((nz, 8, rows), f32),
        vm((2, win, half), f32), vm((2, win, half), f32), vm((3, 2, win, half), bf16),
        vm((2, cols, half), bf16), vm((nz * 2, cols, half), bf16), vm((tokens, 3 * win), bf16), vm((tokens, half), bf16),
        vm((tokens, width), f32), vm((2, 2, rows, width), f32),
        vm((2, rows, width), bf16), vm((2, rows, width), bf16), vm((rows, width), bf16), vm((rows, width), bf16),
    ]
    sems = [
        dma((5,)), dma((1,)), dma((group,)), dma((2,)), dma((8, 2)), dma((1,)),
        dma((1,)), dma((1,)), dma((1,)), dma((1,)), dma((1,)), dma((1,)), dma((1,)), dma((1,)),
        dma((1,)), dma((1,)), dma((1,)), dma((nz, 2)), dma((2, 2)), dma((1,)), dma((half // 128,)), dma((1,)), dma((group,)),
        dma((1,)), dma((1,)), dma((count,)), dma((1,)),
    ]
    whole = pl.BlockSpec(memory_space=vm)
    head_t, hidden_grad, loss = pl.pallas_call(
        plane_kernel,
        out_shape=(
            vm((cols, entries), f32),
            vm((rows, width), f32),
            vm((8, rows), f32),
        ),
        in_specs=[pl.BlockSpec(memory_space=pl.ANY)] * 4,
        out_specs=(whole,) * 3,
        scratch_shapes=buffers + sems,
        compiler_params=pltpu.CompilerParams(
            collective_id=1, has_side_effects=True, vmem_limit_bytes=58 * 1024 * 1024),
    )(hidden, jnp.transpose(head_weight), targets[None, :], valid_mask[None, :])
    anywhere = pl.BlockSpec(memory_space=pl.ANY)
    head_t, hidden_grad, loss = pl.pallas_call(
        finish_kernel,
        out_shape=(
            jax.ShapeDtypeStruct((cols, entries), f32),
            jax.ShapeDtypeStruct((rows, width), f32),
            jax.ShapeDtypeStruct((1, 1), f32),
        ),
        in_specs=[whole] * 3,
        out_specs=(anywhere,) * 3,
        scratch_shapes=[vm((1, 1), f32), dma((3,))],
        compiler_params=pltpu.CompilerParams(vmem_limit_bytes=1024 * 1024),
    )(head_t, hidden_grad, loss)
    return jnp.transpose(head_t), hidden_grad, loss[0, 0]


def in_planes(nb, nv, hidden, head_weight, targets, valid_mask):
    rows, width = hidden.shape
    entries, cols = head_weight.shape
    fits = nb == 8 and nv == 4 and rows == 128 and width % 256 == 0 and width >= 3072
    fits = fits and len(column_groups(width)) <= 8
    return fits and entries % 256 == 0 and entries >= 512 and cols % 32 == 0 and (2 * cols) % 128 == 0


def device(nb, nv, *arrays):
    if in_planes(nb, nv, *arrays):
        return plane_local(*arrays)
    return local(nb, nv, *arrays)


def solution(mesh):
    placed = (
        P(("batch", "vocab"), None),
        P("vocab", "batch"),
        P(("batch", "vocab")),
        P(("batch", "vocab")),
    )
    return jax.shard_map(
        functools.partial(device, mesh.shape["batch"], mesh.shape["vocab"]),
        mesh=mesh,
        in_specs=placed,
        out_specs=(P("vocab", "batch"), P(("batch", "vocab"), None), P()),
        check_vma=False,
    )
```

```python
import functools

import jax
import jax.numpy as jnp
from jax import lax
from jax.experimental import pallas as pl
from jax.experimental.pallas import tpu as pltpu
from jax.sharding import PartitionSpec as P

softcap = 30.0
MESH = pl.DeviceIdType.MESH
f32, bf16 = jnp.float32, jnp.bfloat16


def chunk_of(length, most):
    return max(s for s in range(16, most + 1, 16) if length % s == 0)


def kernel(sizes, h_in, w_in, code_in, head_out, hid_out, loss_out, h_all, w_all, code_got, code_all,
           logits, delta, stat_own, stat_all, loss_own, loss_all, grad, grad_send, r_in,
           part, core_in, x_out, x_in, y_out, y_in, far_own, far_in, *sems):
    nz, ny, nx, nv = sizes
    (own_sem, hs, hf, hd, hr, ws_up, ws_dn, ws_y, wr, cs, cr, ss, sr, ls, lr,
     rs, rr, ds, dr, xs, xr, ys, yr, fs, fr) = sems
    nb = nz * ny
    rows, width = h_in.shape
    cols, half = w_in.shape[1:]
    group = ny * nv
    tokens = rows * group
    entries = ny * half
    b, v = lax.axis_index("batch"), lax.axis_index("vocab")
    z, y = lax.div(b, ny), lax.rem(b, ny)
    x, core = lax.div(v, 2), lax.rem(v, 2)
    other = x * 2 + 1 - core
    me = y * nv + v

    def at(bb, vv):
        return {"batch": bb, "vocab": vv}

    def copy(src, dst, send, recv, bb, vv):
        return pltpu.make_async_remote_copy(
            src_ref=src, dst_ref=dst, send_sem=send, recv_sem=recv, device_id=at(bb, vv), device_id_type=MESH)

    def hrow(i):
        return pl.ds(pl.multiple_of(i * rows, 16), rows)

    def wrow(i):
        return pl.ds(pl.multiple_of(i * cols, 16), cols)

    def turn_y(k):
        return lax.rem(y + k, ny)

    def turn_x(k):
        return lax.rem(x + k, nx)

    peers = [(k, j) for k in range(ny) for j in range(nv) if k or j]

    def peer(n):
        k, j = peers[n]
        return z * ny + turn_y(k), lax.rem(v + j, nv), turn_y(k) * nv + lax.rem(v + j, nv)

    barrier = pltpu.get_barrier_semaphore()
    for k in range(1, nb):
        pl.semaphore_signal(barrier, inc=1, device_id=at(lax.rem(b + k, nb), v), device_id_type=MESH)
    met = [n for n in range(len(peers)) if peers[n][1]]
    for n in met:
        bb, vv, _ = peer(n)
        pl.semaphore_signal(barrier, inc=1, device_id=at(bb, vv), device_id_type=MESH)
    pl.semaphore_wait(barrier, nb - 1 + len(met))

    def w_z(zz, yy, up, own=False):
        i = zz * ny + yy
        dst = w_all.at[wrow(i)]
        sem = (ws_up if up else ws_dn).at[i]
        return copy(w_in.at[y] if own else dst, dst, sem, wr.at[i], b + ny if up else b - ny, v)

    def w_y(k):
        return copy(w_in.at[turn_y(k)], w_all.at[wrow(b)], ws_y.at[k - 1], wr.at[b], z * ny + turn_y(k), v)

    def w_got(zz, yy):
        w_z(zz, yy, True).wait_recv()

    has_up, has_down = z + 1 < nz, z >= 1

    def h_send(n_src, sem, bb, vv, own=False):
        dst = h_all.at[hrow(n_src)]
        return copy(h_in if own else dst, dst, sem, hr.at[n_src], bb, vv)

    def h_x(k):
        return h_send(me, hs.at[k - 1], b, turn_x(k) * 2 + core, True)

    def h_y(k):
        return h_send(me, hs.at[nx + k - 1], z * ny + turn_y(k), v, True)

    def h_xy(kx, ky):
        return h_send(y * nv + turn_x(kx) * 2 + core, hf.at[kx, ky], z * ny + turn_y(ky), v)

    def h_yx(kx, ky):
        return h_send(turn_y(ky) * nv + v, hf.at[kx, ky], b, turn_x(kx) * 2 + core)

    def h_core(kx, ky):
        i = turn_y(ky) * nv + turn_x(kx) * 2 + core
        return h_send(i, hd.at[kx, ky], b, other, kx == 0 and ky == 0)

    def h_got(kx, ky, cc):
        i = turn_y(ky) * nv + turn_x(kx) * 2 + cc
        h_send(i, hd.at[kx, ky], b, other).wait_recv()

    def code_copy(n):
        bb, vv, _ = peer(n)
        return copy(code_in, code_got.at[me], cs.at[n], cr.at[me], bb, vv)

    for k in range(1, ny):
        w_y(k).start()
    pl.when(has_up)(lambda: w_z(z, y, True, True).start())
    pl.when(has_down)(lambda: w_z(z, y, False, True).start())
    for k in range(1, nx):
        h_x(k).start()
    for k in range(1, ny):
        h_y(k).start()
    for n in range(len(peers)):
        code_copy(n).start()
    h_core(0, 0).start()
    local = [
        pltpu.make_async_copy(w_in.at[y], w_all.at[wrow(b)], own_sem.at[0]),
        pltpu.make_async_copy(h_in, h_all.at[hrow(me)], own_sem.at[1]),
    ]
    for one in local:
        one.start()

    for k in range(1, ny):
        w_got(z, turn_y(k))
        pl.when(has_up)(lambda: w_z(z, turn_y(k), True).start())
        pl.when(has_down)(lambda: w_z(z, turn_y(k), False).start())

    def h_pass():
        for kx in range(1, nx):
            h_got(kx, 0, core)
            for ky in range(1, ny):
                pl.when(core == 0)(lambda: h_xy(kx, ky).start())
            h_core(kx, 0).start()
        for ky in range(1, ny):
            h_got(0, ky, core)
            for kx in range(1, nx):
                pl.when(core == 1)(lambda: h_yx(kx, ky).start())
            h_core(0, ky).start()

    def h_rest():
        for kx in range(1, nx):
            for ky in range(1, ny):
                h_got(kx, ky, core)
                h_core(kx, ky).start()

    for k in range(1, nz):
        for j in range(ny):
            yy = turn_y(j)

            @pl.when(z - k >= 0)
            def _():
                w_got(z - k, yy)
                pl.when(has_up)(lambda: w_z(z - k, yy, True).start())

            @pl.when(z + k < nz)
            def _():
                w_got(z + k, yy)
                pl.when(has_down)(lambda: w_z(z + k, yy, False).start())
        if k == 1:
            h_pass()
        if k == min(2, nz - 1):
            h_rest()

    for one in local:
        one.wait()
    for kx in range(nx):
        for ky in range(ny):
            h_got(kx, ky, 1 - core)
    code_got[me] = code_in[...]
    for n in range(len(peers)):
        bb, vv, i = peer(n)
        copy(code_in, code_got.at[i], cs.at[n], cr.at[i], bb, vv).wait_recv()
    for i in range(group):
        code_all[i * rows:(i + 1) * rows, :] = jnp.transpose(jnp.concatenate([code_got[i]] * 16, axis=0))

    step = chunk_of(tokens, 256)
    lanes = lax.broadcasted_iota(jnp.int32, (step, 128), 1)
    first = v * entries + y * half

    def span_of(n):
        return pl.ds(pl.multiple_of(n * step, step), step)

    def hits(n):
        ids = lax.broadcasted_iota(jnp.int32, (step, half), 1) + first
        return ids == code_all[span_of(n), 0:1].astype(jnp.int32)

    for n in range(tokens // step):
        span = pl.ds(n * step, step)
        scores = jnp.dot(h_all[span, :], w_all[...], preferred_element_type=f32)
        capped = softcap * jnp.tanh(scores * (1.0 / softcap))
        logits[span, :] = capped
        total = jnp.sum(jnp.exp(capped), axis=1, keepdims=True)
        hit_sum = jnp.sum(jnp.where(hits(n), capped, 0.0), axis=1, keepdims=True)
        turned = jnp.transpose(jnp.where(lax.rem(lanes, 8) < 4, total, hit_sum))
        stat_own[:, n * step:(n + 1) * step] = turned[0:8]

    def stat_copy(n):
        bb, vv, _ = peer(n)
        return copy(stat_own, stat_all.at[me], ss.at[n], sr.at[me], bb, vv)

    for n in range(len(peers)):
        stat_copy(n).start()
    for n in range(len(peers)):
        bb, vv, i = peer(n)
        copy(stat_own, stat_all.at[i], ss.at[n], sr.at[i], bb, vv).wait_recv()
    stats = stat_own[...]
    for n in range(len(peers)):
        stats = stats + stat_all[peer(n)[2]]

    loss = jnp.zeros((1, 1), f32)
    for n in range(tokens // step):
        span = pl.ds(n * step, step)
        weight = (code_all[span, 0:1] >= 0).astype(f32)
        back = jnp.transpose(jnp.concatenate([stats[:, n * step:(n + 1) * step]] * 16, axis=0))
        partition, target_logit = back[:, 0:1], back[:, 4:5]
        loss = loss + jnp.sum(weight * (jnp.log(partition) - target_logit), axis=0, keepdims=True)
        capped = logits[span, :]
        slope = 1.0 - (capped * (1.0 / softcap)) ** 2
        delta[span, :] = ((jnp.exp(capped) * (weight / partition) - jnp.where(hits(n), weight, 0.0)) * slope
                          ).astype(bf16)
    loss_own[...] = jnp.broadcast_to(loss, loss_own.shape)

    def loss_copy(k):
        return copy(loss_own, loss_all.at[b], ls.at[k - 1], lr.at[b], lax.rem(b + k, nb), v)

    def r_copy(zz, yy):
        i = zz * ny + yy
        return copy(grad_send.at[wrow(i)], r_in.at[z, y], rs.at[i], rr.at[b], i, v)

    def grad_share(span):
        return lax.dot_general(h_all[:, span], delta[...], (((0,), (0,)), ((), ())), preferred_element_type=f32)

    slab = ny * cols
    relay = nz == 4 and slab % 128 == 0
    turn = jnp.where(z * 2 >= nz, 1, nz - 1)
    order = [lax.rem(z + turn * k, nz) for k in range(1, nz)] + [z]
    at_end = (z == 0) | (z == nz - 1)
    far = jnp.where(z * 2 >= nz, 0, nz - 1)
    near = jnp.where(z * 2 >= nz, z - 1, z + 1)

    def far_copy(yy):
        return copy(grad_send.at[wrow(far * ny + yy)], far_in.at[yy], fs.at[yy], fr.at[yy], near * ny + y, v)

    def direct(zz):
        return jnp.logical_not(at_end & (zz == far))
    if slab % 128 == 0:
        mine = y * cols
        for n in range(nz):
            zz = order[n]
            span = pl.ds(pl.multiple_of(zz * slab, 128), slab)
            share = grad_share(span)
            held = relay and n == 1
            if n == nz - 1:
                grad[...] = share
            if held:
                @pl.when(jnp.logical_not(at_end))
                def _():
                    far_own[...] = share

                @pl.when(at_end)
                def _():
                    grad_send[span, :] = share.astype(bf16)
                    for k in range(ny):
                        r_copy(zz, turn_y(k)).start()
            else:
                grad_send[span, :] = share.astype(bf16)
                for k in range(ny):
                    yy = turn_y(k)
                    if relay and n == 0:
                        pl.when(at_end)(lambda: far_copy(yy).start())
                        pl.when(jnp.logical_not(at_end))(lambda: r_copy(zz, yy).start())
                    elif n < nz - 1 or k:
                        r_copy(zz, yy).start()
    else:
        mine = b * cols
        wide = chunk_of(width, 256)

        def grad_step(j, carry):
            span = pl.ds(pl.multiple_of(j * wide, wide), wide)
            share = grad_share(span)
            grad[span, :] = share
            grad_send[span, :] = share.astype(bf16)
            return carry

        lax.fori_loop(0, width // wide, grad_step, 0)
        for n in range(nz):
            for k in range(ny):
                if n < nz - 1 or k:
                    r_copy(order[n], turn_y(k)).start()
    for k in range(1, nb):
        loss_copy(k).start()

    wide = chunk_of(width, 256)

    def part_step(j, carry):
        span = pl.ds(pl.multiple_of(j * wide, wide), wide)
        part[:, span] = lax.dot_general(
            delta[...], w_all[span, :], (((1,), (1,)), ((), ())), preferred_element_type=f32)
        return carry

    lax.fori_loop(0, width // wide, part_step, 0)

    def core_copy(kx, ky):
        i = turn_y(ky) * nv + turn_x(kx) * 2 + 1 - core
        return copy(part.at[hrow(i)], core_in.at[kx, ky], ds.at[kx, ky], dr.at[kx, ky], b, other)

    def x_copy(kx, ky):
        return copy(x_out.at[kx - 1, ky], x_in.at[kx - 1, ky], xs.at[kx, ky], xr.at[kx, ky],
                    b, turn_x(kx) * 2 + core)

    def y_copy(ky):
        return copy(y_out.at[ky - 1], y_in.at[ky - 1], ys.at[ky], yr.at[ky], z * ny + turn_y(ky), v)

    ways = [(kx % nx, ky % ny) for kx in range(1, nx + 1) for ky in range(1, ny + 1)]
    for kx, ky in ways:
        core_copy(kx, ky).start()
    hstep = 16

    def over_rows(start, body):
        def one(r, carry):
            body(pl.ds(pl.multiple_of(r * hstep, hstep), hstep),
                 pl.ds(pl.multiple_of(start + r * hstep, hstep), hstep))
            return carry

        lax.fori_loop(0, rows // hstep, one, 0)

    def start_of(kx, ky):
        return (turn_y(ky) * nv + turn_x(kx) * 2 + core) * rows

    for kx, ky in ways:
        core_copy(kx, ky).wait_recv()

        def core_sum(span, here):
            both = part[here, :] + core_in[kx, ky, span, :]
            if kx:
                x_out[kx - 1, ky, span, :] = both.astype(bf16)
            else:
                part[here, :] = both

        over_rows(start_of(kx, ky), core_sum)
        if kx:
            x_copy(kx, ky).start()

    cstep = chunk_of(cols, 64)

    def over_cols(body):
        def one(r, carry):
            body(pl.multiple_of(r * cstep, 16))
            return carry

        lax.fori_loop(0, cols // cstep, one, 0)

    if relay:
        @pl.when(jnp.logical_not(at_end))
        def _():
            for k in range(ny):
                yy = turn_y(k)
                far_copy(yy).wait_recv()

                def far_sum(r):
                    here = pl.ds(pl.multiple_of(yy * cols + r, 16), cstep)
                    there = pl.ds(pl.multiple_of((far * ny + yy) * cols + r, 16), cstep)
                    grad_send[there, :] = (far_own[here, :] + far_in[yy, pl.ds(r, cstep), :].astype(f32)).astype(bf16)

                over_cols(far_sum)
                r_copy(far, yy).start()

    for ky in [k % ny for k in range(1, ny + 1)]:
        for kx in range(1, nx):
            x_copy(kx, ky).wait_recv()

        def x_sum(span, here):
            total = part[here, :]
            for kx in range(1, nx):
                total = total + x_in[kx - 1, ky, span, :].astype(f32)
            if ky:
                y_out[ky - 1, span, :] = total.astype(bf16)
            else:
                hid_out[span, :] = total

        over_rows(start_of(0, ky), x_sum)
        if ky:
            y_copy(ky).start()

    def r_got(zz, yy):
        i = zz * ny + yy
        copy(grad_send.at[wrow(i)], r_in.at[zz, yy], rs.at[i], rr.at[i], i, v).wait_recv()

    for k in range(1, ny):
        r_got(z, turn_y(k))

    def first_sum(r):
        head_out[y, pl.ds(r, cstep), :] = grad[pl.ds(pl.multiple_of(mine + r, 16), cstep), :]
        for k in range(1, ny):
            head_out[turn_y(k), pl.ds(r, cstep), :] = r_in[z, turn_y(k), pl.ds(r, cstep), :].astype(f32)

    over_cols(first_sum)
    hops = [jnp.where(z * 2 >= nz, lax.rem(z + nz - n, nz), lax.rem(z + n, nz)) for n in range(1, nz)]
    for n in range(1, nz):
        zz = hops[n - 1]
        if n == nz - 1:
            for ky in range(1, ny):
                y_copy(ky).wait_recv()

                def y_sum(span, here):
                    hid_out[span, :] += y_in[ky - 1, span, :].astype(f32)

                over_rows(0, y_sum)

        def more_sum(r):
            for k in range(ny):
                head_out[turn_y(k), pl.ds(r, cstep), :] += r_in[zz, turn_y(k), pl.ds(r, cstep), :].astype(f32)

        def arrived():
            for k in range(ny):
                r_got(zz, turn_y(k))
            over_cols(more_sum)

        if relay:
            pl.when(direct(zz))(arrived)
        else:
            arrived()

    losses = loss_own[...]
    for k in range(1, nb):
        i = lax.rem(b + k, nb)
        copy(loss_own, loss_all.at[i], ls.at[k - 1], lr.at[i], i, v).wait_recv()
        losses = losses + loss_all[i]
    loss_out[...] = losses * (1.0 / (tokens * nb))

    for j in range(ny):
        yy = turn_y(j)
        pl.when(has_up)(lambda: w_z(z, yy, True, j == 0).wait_send())
        pl.when(has_down)(lambda: w_z(z, yy, False, j == 0).wait_send())
        for k in range(1, nz):
            @pl.when(z - k >= 0)
            def _():
                pl.when(has_up)(lambda: w_z(z - k, yy, True).wait_send())

            @pl.when(z + k < nz)
            def _():
                pl.when(has_down)(lambda: w_z(z + k, yy, False).wait_send())
    for k in range(1, ny):
        w_y(k).wait_send()
        h_y(k).wait_send()
        y_copy(k).wait_send()
    for k in range(1, nx):
        h_x(k).wait_send()
        for ky in range(1, ny):
            pl.when(core == 0)(lambda: h_xy(k, ky).wait_send())
            pl.when(core == 1)(lambda: h_yx(k, ky).wait_send())
    for kx, ky in ways:
        h_core(kx, ky).wait_send()
        core_copy(kx, ky).wait_send()
        if kx:
            x_copy(kx, ky).wait_send()
    for n in range(len(peers)):
        code_copy(n).wait_send()
        stat_copy(n).wait_send()
    for k in range(1, nb):
        loss_copy(k).wait_send()
    for n in range(nz):
        for k in range(ny):
            yy = turn_y(k)
            if relay and n == 0:
                pl.when(at_end)(lambda: far_copy(yy).wait_send())
                pl.when(jnp.logical_not(at_end))(lambda: r_copy(order[n], yy).wait_send())
            elif n < nz - 1 or k:
                r_copy(order[n], yy).wait_send()


def local(nb, nv, hidden, head_weight, targets, valid_mask):
    nx = nv // 2
    ny = nx if nx <= 2 and nb % nx == 0 else 1
    nz = nb // ny
    rows, width = hidden.shape
    entries, cols = head_weight.shape
    half = entries // ny
    group = ny * nv
    tokens = rows * group
    code = jnp.broadcast_to(jnp.where(valid_mask != 0, targets, -1).astype(f32)[None, :], (8, rows))
    weight = jnp.transpose(head_weight.reshape(ny, half, cols), (0, 2, 1))
    vm = pltpu.VMEM
    dma = pltpu.SemaphoreType.DMA
    slab = ny * cols
    ly, lx = max(ny - 1, 1), max(nx - 1, 1)
    buffers = [
        vm((tokens, width), bf16), vm((width, half), bf16), vm((group, 8, rows), f32), vm((tokens, 128), f32),
        vm((tokens, half), f32), vm((tokens, half), bf16),
        vm((8, tokens), f32), vm((group, 8, tokens), f32), vm((8, 128), f32), vm((nb, 8, 128), f32),
        vm((slab if slab % 128 == 0 else width, half), f32), vm((width, half), bf16), vm((nz, ny, cols, half), bf16),
        vm((tokens, width), f32), vm((nx, ny, rows, width), f32),
        vm((lx, ny, rows, width), bf16), vm((lx, ny, rows, width), bf16),
        vm((ly, rows, width), bf16), vm((ly, rows, width), bf16),
        vm((slab if nz == 4 else 16, half), f32), vm((ny, cols if nz == 4 else 16, half), bf16),
    ]
    sems = [
        dma((2,)), dma((nx + ny,)), dma((nx, ny)), dma((nx, ny)), dma((group,)), dma((nb,)), dma((nb,)),
        dma((ly,)), dma((nb,)), dma((group,)), dma((group,)), dma((group,)), dma((group,)), dma((nb,)), dma((nb,)),
        dma((nb,)), dma((nb,)), dma((nx, ny)), dma((nx, ny)), dma((nx, ny)), dma((nx, ny)), dma((ny,)), dma((ny,)),
        dma((ny,)), dma((ny,)),
    ]
    whole = pl.BlockSpec(memory_space=vm)
    head_t, hidden_grad, loss = pl.pallas_call(
        functools.partial(kernel, (nz, ny, nx, nv)),
        out_shape=(
            jax.ShapeDtypeStruct((ny, cols, half), f32),
            jax.ShapeDtypeStruct((rows, width), f32),
            jax.ShapeDtypeStruct((8, 128), f32),
        ),
        in_specs=[whole] * 3,
        out_specs=(whole,) * 3,
        scratch_shapes=buffers + sems,
        compiler_params=pltpu.CompilerParams(
            collective_id=0, has_side_effects=True, vmem_limit_bytes=67043328),
    )(hidden, weight, code)
    return jnp.transpose(head_t, (0, 2, 1)).reshape(entries, cols), hidden_grad, loss[0, 0]


def column_groups(width):
    left = width // 256 - 11
    sizes = [1, 2, 3, 2]
    while left > 0:
        sizes.append(min(3, left))
        left -= sizes[-1]
    sizes += [2, 1]
    starts = [sum(sizes[:n]) for n in range(len(sizes))]
    return [(s, n) for s, n in zip(starts, sizes)]


def plane_kernel(h_in, w_in, ids_in, mask_in, head_out, hid_out, loss_out, h_all, w_all, w_over, ids_own, mask_own,
                 code_own, code_got, code_all,
                 logits, expo, delta, stat_own, stat_all, loss_one, loss_two, loss_all, loss_zs,
                 grad_own, held, grad_send, far_in, r_in, h_end, d_end, part, core_in, x_out, x_in, y_out, y_in, *sems):
    (own_sem, hs, hr, ws, wr, wys, cs, cr, ss, sr, ls, lr, ms, mr,
     es, er, rs, rr, fr, zs, zr, us, ur, ds, xs, xr, ys) = sems
    nz, ny, nv = 4, 2, 4
    nb = nz * ny
    rows, width = h_in.shape
    cols, half = w_in.shape[0], w_in.shape[1] // ny
    piece = cols // 2
    group = ny * nv
    tokens = rows * group
    slab = ny * cols
    shift, lo = cols % 128, cols - cols % 128
    win = -(-(cols + shift) // 128) * 128
    b, v = lax.axis_index("batch"), lax.axis_index("vocab")
    z, y = lax.div(b, ny), lax.rem(b, ny)
    x, core = lax.div(v, 2), lax.rem(v, 2)
    me = y * nv + v
    low = z * 2 < nz
    at_end = (z == 0) | (z == nz - 1)
    inside = jnp.logical_not(at_end)

    def flip(a, k):
        return 1 - a if k else a

    def copy(src, dst, send, recv, bb, vv):
        return pltpu.make_async_remote_copy(
            src_ref=src, dst_ref=dst, send_sem=send, recv_sem=recv,
            device_id={"batch": bb, "vocab": vv}, device_id_type=MESH)

    def hrow(i):
        return pl.ds(pl.multiple_of(i * rows, 16), rows)

    far = jnp.where(low, nz - 1, 0)
    across = jnp.where(low, 2, 1)
    near_end = jnp.where(low, 1, 2)
    over_x, over_y, over_core = (1 - x) * 2 + core, z * ny + 1 - y, x * 2 + 1 - core
    peers = [(ky, kx, kc) for ky in range(2) for kx in range(2) for kc in range(2) if ky or kx or kc]

    def peer(n):
        ky, kx, kc = peers[n]
        yy, vv = flip(y, ky), flip(x, kx) * 2 + flip(core, kc)
        return z * ny + yy, vv, yy * nv + vv

    def z_peer(k):
        return lax.rem(z + k, nz) * ny + y

    has_up, has_down = z + 1 < nz, z >= 1
    barrier = pltpu.get_barrier_semaphore()

    def greet(bb, vv):
        pl.semaphore_signal(barrier, inc=1, device_id={"batch": bb, "vocab": vv}, device_id_type=MESH)

    pl.when(has_up)(lambda: greet(b + ny, v))
    pl.when(has_down)(lambda: greet(b - ny, v))
    greet(over_y, v)
    greet(b, over_x)
    greet(b, over_core)
    first = pl.ds(pl.multiple_of(y * half, 128), half)
    second = pl.ds(pl.multiple_of((1 - y) * half, 128), half)
    local = [
        pltpu.make_async_copy(w_in.at[:, second], w_over, own_sem.at[0]),
        pltpu.make_async_copy(w_in.at[:, first], w_all.at[pl.ds(pl.multiple_of(b * cols, 16), cols)], own_sem.at[1]),
        pltpu.make_async_copy(ids_in, ids_own, own_sem.at[2]),
        pltpu.make_async_copy(mask_in, mask_own, own_sem.at[3]),
        pltpu.make_async_copy(h_in, h_all.at[hrow(me)], own_sem.at[4]),
    ]
    for one in local:
        one.start()
    for one in local[:2]:
        one.wait()
    pl.semaphore_wait(barrier, jnp.where(inside, 5, 4))

    def w_ref(i, h):
        return w_all.at[pl.ds(pl.multiple_of(i * cols + h * piece, 16), piece)]

    def w_z(i, h, up):
        return copy(w_ref(i, h), w_ref(i, h), ws.at[0 if up else 1],
                    wr.at[i, h], b + ny if up else b - ny, v)

    def w_pass(i, h, up):
        return copy(w_ref(i, h), w_ref(i, h), ws.at[jnp.where(up, 0, 1)], wr.at[i, h], jnp.where(up, b + ny, b - ny), v)

    def w_y(h):
        return copy(w_over.at[pl.ds(h * piece, piece)], w_ref(b, h), wys.at[0], wr.at[b, h], over_y, v)

    def w_got(i, h):
        copy(w_ref(i, h), w_ref(i, h), wys.at[0], wr.at[i, h], over_y, v).wait_recv()

    near = z + 1 - 2 * lax.rem(z, 2)
    slabs = [z, near, jnp.where(low, 2, 1), jnp.where(low, 3, 0)]

    def h_send(i, bb, vv):
        return copy(h_all.at[hrow(i)], h_all.at[hrow(i)], hs.at[0], hr.at[i], bb, vv)

    def h_x():
        return h_send(me, b, over_x)

    def h_y():
        return h_send(me, over_y, v)

    def h_xy():
        return h_send(y * nv + over_x, over_y, v)

    def h_yx():
        return h_send((1 - y) * nv + v, b, over_x)

    def h_core(kx, ky):
        i = flip(y, ky) * nv + flip(x, kx) * 2 + core
        return h_send(i, b, over_core)

    def h_got(kx, ky, cc):
        i = flip(y, ky) * nv + flip(x, kx) * 2 + cc
        h_send(i, b, over_core).wait_recv()

    def window(zz):
        return pl.ds(pl.multiple_of(zz * slab + y * lo, 128), win)

    def mine_of(kx, ky):
        return flip(y, ky) * nv + flip(x, kx) * 2 + core

    def h_out(kx, ky, j):
        i = mine_of(kx, ky)
        return copy(h_all.at[hrow(i), window((far, across, near_end)[j])], h_end.at[hrow(i), pl.ds(j * win, win)],
                    us.at[0], ur.at[i], near_end * ny + y, v)

    def send_out(kx, ky):
        @pl.when(at_end)
        def _():
            for j in range(3):
                h_out(kx, ky, j).start()

    def end_copy(i):
        return copy(h_end.at[hrow(i)], h_end.at[hrow(i)], us.at[0], ur.at[i], b, over_core)

    def share_end(kx, ky):
        @pl.when(inside)
        def _():
            end_copy(mine_of(kx, ky)).wait_recv()
            end_copy(mine_of(kx, ky)).start()

    def code_copy(n):
        bb, vv, _ = peer(n)
        return copy(code_own, code_got.at[me], cs.at[0], cr.at[0], bb, vv)

    for h in range(2):
        w_y(h).start()
    for h in range(2):
        pl.when(has_up)(lambda: w_z(b, h, True).start())
        pl.when(has_down)(lambda: w_z(b, h, False).start())
    for one in local[2:]:
        one.wait()
    code = jnp.where(mask_own[...] != 0, ids_own[...], -1).astype(f32)
    code_own[...] = jnp.broadcast_to(code, code_own.shape)
    h_x().start()
    h_y().start()
    h_core(0, 0).start()

    def send_codes(count):
        for n in range(len(peers)):
            if sum(peers[n]) == count:
                code_copy(n).start()

    send_codes(1)
    for h in range(2):
        i = z * ny + 1 - y
        w_got(i, h)
        pl.when(has_up)(lambda: w_z(i, h, True).start())
        pl.when(has_down)(lambda: w_z(i, h, False).start())
    send_out(0, 0)

    def w_slab(zz, onward, which=(0, 1), halves=(0, 1)):
        for k in which:
            for h in halves:
                i = zz * ny + flip(y, k)
                w_got(i, h)
                if onward:
                    w_pass(i, h, zz < z).start()

    @pl.when(at_end)
    def _():
        w_slab(slabs[1], False)

    @pl.when(inside)
    def _():
        w_slab(slabs[1], True)
        w_slab(slabs[2], True)

    h_got(1, 0, core)
    pl.when(core == 0)(lambda: h_xy().start())
    h_core(1, 0).start()
    send_out(1, 0)
    h_got(0, 1, core)
    pl.when(core == 1)(lambda: h_yx().start())
    h_core(0, 1).start()
    send_out(0, 1)
    send_codes(2)

    @pl.when(at_end)
    def _():
        w_slab(slabs[2], False)

    @pl.when(inside)
    def _():
        w_slab(slabs[3], True)

    h_got(1, 1, core)
    h_core(1, 1).start()
    send_out(1, 1)
    send_codes(3)
    for kx in range(2):
        for ky in range(2):
            h_got(kx, ky, 1 - core)

    step = 2 * rows
    steps = tokens // step
    lines = lax.broadcasted_iota(jnp.int32, (8, rows), 0)

    def scores(n, zz, at=0, wide=slab):
        here = pl.ds(pl.multiple_of(zz * slab + at, 128), wide)
        there = pl.ds(pl.multiple_of(zz * slab + at, 16), wide)
        return jnp.dot(h_all[n * step:(n + 1) * step, here], w_all[there, :], preferred_element_type=f32)

    for j in range(nz - 1):
        for n in range(steps):
            span = pl.ds(n * step, step)
            if j:
                logits[span, :] += scores(n, slabs[j])
            else:
                logits[span, :] = scores(n, slabs[j])

    code_got[me] = code_own[...]
    others = pl.ds(0, group - 1)
    copy(code_got.at[others], code_got.at[others], cs.at[0], cr.at[0], b, over_x).wait_recv()
    for i in range(group):
        code_all[i * rows:(i + 1) * rows, :] = jnp.transpose(jnp.concatenate([code_got[i]] * (rows // 8), axis=0))

    early = lo
    pl.when(at_end)(lambda: w_slab(slabs[3], False, (0,)))
    for n in range(steps):
        logits[n * step:(n + 1) * step, :] += scores(n, slabs[3], y * (slab - early), early)
    pl.when(at_end)(lambda: w_slab(slabs[3], False, (1,), (0,)))
    for n in range(steps):
        logits[n * step:(n + 1) * step, :] += scores(n, slabs[3], (1 - y) * early, 128)
    pl.when(at_end)(lambda: w_slab(slabs[3], False, (1,), (1,)))

    sums = jnp.zeros((8, rows), f32)
    for n in range(steps):
        span = pl.ds(n * step, step)
        capped = softcap * jnp.tanh((logits[span, :] + scores(n, slabs[3], (1 - y) * early + 128, slab - early - 128)) * (1.0 / softcap))
        raised = jnp.exp(capped)
        logits[span, :] = capped
        expo[span, :] = raised
        total = jnp.broadcast_to(jnp.sum(raised, axis=1, keepdims=True), (step, 128))
        for k in range(2):
            turned = jnp.transpose(total[k * rows:(k + 1) * rows])
            sums = jnp.where(lines == 2 * n + k, turned[0:8], sums)
    stat_own[...] = sums

    def stat_copy(n):
        bb, vv, _ = peer(n)
        return copy(stat_own, stat_all.at[me], ss.at[0], sr.at[0], bb, vv)

    for n in range(len(peers)):
        stat_copy(n).start()

    ids = (lax.broadcasted_iota(jnp.int32, (step, half), 1) + (v * ny + y) * half).astype(f32)
    hit_total = jnp.zeros((step, 1), f32)
    for n in range(steps):
        span = pl.ds(n * step, step)
        capped = logits[span, :]
        hit = ids == code_all[span, 0:1]
        slope = 1.0 - (capped * (1.0 / softcap)) ** 2
        expo[span, :] = expo[span, :] * slope
        logits[span, :] = jnp.where(hit, slope, 0.0)
        hit_total = hit_total + jnp.sum(jnp.where(hit, capped, 0.0), axis=1, keepdims=True)
    hit_total = jnp.sum(hit_total, axis=0, keepdims=True)
    loss_one[...] = jnp.broadcast_to(hit_total, loss_one.shape)

    def hit_copy(n):
        bb, vv, _ = peer(n)
        return copy(loss_one, loss_all.at[me], ls.at[0], lr.at[0], bb, vv)

    for n in range(len(peers)):
        hit_copy(n).start()
    code_rows = jnp.zeros((8, rows), f32)
    for i in range(group):
        code_rows = jnp.where(lines == i, code_got[i], code_rows)
    weight = (code_rows >= 0).astype(f32)

    share_end(0, 0)
    share_end(1, 0)
    stat_all[me] = sums
    copy(stat_all.at[others], stat_all.at[others], ss.at[0], sr.at[0], b, over_x).wait_recv()
    partition = stat_all[0]
    for i in range(1, group):
        partition = partition + stat_all[i]
    scale = weight / partition

    lane_parts = [pl.ds(n * 128, 128) for n in range(half // 128)]
    over_parts = [pl.ds(0, 128), pl.ds(128, half - 128)]

    def delta_copy(p):
        here = over_parts[p]
        return copy(delta.at[0, :, here], delta.at[1, :, here], es.at[0], (cr, er)[p].at[0], over_y, v)

    chunks = range(half // 128)

    def chunk_of_delta(n):
        here = pl.ds(n * 128, 128)
        return copy(delta.at[0, :, here], d_end.at[:, here], zs.at[0], zr.at[n], near_end * ny + y, v)

    by_row = [jnp.transpose(jnp.broadcast_to(scale[i:i + 1, :], (rows, rows))) for i in range(group)]
    for n in chunks:
        here = pl.ds(n * 128, 128)
        for i in range(group):
            span = pl.ds(i * rows, rows)
            delta[0, span, here] = (expo[span, here] * by_row[i] - logits[span, here]).astype(bf16)
        pl.when(at_end)(lambda: chunk_of_delta(n).start())
        if n in (0, half // 128 - 1):
            delta_copy(min(n, 1)).start()

    targets = [jnp.where(at_end, far, across), jnp.where(at_end, across, near), jnp.where(at_end, near_end, far), z]
    top = y * shift

    def over_tokens(left, right):
        return lax.dot_general(left, right, (((0,), (0,)), ((), ())), preferred_element_type=f32)

    def grad_share(zz, r):
        return over_tokens(h_all[:, window(zz)], delta[r])

    def sent(k, r):
        return grad_send.at[k, r, pl.ds(pl.multiple_of(top, 16), cols)]

    def r_copy(k, r):
        return copy(sent(k, r), r_in.at[z * 2 + r], rs.at[0], rr.at[z, r], targets[k] * ny + y, v)

    def relay_copy(n, p):
        src = grad_send.at[n, 1, pl.ds(pl.multiple_of(top, 16), cols), lane_parts[p]]
        return copy(src, far_in.at[n, :, lane_parts[p]], rs.at[0], fr.at[n, p], near_end * ny + y, v)

    def part_copy(k, p):
        src = grad_send.at[k, 1, pl.ds(pl.multiple_of(top, 16), cols), lane_parts[p]]
        return copy(src, r_in.at[z * 2 + 1, :, lane_parts[p]], rs.at[0], rr.at[z, 1], targets[k] * ny + y, v)

    def chunk_copy(k, n):
        here = pl.ds(n * 128, 128)
        src = grad_send.at[k, 0, pl.ds(pl.multiple_of(top, 16), cols), here]
        return copy(src, r_in.at[z * 2, :, here], rs.at[0], rr.at[z, 0], targets[k] * ny + y, v)

    def to_end():
        @pl.when(inside)
        def _():
            grad_send[1, 0] = grad_share(near, 0).astype(bf16)
            r_copy(1, 0).start()

    def keep():
        @pl.when(inside)
        def _():
            held[0] = grad_share(across, 0)
            held[1] = grad_share(far, 0)

    def chunk(n):
        first = n * 128

        @pl.when(inside)
        def _():
            if n == 0:
                for kx in range(2):
                    for ky in range(2):
                        end_copy(flip(y, ky) * nv + flip(x, kx) * 2 + 1 - core).wait_recv()
            chunk_of_delta(n).wait_recv()
            right = d_end[:, first:first + 128]
            for k, slot, j in ((0, 0, 1), (2, 1, 0)):
                share = held[slot, :, first:first + 128] + over_tokens(h_end[:, j * win:(j + 1) * win], right)
                grad_send[k, 0, :, first:first + 128] = share.astype(bf16)
                chunk_copy(k, n).start()
            grad_own[0, :, first:first + 128] += over_tokens(h_end[:, 2 * win:3 * win], right)

    def head_part(k, p):
        here = over_parts[p]
        share = over_tokens(h_all[:, window(targets[k])], delta[1, :, here])
        which = chunks[1:] if p else chunks[:1]
        if k:
            grad_send[k, 1, :, here] = share.astype(bf16)
            for q in which:
                pl.when(at_end)(lambda: relay_copy(1, q).start())
                pl.when(inside)(lambda: part_copy(k, q).start())
        else:
            @pl.when(at_end)
            def _():
                grad_send[k, 1, :, here] = share.astype(bf16)
                for q in which:
                    relay_copy(0, q).start()

            @pl.when(inside)
            def _():
                held[0, :, here] = share

    def head_rest():
        share = grad_share(targets[2], 1)

        @pl.when(at_end)
        def _():
            grad_send[2, 1] = share.astype(bf16)
            r_copy(2, 1).start()

        @pl.when(inside)
        def _():
            held[1] = share

    cstep = chunk_of(cols, 64)

    def over_cols(body):
        def one(n, carry):
            body(pl.multiple_of(n * cstep, 16))
            return carry

        lax.fori_loop(0, cols // cstep, one, 0)

    def relay(k, n, p):
        lane = lane_parts[p]

        @pl.when(inside)
        def _():
            relay_copy(n, p).wait_recv()

            def add(m):
                here = pl.ds(pl.multiple_of(top + m, 16), cstep)
                there = pl.ds(m, cstep)
                grad_send[k, 1, here, lane] = (
                    held[k // 2, here, lane] + far_in[n, there, lane].astype(f32)).astype(bf16)

            over_cols(add)
            part_copy(k, p).start()

    groups = column_groups(width)
    blocks = [(1, 1), (1, 0), (0, 1), (0, 0)]
    unit = width // (width // 256)

    def span_of(g):
        first, n = groups[g]
        return pl.ds(first * unit, n * unit)

    y_first = (3,)

    def block(g, one, two, cc):
        kx, ky = (two, one) if g in y_first else (one, two)
        return flip(y, ky) * nv + flip(x, kx) * 2 + cc

    def core_copy(g, one, two):
        return copy(part.at[hrow(block(g, one, two, 1 - core)), span_of(g)], core_in.at[one, two, :, span_of(g)],
                    ds.at[0], wr.at[g, 0], b, over_core)

    def over_one(g):
        return (over_y, v) if g in y_first else (b, over_x)

    def over_two(g):
        return (b, over_x) if g in y_first else (over_y, v)

    def one_copy(g, two):
        return copy(x_out.at[two, :, span_of(g)], x_in.at[two, :, span_of(g)], xs.at[0], (hr if two else xr).at[g],
                    *over_one(g))

    def two_copy(g):
        return copy(y_out.at[:, span_of(g)], y_in.at[:, span_of(g)], ys.at[0], wr.at[g, 1], *over_two(g))

    def part_group(g):
        first, n = groups[g]

        def columns(j, carry):
            span = pl.ds(pl.multiple_of(j * unit, 128), unit)
            part[:, span] = lax.dot_general(
                delta[0], w_all[span, :], (((1,), (1,)), ((), ())), preferred_element_type=f32)
            return carry

        lax.fori_loop(first, first + n, columns, 0)
        for one, two in blocks:
            core_copy(g, one, two).start()

    hstep = 16

    def over_rows(body):
        def one(n, carry):
            body(pl.multiple_of(n * hstep, hstep))
            return carry

        lax.fori_loop(0, rows // hstep, one, 0)

    def core_sum(g):
        span = span_of(g)
        landed = core_in.at[:, :, :, span]
        copy(landed, landed, ds.at[0], wr.at[g, 0], b, over_core).wait_recv()
        for one, two in blocks:
            start = block(g, one, two, core) * rows

            def add(n):
                here = pl.ds(pl.multiple_of(start + n, hstep), hstep)
                both = part[here, span] + core_in[one, two, pl.ds(n, hstep), span]
                if one:
                    x_out[two, pl.ds(n, hstep), span] = both.astype(bf16)
                else:
                    part[here, span] = both

            over_rows(add)
            if one:
                one_copy(g, two).start()

    def one_sum(g):
        span = span_of(g)
        for two in (1, 0):
            one_copy(g, two).wait_recv()
            start = block(g, 0, two, core) * rows

            def add(n):
                here = pl.ds(pl.multiple_of(start + n, hstep), hstep)
                total = part[here, span] + x_in[two, pl.ds(n, hstep), span].astype(f32)
                if two:
                    y_out[pl.ds(n, hstep), span] = total.astype(bf16)
                else:
                    hid_out[pl.ds(n, hstep), span] = total

            over_rows(add)
            if two:
                two_copy(g).start()

    def two_sum(g):
        span = span_of(g)
        two_copy(g).wait_recv()

        def add(n):
            here = pl.ds(n, hstep)
            hid_out[here, span] += y_in[here, span].astype(f32)

        over_rows(add)

    count = len(groups)

    def plane_copy(k):
        return copy(loss_two, loss_zs.at[z], ms.at[0], mr.at[0], z_peer(k), v)

    def plane_loss():
        loss_all[me] = loss_one[...]
        copy(loss_all.at[others], loss_all.at[others], ls.at[0], lr.at[0], b, over_x).wait_recv()
        hits = loss_all[0]
        for i in range(1, group):
            hits = hits + loss_all[i]
        logs = jnp.sum(weight * jnp.log(partition), axis=1, keepdims=True)
        loss_two[...] = jnp.broadcast_to(jnp.sum(logs, axis=0, keepdims=True), (8, rows)) - hits
        for k in range(1, nz):
            plane_copy(k).start()

    part_group(0)
    part_group(1)
    to_end()
    plane_loss()
    core_sum(0)
    part_group(2)
    core_sum(1)
    share_end(0, 1)
    keep()
    part_group(3)
    core_sum(2)
    share_end(1, 1)
    grad_own[0] = grad_share(z, 0)
    part_group(4)
    core_sum(3)
    chunk(0)
    for g in range(5, count):
        part_group(g)
        core_sum(g - 1)
    core_sum(count - 1)
    for n in chunks[1:-1]:
        chunk(n)
    one_sum(0)

    delta_copy(0).wait_recv()
    head_part(0, 0)
    head_part(1, 0)
    chunk(len(chunks) - 1)
    delta_copy(1).wait_recv()
    head_part(0, 1)
    head_part(1, 1)
    one_sum(1)
    head_rest()
    grad_own[1] = grad_share(z, 1)
    one_sum(2)
    relay(2, 0, 0)

    copy(w_over, w_over, wys.at[0], wr.at[0, 0], over_y, v).wait_send()
    for n in range(1, nz):
        sent_rows = w_all.at[pl.ds(0, n * slab)]
        for way, slabs_sent in ((0, z + 1), (1, nz - z)):
            going = (slabs_sent == n) & (has_down if way else has_up)
            pl.when(going)(lambda: copy(sent_rows, sent_rows, ws.at[way], wr.at[0, 0], b, over_x).wait_send())
    seven = h_all.at[pl.ds(0, 7 * rows)]
    copy(seven, seven, hs.at[0], hr.at[0], b, over_x).wait_send()
    for got, sem in ((code_got, cs), (stat_all, ss), (loss_all, ls)):
        copy(got.at[others], got.at[others], sem.at[0], sem.at[0], b, over_x).wait_send()
    one_sum(3)
    two_sum(0)
    copy(delta.at[0], delta.at[1], es.at[0], cr.at[0], over_y, v).wait_send()
    relay(0, 1, 0)
    copy(core_in, core_in, ds.at[0], wr.at[0, 0], b, over_core).wait_send()
    one_sum(4)
    two_sum(1)
    for p in chunks[1:]:
        relay(2, 0, p)
    for p in chunks[1:]:
        relay(0, 1, p)
    for g in range(5, count):
        one_sum(g)
    two_sum(2)
    for g in range(4, count - 1):
        two_sum(g)

    def r_got(zz, r):
        whole = r_in.at[zz * 2 + r]
        copy(whole, whole, rs.at[0], rr.at[zz, r], z_peer(1), v).wait_recv()

    def lanes(r):
        return pl.ds(pl.multiple_of(flip(y, r) * half, 128), half)

    def head_sum(r):
        r_got(across, r)

        def add(n):
            here = pl.ds(n, cstep)
            total = grad_own[r, pl.ds(pl.multiple_of(top + n, 16), cstep), :]
            head_out[here, lanes(r)] = total + r_in[across * 2 + r, here, :].astype(f32)

        over_cols(add)

        def by_near():
            r_got(near, r)

            def last(n):
                here = pl.ds(n, cstep)
                head_out[here, lanes(r)] += r_in[near * 2 + r, here, :].astype(f32)

            over_cols(last)

        if r:
            by_near()
        else:
            pl.when(at_end)(by_near)

    head_sum(0)
    loss_zs[z] = loss_two[...]
    along = loss_zs.at[pl.ds(0, nz - 1)]
    copy(along, along, ms.at[0], mr.at[0], z_peer(1), v).wait_recv()
    losses = loss_zs[0]
    for i in range(1, nz):
        losses = losses + loss_zs[i]
    loss_out[...] = losses * (1.0 / (tokens * nz))
    copy(along, along, ms.at[0], mr.at[0], z_peer(1), v).wait_send()
    two_sum(3)
    two_sum(count - 1)
    head_sum(1)

    rows_out = h_end.at[pl.ds(0, tokens // 2)]
    for part_sent, sem in ((x_out, xs), (y_out, ys), (rows_out, us)):
        copy(part_sent, part_sent, sem.at[0], sem.at[0], b, over_x).wait_send()

    @pl.when(at_end)
    def _():
        for part_sent, sem in ((d_end, zs), (r_in.at[pl.ds(0, 3)], rs)):
            copy(part_sent, part_sent, sem.at[0], sem.at[0], b, over_x).wait_send()

    @pl.when(inside)
    def _():
        six = r_in.at[pl.ds(0, 6)]
        copy(six, six, rs.at[0], rs.at[0], b, over_x).wait_send()


def finish_kernel(head_in, hid_in, loss_in, head_out, hid_out, loss_out, loss_one, sem):
    moves = [
        pltpu.make_async_copy(hid_in, hid_out, sem.at[0]),
        pltpu.make_async_copy(head_in, head_out, sem.at[1]),
        pltpu.make_async_copy(loss_one, loss_out, sem.at[2]),
    ]
    for one in moves[:2]:
        one.start()
    loss_one[...] = loss_in[0:1, 0:1]
    moves[2].start()
    for one in moves:
        one.wait()


def plane_local(hidden, head_weight, targets, valid_mask):
    nz, ny, nv = 4, 2, 4
    rows, width = hidden.shape
    entries, cols = head_weight.shape
    half = entries // ny
    group = ny * nv
    tokens = rows * group
    shift = cols % 128
    win = -(-(cols + shift) // 128) * 128
    vm = pltpu.VMEM
    dma = pltpu.SemaphoreType.DMA
    count = len(column_groups(width))
    line = vm((8, rows), f32)
    buffers = [
        vm((tokens, width), bf16), vm((width, half), bf16), vm((cols, half), bf16),
        vm((1, rows), jnp.int32), vm((1, rows), jnp.int32), line, vm((group, 8, rows), f32), vm((tokens, 128), f32),
        vm((tokens, half), f32), vm((tokens, half), f32), vm((2, tokens, half), bf16),
        line, vm((group, 8, rows), f32), line, line, vm((group, 8, rows), f32), vm((nz, 8, rows), f32),
        vm((2, win, half), f32), vm((2, win, half), f32), vm((3, 2, win, half), bf16),
        vm((2, cols, half), bf16), vm((nz * 2, cols, half), bf16), vm((tokens, 3 * win), bf16), vm((tokens, half), bf16),
        vm((tokens, width), f32), vm((2, 2, rows, width), f32),
        vm((2, rows, width), bf16), vm((2, rows, width), bf16), vm((rows, width), bf16), vm((rows, width), bf16),
    ]
    sems = [
        dma((5,)), dma((1,)), dma((group,)), dma((2,)), dma((8, 2)), dma((1,)),
        dma((1,)), dma((1,)), dma((1,)), dma((1,)), dma((1,)), dma((1,)), dma((1,)), dma((1,)),
        dma((1,)), dma((1,)), dma((1,)), dma((nz, 2)), dma((2, half // 128)), dma((1,)), dma((half // 128,)), dma((1,)), dma((group,)),
        dma((1,)), dma((1,)), dma((count,)), dma((1,)),
    ]
    whole = pl.BlockSpec(memory_space=vm)
    head_t, hidden_grad, loss = pl.pallas_call(
        plane_kernel,
        out_shape=(
            vm((cols, entries), f32),
            vm((rows, width), f32),
            vm((8, rows), f32),
        ),
        in_specs=[pl.BlockSpec(memory_space=pl.ANY)] * 4,
        out_specs=(whole,) * 3,
        scratch_shapes=buffers + sems,
        compiler_params=pltpu.CompilerParams(
            collective_id=1, has_side_effects=True, vmem_limit_bytes=58 * 1024 * 1024),
    )(hidden, jnp.transpose(head_weight), targets[None, :], valid_mask[None, :])
    anywhere = pl.BlockSpec(memory_space=pl.ANY)
    head_t, hidden_grad, loss = pl.pallas_call(
        finish_kernel,
        out_shape=(
            jax.ShapeDtypeStruct((cols, entries), f32),
            jax.ShapeDtypeStruct((rows, width), f32),
            jax.ShapeDtypeStruct((1, 1), f32),
        ),
        in_specs=[whole] * 3,
        out_specs=(anywhere,) * 3,
        scratch_shapes=[vm((1, 1), f32), dma((3,))],
        compiler_params=pltpu.CompilerParams(vmem_limit_bytes=1024 * 1024),
    )(head_t, hidden_grad, loss)
    return jnp.transpose(head_t), hidden_grad, loss[0, 0]


def in_planes(nb, nv, hidden, head_weight, targets, valid_mask):
    rows, width = hidden.shape
    entries, cols = head_weight.shape
    fits = nb == 8 and nv == 4 and rows == 128 and width % 256 == 0 and width >= 3072
    fits = fits and len(column_groups(width)) <= 8
    return fits and cols >= 256 and entries % 256 == 0 and entries >= 512 and cols % 32 == 0 and (2 * cols) % 128 == 0


def device(nb, nv, *arrays):
    if in_planes(nb, nv, *arrays):
        return plane_local(*arrays)
    return local(nb, nv, *arrays)


def solution(mesh):
    placed = (
        P(("batch", "vocab"), None),
        P("vocab", "batch"),
        P(("batch", "vocab")),
        P(("batch", "vocab")),
    )
    return jax.shard_map(
        functools.partial(device, mesh.shape["batch"], mesh.shape["vocab"]),
        mesh=mesh,
        in_specs=placed,
        out_specs=(P("vocab", "batch"), P(("batch", "vocab"), None), P()),
        check_vma=False,
    )
```
